8 devices in a mesh: dp: 2 (over z, y), tp: 4 (over x, core).
Axes of the slice: x: 2, y: 2, z: 1, core: 2. Of those that a mesh axis runs over, the one named last changes fastest.
Arguments:
- x_in: bfloat16 [1024, 3584], P('dp'), parts along dimension 0
- lengths: int32 [1024], P('dp'), parts along dimension 0
- norm_gain: bfloat16 [2, 3584], replicated
- w_q: bfloat16 [2, 3584, 4096], P(None, None, 'tp')
- w_k: bfloat16 [2, 3584, 2048], P(None, None, 'tp')
- w_v: bfloat16 [2, 3584, 2048], P(None, None, 'tp')
- w_o: bfloat16 [2, 4096, 3584], P(None, 'tp')
- w_gate: bfloat16 [2, 3584, 14336], P(None, None, 'tp')
- w_up: bfloat16 [2, 3584, 14336], P(None, None, 'tp')
- w_down: bfloat16 [2, 14336, 3584], P(None, 'tp')
- k_cache: bfloat16 [2, 1024, 32, 8, 256], P(None, 'dp', None, 'tp'), parts along dimension 1
- v_cache: bfloat16 [2, 1024, 32, 8, 256], P(None, 'dp', None, 'tp'), parts along dimension 1
Outputs:
- output: bfloat16 [1024, 3584], P('dp'), parts along dimension 0
There are 2 independent parts. The reference program is written for one: setup_inputs(seed, part) draws one part's arguments, and reference() takes and returns one part's arrays. A program takes and returns all parts, laid end to end along the dimension named above; an argument that names none is the same for every part.
All inputs are finite; a program needn't handle non-finite values.
Results may differ from the reference program's by a relative error of at most 0.0171358.
Values are sent between devices in bfloat16 or wider.
A program may use at most 1.25 GiB of HBM per device.

```python
import math
import jax
import jax.numpy as jnp
from jax import lax

D = 3584
HEADS = 16
KV_HEADS = 8
FF = 14336
HEAD = 256
BATCH = 512
SEQ = 32
LAYERS = 2
ROPE_BASE = 500000
NORM_EPS = 1e-5
GROUP = HEADS // KV_HEADS
LOG_LEVELS = int(math.log2(SEQ)) + 1


def draw_lengths(len_key):
    exp_key, val_key, top_key = jax.random.split(len_key, 3)
    span_exp = jax.random.randint(exp_key, (BATCH,), 0, LOG_LEVELS)
    span_limit = jnp.minimum(jnp.left_shift(jnp.ones_like(span_exp), span_exp), SEQ - 1)
    drawn_len = 1 + jax.random.randint(val_key, (BATCH,), 0, span_limit)
    full_slot = jax.random.randint(top_key, (), 0, BATCH)
    return jnp.where(jnp.arange(BATCH) == full_slot, SEQ - 1, drawn_len).astype(jnp.int32)


def setup_inputs(seed: int = 0, part: int = 0) -> dict:
    base_key = jax.random.key(seed)
    shared_keys = jax.random.split(base_key, 8)
    own_keys = jax.random.split(jax.random.fold_in(base_key, part), 4)
    q_width = HEADS * HEAD
    kv_width = KV_HEADS * HEAD

    def draw_weight(key_index, arr_shape, std_scale):
        return (jax.random.normal(shared_keys[key_index], arr_shape, jnp.float32) * std_scale).astype(jnp.bfloat16)

    return {
        'x_in': jax.random.normal(own_keys[0], (BATCH, D), jnp.float32).astype(jnp.bfloat16),
        'lengths': draw_lengths(own_keys[1]),
        'norm_gain': (1.0 + 0.3 * jax.random.normal(shared_keys[0], (LAYERS, D), jnp.float32)).astype(jnp.bfloat16),
        'w_q': draw_weight(1, (LAYERS, D, q_width), D ** -0.5),
        'w_k': draw_weight(2, (LAYERS, D, kv_width), 2.0 * D ** -0.5),
        'w_v': draw_weight(3, (LAYERS, D, kv_width), D ** -0.5),
        'w_o': draw_weight(4, (LAYERS, q_width, D), 2.0 * q_width ** -0.5),
        'w_gate': draw_weight(5, (LAYERS, D, FF), D ** -0.5),
        'w_up': draw_weight(6, (LAYERS, D, FF), D ** -0.5),
        'w_down': draw_weight(7, (LAYERS, FF, D), FF ** -0.5),
        'k_cache': (2.0 * jax.random.normal(own_keys[2], (LAYERS, BATCH, SEQ, KV_HEADS, HEAD), jnp.float32)).astype(jnp.bfloat16),
        'v_cache': jax.random.normal(own_keys[3], (LAYERS, BATCH, SEQ, KV_HEADS, HEAD), jnp.float32).astype(jnp.bfloat16),
    }


def rms_norm(x_res, gain_row):
    x_f32 = x_res.astype(jnp.float32)
    inv_rms = lax.rsqrt(jnp.mean(x_f32 * x_f32, axis=-1, keepdims=True) + NORM_EPS)
    return (x_f32 * inv_rms * gain_row.astype(jnp.float32)).astype(jnp.bfloat16)


def rope_rotate(head_vecs, positions):
    half_dim = HEAD // 2
    inv_freq = 1.0 / (ROPE_BASE ** (jnp.arange(0, HEAD, 2).astype(jnp.float32) / HEAD))
    angles = positions.astype(jnp.float32)[:, None] * inv_freq[None, :]
    cos_ang = jnp.cos(angles)[:, None, :]
    sin_ang = jnp.sin(angles)[:, None, :]
    vec_f32 = head_vecs.astype(jnp.float32)
    rot_first = vec_f32[..., :half_dim]
    rot_second = vec_f32[..., half_dim:]
    return jnp.concatenate([rot_first * cos_ang - rot_second * sin_ang, rot_second * cos_ang + rot_first * sin_ang], axis=-1).astype(jnp.bfloat16)


def decode_attention(q_rot, k_rot, v_new, k_layer, v_layer, lengths):
    attn_scale = HEAD ** -0.5
    q_f32 = q_rot.astype(jnp.float32)
    cache_logits = jnp.einsum('bkgd,bskd->bkgs', q_f32, k_layer.astype(jnp.float32)) * attn_scale
    valid_mask = jnp.arange(SEQ)[None, :] < lengths[:, None]
    cache_logits = jnp.where(valid_mask[:, None, None, :], cache_logits, -jnp.inf)
    self_logit = jnp.einsum('bkgd,bkd->bkg', q_f32, k_rot.astype(jnp.float32)) * attn_scale
    row_peak = jnp.maximum(jnp.max(cache_logits, axis=-1), self_logit)
    cache_w = jnp.exp(cache_logits - row_peak[..., None])
    self_w = jnp.exp(self_logit - row_peak)
    prob_denom = jnp.sum(cache_w, axis=-1) + self_w
    cache_p = (cache_w / prob_denom[..., None]).astype(jnp.bfloat16)
    self_p = (self_w / prob_denom).astype(jnp.bfloat16)
    cache_part = jnp.einsum('bkgs,bskd->bkgd', cache_p.astype(jnp.float32), v_layer.astype(jnp.float32))
    self_part = self_p.astype(jnp.float32)[..., None] * v_new.astype(jnp.float32)[:, :, None, :]
    return (cache_part + self_part).astype(jnp.bfloat16)


def reference(x_in, lengths, norm_gain, w_q, w_k, w_v, w_o, w_gate, w_up, w_down, k_cache, v_cache):
    def layer_step(x_res, layer_args):
        gain_row, wq_layer, wk_layer, wv_layer, wo_layer, wg_layer, wu_layer, wd_layer, k_layer, v_layer = layer_args
        normed = rms_norm(x_res, gain_row)
        q_proj = jnp.dot(normed, wq_layer, preferred_element_type=jnp.float32).astype(jnp.bfloat16).reshape(BATCH, HEADS, HEAD)
        k_proj = jnp.dot(normed, wk_layer, preferred_element_type=jnp.float32).astype(jnp.bfloat16).reshape(BATCH, KV_HEADS, HEAD)
        v_new = jnp.dot(normed, wv_layer, preferred_element_type=jnp.float32).astype(jnp.bfloat16).reshape(BATCH, KV_HEADS, HEAD)
        q_rot = rope_rotate(q_proj, lengths).reshape(BATCH, KV_HEADS, GROUP, HEAD)
        k_rot = rope_rotate(k_proj, lengths)
        attn_flat = decode_attention(q_rot, k_rot, v_new, k_layer, v_layer, lengths).reshape(BATCH, HEADS * HEAD)
        attn_proj = jnp.dot(attn_flat, wo_layer, preferred_element_type=jnp.float32)
        gate_act = jnp.dot(normed, wg_layer, preferred_element_type=jnp.float32).astype(jnp.bfloat16)
        up_act = jnp.dot(normed, wu_layer, preferred_element_type=jnp.float32).astype(jnp.bfloat16)
        mlp_hidden = (jax.nn.silu(gate_act.astype(jnp.float32)) * up_act.astype(jnp.float32)).astype(jnp.bfloat16)
        mlp_proj = jnp.dot(mlp_hidden, wd_layer, preferred_element_type=jnp.float32)
        x_next = (x_res.astype(jnp.float32) + attn_proj + mlp_proj).astype(jnp.bfloat16)
        return x_next, None

    scan_result = lax.scan(layer_step, x_in, (norm_gain, w_q, w_k, w_v, w_o, w_gate, w_up, w_down, k_cache, v_cache))
    return scan_result[0]
```

```python
import functools

import jax
import jax.numpy as jnp
from jax import lax
from jax.experimental import pallas as pl
from jax.experimental.pallas import tpu as pltpu
from jax.sharding import PartitionSpec as P

NORM_EPS = 1e-5
ROPE_BASE = 500000.0
MESH = pl.DeviceIdType.MESH

ROWS = 256
HALF = 128
TILE = 512
SLOTS = 7
WO_SLOTS = 2
KV_SLOTS = 4
KV_TOK = 16


def kernel(cfg, lens_ref, cos_ref, sin_ref, gain_ref, x_in, wq, wk, wv, wo, wg, wu, wd, kc, vc, x_out,
           xs, a_s, q_s, k_s, v_s, att_s, u_s, graw, uraw, sidx, wbuf, wobuf, kbuf, vbuf, ybuf, irecv, rown, xrecv,
           wsem, wosem, kvsem, xsem, isend, irsem, xsend, xrsem, nsend, nrsem, osem):
    layers, tokens, width, seq, kv_heads = cfg
    tok_rows = seq * kv_heads * 2
    chunks = tokens // ROWS
    stages = layers * chunks
    n_dn = width // TILE
    n_ff = wg.shape[2] // TILE
    n_q = wq.shape[2] // TILE
    n_w = n_q + 2 + 2 * n_ff + n_dn
    n_kv = ROWS // KV_TOK
    all_w, all_wo, all_kv = stages * n_w, stages * n_dn, stages * n_kv

    tp = lax.axis_index("tp")
    core = lax.rem(tp, 2)
    sib = tp + 1 - 2 * core
    partner = lax.rem(tp + 2, 4)
    own_row = pl.multiple_of(core * HALF, HALF)
    sib_row = pl.multiple_of((1 - core) * HALF, HALF)

    def w_start(gt):
        st = lax.div(gt, n_w)
        t = gt - st * n_w
        layer = lax.div(st, chunks)
        slot = lax.rem(gt, SLOTS)

        def put(src):
            pltpu.make_async_copy(src, wbuf.at[slot], wsem.at[slot]).start()

        def cols(i):
            return pl.ds(pl.multiple_of(i * TILE, TILE), TILE)

        f = t - (n_q + 2)

        @pl.when(t < n_q)
        def _():
            put(wq.at[layer, :, cols(t)])

        @pl.when(t == n_q)
        def _():
            put(wk.at[layer])

        @pl.when(t == n_q + 1)
        def _():
            put(wv.at[layer])

        @pl.when((f >= 0) & (f < 2 * n_ff) & (lax.rem(f + 2, 2) == 0))
        def _():
            put(wg.at[layer, :, cols(lax.div(f, 2))])

        @pl.when((f >= 0) & (f < 2 * n_ff) & (lax.rem(f + 2, 2) == 1))
        def _():
            put(wu.at[layer, :, cols(lax.div(f, 2))])

        @pl.when(f >= 2 * n_ff)
        def _():
            put(wd.at[layer, :, cols(f - 2 * n_ff)])

    def w_next(gt):
        @pl.when(gt + SLOTS < all_w)
        def _():
            w_start(gt + SLOTS)

    def w_wait(gt):
        slot = lax.rem(gt, SLOTS)
        pltpu.make_async_copy(wk.at[0], wbuf.at[slot], wsem.at[slot]).wait()
        return slot

    def wo_copy(go):
        st = lax.div(go, n_dn)
        j = go - st * n_dn
        slot = lax.rem(go, WO_SLOTS)
        cols = pl.ds(pl.multiple_of(j * TILE, TILE), TILE)
        return pltpu.make_async_copy(wo.at[lax.div(st, chunks), :, cols], wobuf.at[slot], wosem.at[slot])

    def kv_copies(gb):
        st = lax.div(gb, n_kv)
        b = gb - st * n_kv
        layer = lax.div(st, chunks)
        tok = layer * tokens + (st - layer * chunks) * ROWS + b * KV_TOK
        slot = lax.rem(gb, KV_SLOTS)
        rows = pl.ds(pl.multiple_of(tok * tok_rows, KV_TOK * tok_rows), KV_TOK * tok_rows)
        return (pltpu.make_async_copy(kc.at[rows], kbuf.at[slot], kvsem.at[0, slot]),
                pltpu.make_async_copy(vc.at[rows], vbuf.at[slot], kvsem.at[1, slot]))

    def chip_copy(par, j):
        return pltpu.make_async_remote_copy(
            src_ref=ybuf.at[j, pl.ds(sib_row, HALF)], dst_ref=irecv.at[par, j], send_sem=isend.at[j],
            recv_sem=irsem.at[par, j], device_id={"tp": sib}, device_id_type=MESH)

    def link_copy(par, j):
        return pltpu.make_async_remote_copy(
            src_ref=rown.at[j], dst_ref=xrecv.at[par, j], send_sem=xsend.at[j],
            recv_sem=xrsem.at[par, j], device_id={"tp": partner}, device_id_type=MESH)

    def x_piece(par, row, j):
        return xs.at[pl.ds(pl.multiple_of(par * ROWS + row, HALF), HALF), pl.ds(pl.multiple_of(j * TILE, TILE), TILE)]

    def new_copy(par, j):
        piece = x_piece(par, own_row, j)
        return pltpu.make_async_remote_copy(
            src_ref=piece, dst_ref=piece, send_sem=nsend.at[par, j],
            recv_sem=nrsem.at[par, j], device_id={"tp": sib}, device_id_type=MESH)

    def chip_sum(par, j):
        chip_copy(par, j).wait_recv()
        rown[j] = (ybuf[j, pl.ds(own_row, HALF)] + irecv[par, j]).astype(jnp.bfloat16)
        link_copy(par, j).start()

    def finish(par):
        def step(j, _):
            link_copy(par, j).wait()
            chip_copy(par, j).wait_send()
            piece = x_piece(par, own_row, j)
            total = rown[j].astype(jnp.float32) + xrecv[par, j].astype(jnp.float32)
            piece[...] = (piece[...].astype(jnp.float32) + total).astype(jnp.bfloat16)
            new_copy(par, j).start()
            return 0

        lax.fori_loop(0, n_dn, step, 0)

    def new_wait(par):
        def step(j, _):
            new_copy(par, j).wait()
            return 0

        lax.fori_loop(0, n_dn, step, 0)

    def x_copy(c):
        rows = pl.ds(pl.multiple_of(c * ROWS, ROWS), ROWS)
        return pltpu.make_async_copy(x_in.at[rows], xs.at[rows], xsem.at[c])

    def out_copy(c):
        rows = pl.ds(c * ROWS, ROWS)
        return pltpu.make_async_copy(xs.at[rows], x_out.at[rows], osem.at[c])

    for c in range(chunks):
        x_copy(c).start()
    for g in range(SLOTS):
        w_start(jnp.int32(g))
    for g in range(KV_SLOTS):
        for cp in kv_copies(jnp.int32(g)):
            cp.start()
    for g in range(WO_SLOTS):
        wo_copy(jnp.int32(g)).start()

    barrier = pltpu.get_barrier_semaphore()
    for other in (sib, partner):
        pl.semaphore_signal(barrier, inc=1, device_id={"tp": other}, device_id_type=MESH)
    pl.semaphore_wait(barrier, 2)

    n_key = 8 * tok_rows
    lane = lax.broadcasted_iota(jnp.int32, (32, n_key), 1)
    row = lax.broadcasted_iota(jnp.int32, (32, n_key), 0)
    per = 2 * kv_heads
    match = (lax.div(lane, tok_rows) == lax.rem(row, 8)) & (lax.rem(lane, kv_heads) == lax.div(row, 16)) & (lax.rem(lane, per) < kv_heads)
    sidx[...] = jnp.where(match, lax.rem(lax.div(lane, per), seq), 2 * seq)

    def rope(y, base, dst, col, rows):
        cos, sin = cos_ref[rows], sin_ref[rows]
        for h in range(TILE // 256):
            first = y[:, h * 256:h * 256 + 128].astype(jnp.bfloat16).astype(jnp.float32)
            second = y[:, h * 256 + 128:h * 256 + 256].astype(jnp.bfloat16).astype(jnp.float32)
            at = col + h * 256
            dst[:, at:at + 128] = (first * cos - second * sin).astype(jnp.bfloat16).astype(jnp.float32)
            dst[:, at + 128:at + 256] = (second * cos + first * sin).astype(jnp.bfloat16).astype(jnp.float32)

    def dot(a, b):
        return jnp.dot(a, b, preferred_element_type=jnp.float32)

    def attend(slot, b, c, half):
        base = pl.multiple_of(b * KV_TOK, KV_TOK) + half * 8
        base = pl.multiple_of(base, 8)
        tok = pl.ds(base, 8)
        q8, k8, v8 = q_s[tok], k_s[tok], v_s[tok]
        q = jnp.concatenate([q8[:, h * 256:(h + 1) * 256] for h in range(4)], 0)
        kn = jnp.concatenate([k8[:, (h // 2) * 256:(h // 2 + 1) * 256] for h in range(4)], 0)
        vn = jnp.concatenate([v8[:, (h // 2) * 256:(h // 2 + 1) * 256] for h in range(4)], 0)
        len8 = lens_ref[pl.ds(pl.multiple_of(c * ROWS + base, 8), 8), :]
        lens = jnp.concatenate([len8] * 4, 0)
        scale = 1.0 / 16.0
        qq = jnp.concatenate([q[:, :128], q[:, 128:]], 0).astype(jnp.bfloat16)
        rows = pl.ds(half * 8 * tok_rows, 8 * tok_rows)
        s2 = lax.dot_general(qq, kbuf[slot, rows], (((1,), (1,)), ((), ())), preferred_element_type=jnp.float32)
        s = (s2[:32] + jnp.concatenate([s2[32:, 2:], s2[32:, :2]], 1)) * scale
        s = jnp.where(sidx[...] < lens, s, -jnp.inf)
        self_logit = jnp.sum(q * kn, axis=-1, keepdims=True) * scale
        peak = jnp.maximum(jnp.max(s, axis=-1, keepdims=True), self_logit)
        w = jnp.exp(s - peak)
        sw = jnp.exp(self_logit - peak)
        inv = 1.0 / (jnp.sum(w, axis=-1, keepdims=True) + sw)
        p = w * inv
        sp = (sw * inv).astype(jnp.bfloat16).astype(jnp.float32)
        pp = jnp.concatenate([p, jnp.concatenate([p[:, n_key - 2:], p[:, :n_key - 2]], 1)], 0).astype(jnp.bfloat16)
        o2 = dot(pp, vbuf[slot, rows])
        return jnp.concatenate([o2[:32], o2[32:]], 1) + sp * vn

    def swiglu(i):
        g = graw[...].astype(jnp.float32)
        u = uraw[...].astype(jnp.float32)
        u_s[:, pl.ds(pl.multiple_of(i * TILE, TILE), TILE)] = (g * (1.0 / (1.0 + jnp.exp(-g))) * u).astype(jnp.bfloat16)

    def stage(st, _):
        layer = lax.div(st, chunks)
        c = st - layer * chunks
        par = c
        rows = pl.ds(pl.multiple_of(c * ROWS, ROWS), ROWS)
        w0 = st * n_w

        @pl.when(st < chunks)
        def _():
            x_copy(c).wait()

        @pl.when(st >= chunks)
        def _():
            new_wait(par)

        gains = gain_ref[...].astype(jnp.float32)
        gain = gains[:1]
        for other in range(1, layers):
            gain = jnp.where(layer == other, gains[other:other + 1], gain)

        def norm(i, _):
            r = pl.ds(pl.multiple_of(c * ROWS + i * 32, 32), 32)
            x = xs[r].astype(jnp.float32)
            inv = lax.rsqrt(jnp.sum(x * x, axis=-1, keepdims=True) / width + NORM_EPS)
            a_s[pl.ds(pl.multiple_of(i * 32, 32), 32)] = (x * inv * gain).astype(jnp.bfloat16)
            return 0

        lax.fori_loop(0, ROWS // 32, norm, 0)

        @pl.when(st >= 1)
        def _():
            for j in range(n_dn - 2, n_dn):
                chip_sum(1 - par, j)

        s0, s1 = w_wait(w0), w_wait(w0 + 1)
        rope(dot(a_s[...], wbuf[s0]), 0, q_s, 0, rows)
        rope(dot(a_s[...], wbuf[s1]), 0, q_s, TILE, rows)
        w_next(w0)
        w_next(w0 + 1)
        s0, s1 = w_wait(w0 + 2), w_wait(w0 + 3)
        rope(dot(a_s[...], wbuf[s0]), 0, k_s, 0, rows)
        v_s[...] = dot(a_s[...], wbuf[s1]).astype(jnp.bfloat16).astype(jnp.float32)
        w_next(w0 + 2)
        w_next(w0 + 3)

        def block(b, _):
            gb = st * n_kv + b
            slot = lax.rem(gb, KV_SLOTS)
            for cp in kv_copies(gb):
                cp.wait()
            o0, o1 = attend(slot, b, c, 0), attend(slot, b, c, 1)
            t = pl.ds(pl.multiple_of(b * KV_TOK, KV_TOK), KV_TOK)
            for h in range(4):
                o = jnp.concatenate([o0[h * 8:h * 8 + 8], o1[h * 8:h * 8 + 8]], 0)
                att_s[t, h * 256:(h + 1) * 256] = o.astype(jnp.bfloat16)

            @pl.when(gb + KV_SLOTS < all_kv)
            def _():
                for cp in kv_copies(gb + KV_SLOTS):
                    cp.start()

            return 0

        lax.fori_loop(0, n_kv, block, 0)

        def ff(i, _):
            gt = w0 + n_q + 2 + 2 * i
            s0, s1 = w_wait(gt), w_wait(gt + 1)
            swiglu(lax.rem(i + n_ff - 1, n_ff))
            graw[...] = dot(a_s[...], wbuf[s0]).astype(jnp.bfloat16)
            uraw[...] = dot(a_s[...], wbuf[s1]).astype(jnp.bfloat16)
            w_next(gt)
            w_next(gt + 1)
            return 0

        lax.fori_loop(0, n_ff, ff, 0)
        swiglu(n_ff - 1)

        @pl.when(st >= 1)
        def _():
            finish(1 - par)

        def down(j, _):
            gt = w0 + n_q + 2 + 2 * n_ff + j
            go = st * n_dn + j
            s0 = w_wait(gt)
            wo_copy(go).wait()

            @pl.when(j >= 2)
            def _():
                chip_sum(par, j - 2)

            ybuf[j] = dot(u_s[...], wbuf[s0]) + dot(att_s[...], wobuf[lax.rem(go, WO_SLOTS)])
            chip_copy(par, j).start()
            w_next(gt)

            @pl.when(go + WO_SLOTS < all_wo)
            def _():
                wo_copy(go + WO_SLOTS).start()

            return 0

        lax.fori_loop(0, n_dn, down, 0)
        return 0

    graw[...] = jnp.zeros_like(graw)
    uraw[...] = jnp.zeros_like(uraw)
    lax.fori_loop(0, stages, stage, 0)

    last = (stages - 1) % chunks
    for j in range(n_dn - 2, n_dn):
        chip_sum(last, j)
    new_wait(1 - last)
    out_copy(1 - last).start()
    finish(last)
    new_wait(last)
    out_copy(last).start()
    for c in range(chunks):
        out_copy(c).wait()


def solution(mesh):
    arg_specs = (P('dp', None), P('dp'), P(), P(None, None, 'tp'), P(None, None, 'tp'), P(None, None, 'tp'), P(None, 'tp', None), P(None, None, 'tp'), P(None, None, 'tp'), P(None, 'tp', None), P(None, 'dp', None, 'tp', None), P(None, 'dp', None, 'tp', None))

    def per_device(x_in, lengths, norm_gain, w_q, w_k, w_v, w_o, w_gate, w_up, w_down, k_cache, v_cache):
        layers, tokens, seq, kv_heads, head = k_cache.shape
        width = x_in.shape[1]
        half = head // 2
        inv_freq = 1.0 / (ROPE_BASE ** (jnp.arange(0, head, 2).astype(jnp.float32) / head))
        angles = lengths.astype(jnp.float32)[:, None] * inv_freq[None, :]
        cos, sin = jnp.cos(angles), jnp.sin(angles)

        def rows_of(cache):
            r = cache.reshape(layers * tokens * seq, kv_heads, 2, half).transpose(0, 2, 1, 3)
            return r.reshape(layers * tokens * seq * kv_heads * 2, half)

        tok_rows = seq * kv_heads * 2
        n_dn = width // TILE
        vm = pl.BlockSpec(memory_space=pltpu.VMEM)
        hbm = pl.BlockSpec(memory_space=pl.ANY)
        bf, f32 = jnp.bfloat16, jnp.float32
        dma = pltpu.SemaphoreType.DMA
        return pl.pallas_call(
            functools.partial(kernel, (layers, tokens, width, seq, kv_heads)),
            out_shape=jax.ShapeDtypeStruct(x_in.shape, bf),
            in_specs=[vm] * 4 + [hbm] * 10,
            out_specs=hbm,
            scratch_shapes=[
                pltpu.VMEM((tokens, width), bf),
                pltpu.VMEM((ROWS, width), bf),
                pltpu.VMEM((ROWS, w_q.shape[2]), f32),
                pltpu.VMEM((ROWS, w_k.shape[2]), f32),
                pltpu.VMEM((ROWS, w_v.shape[2]), f32),
                pltpu.VMEM((ROWS, w_q.shape[2]), bf),
                pltpu.VMEM((ROWS, w_gate.shape[2]), bf),
                pltpu.VMEM((ROWS, TILE), bf),
                pltpu.VMEM((ROWS, TILE), bf),
                pltpu.VMEM((32, 8 * tok_rows), jnp.int32),
                pltpu.VMEM((SLOTS, width, TILE), bf),
                pltpu.VMEM((WO_SLOTS, w_o.shape[1], TILE), bf),
                pltpu.VMEM((KV_SLOTS, KV_TOK * tok_rows, half), bf),
                pltpu.VMEM((KV_SLOTS, KV_TOK * tok_rows, half), bf),
                pltpu.VMEM((n_dn, ROWS, TILE), f32),
                pltpu.VMEM((2, n_dn, HALF, TILE), f32),
                pltpu.VMEM((n_dn, HALF, TILE), bf),
                pltpu.VMEM((2, n_dn, HALF, TILE), bf),
                dma((SLOTS,)), dma((WO_SLOTS,)), dma((2, KV_SLOTS)), dma((2,)),
                dma((n_dn,)), dma((2, n_dn)), dma((n_dn,)), dma((2, n_dn)), dma((2, n_dn)), dma((2, n_dn)), dma((2,)),
            ],
            compiler_params=pltpu.CompilerParams(
                collective_id=0, has_side_effects=True, vmem_limit_bytes=67_043_328),
            name="decoder",
        )(lengths[:, None], cos, sin, norm_gain, x_in, w_q, w_k, w_v, w_o, w_gate, w_up, w_down,
          rows_of(k_cache), rows_of(v_cache))

    return jax.shard_map(per_device, mesh=mesh, in_specs=arg_specs, out_specs=P('dp', None), check_vma=False)
```

```python
import functools

import jax
import jax.numpy as jnp
from jax import lax
from jax.experimental import pallas as pl
from jax.experimental.pallas import tpu as pltpu
from jax.sharding import PartitionSpec as P

NORM_EPS = 1e-5
ROPE_BASE = 500000.0
MESH = pl.DeviceIdType.MESH

ROWS = 256
HALF = 128
TILE = 512
SLOTS = 7
KV_SLOTS = 3
KV_TOK = 32


def kernel(cfg, lens_ref, cos_ref, sin_ref, gain_ref, x_in, wq, wk, wv, wo, wg, wu, wd, kc, vc, x_out,
           xs, a_s, q_s, k_s, v_s, att_s, u_s, graw, uraw, sidx, wbuf, wobuf, kbuf, vbuf, ybuf, irecv, rown, xrecv,
           wsem, wosem, kvsem, xsem, isend, irsem, xsend, xrsem, nsend, nrsem, osem):
    layers, tokens, width, seq, kv_heads = cfg
    tok_rows = seq * kv_heads * 2
    chunks = tokens // ROWS
    stages = layers * chunks
    n_dn = width // TILE
    n_ff = wg.shape[2] // TILE
    n_q = wq.shape[2] // TILE
    n_w = n_q + 2 + 2 * n_ff + n_dn
    n_kv = ROWS // KV_TOK
    all_w, all_kv = stages * n_w, stages * n_kv

    tp = lax.axis_index("tp")
    core = lax.rem(tp, 2)
    sib = tp + 1 - 2 * core
    partner = lax.rem(tp + 2, 4)
    own_row = pl.multiple_of(core * HALF, HALF)
    sib_row = pl.multiple_of((1 - core) * HALF, HALF)

    def w_start(gt):
        st = lax.div(gt, n_w)
        t = gt - st * n_w
        layer = lax.div(st, chunks)
        slot = lax.rem(gt, SLOTS)

        def put(src):
            pltpu.make_async_copy(src, wbuf.at[slot], wsem.at[slot]).start()

        def cols(i):
            return pl.ds(pl.multiple_of(i * TILE, TILE), TILE)

        f = t - (n_q + 2)

        @pl.when(t < n_q)
        def _():
            put(wq.at[layer, :, cols(t)])

        @pl.when(t == n_q)
        def _():
            put(wk.at[layer])

        @pl.when(t == n_q + 1)
        def _():
            put(wv.at[layer])

        @pl.when((f >= 0) & (f < 2 * n_ff) & (lax.rem(f + 2, 2) == 0))
        def _():
            put(wg.at[layer, :, cols(lax.div(f, 2))])

        @pl.when((f >= 0) & (f < 2 * n_ff) & (lax.rem(f + 2, 2) == 1))
        def _():
            put(wu.at[layer, :, cols(lax.div(f, 2))])

        @pl.when(f >= 2 * n_ff)
        def _():
            put(wd.at[layer, :, cols(f - 2 * n_ff)])

    def w_next(gt):
        @pl.when(gt + SLOTS < all_w)
        def _():
            w_start(gt + SLOTS)

    def w_wait(gt):
        slot = lax.rem(gt, SLOTS)
        pltpu.make_async_copy(wk.at[0], wbuf.at[slot], wsem.at[slot]).wait()
        return slot

    def wo_copy(layer, j):
        cols = pl.ds(pl.multiple_of(j * TILE, TILE), TILE)
        return pltpu.make_async_copy(wo.at[layer, :, cols], wobuf.at[j], wosem.at[j])

    def kv_copies(gb):
        st = lax.div(gb, n_kv)
        b = gb - st * n_kv
        layer = lax.div(st, chunks)
        tok = layer * tokens + (st - layer * chunks) * ROWS + b * KV_TOK
        slot = lax.rem(gb, KV_SLOTS)
        rows = pl.ds(pl.multiple_of(tok * tok_rows, KV_TOK * tok_rows), KV_TOK * tok_rows)
        return (pltpu.make_async_copy(kc.at[rows], kbuf.at[slot], kvsem.at[0, slot]),
                pltpu.make_async_copy(vc.at[rows], vbuf.at[slot], kvsem.at[1, slot]))

    def chip_copy(par, j):
        return pltpu.make_async_remote_copy(
            src_ref=ybuf.at[j, pl.ds(sib_row, HALF)], dst_ref=irecv.at[par, j], send_sem=isend.at[j],
            recv_sem=irsem.at[par, j], device_id={"tp": sib}, device_id_type=MESH)

    def link_copy(par, j):
        return pltpu.make_async_remote_copy(
            src_ref=rown.at[j], dst_ref=xrecv.at[par, j], send_sem=xsend.at[j],
            recv_sem=xrsem.at[par, j], device_id={"tp": partner}, device_id_type=MESH)

    def x_piece(par, row, j):
        return xs.at[pl.ds(pl.multiple_of(par * ROWS + row, HALF), HALF), pl.ds(pl.multiple_of(j * TILE, TILE), TILE)]

    def new_copy(par, j):
        piece = x_piece(par, own_row, j)
        return pltpu.make_async_remote_copy(
            src_ref=piece, dst_ref=piece, send_sem=nsend.at[par, j],
            recv_sem=nrsem.at[par, j], device_id={"tp": sib}, device_id_type=MESH)

    def chip_sum(par, j):
        chip_copy(par, j).wait_recv()
        rown[j] = (ybuf[j, pl.ds(own_row, HALF)] + irecv[par, j]).astype(jnp.bfloat16)
        link_copy(par, j).start()

    def finish(par):
        def step(j, _):
            link_copy(par, j).wait()
            chip_copy(par, j).wait_send()
            piece = x_piece(par, own_row, j)
            total = rown[j].astype(jnp.float32) + xrecv[par, j].astype(jnp.float32)
            piece[...] = (piece[...].astype(jnp.float32) + total).astype(jnp.bfloat16)
            new_copy(par, j).start()
            return 0

        lax.fori_loop(0, n_dn, step, 0)

    def new_wait(par):
        def step(j, _):
            new_copy(par, j).wait()
            return 0

        lax.fori_loop(0, n_dn, step, 0)

    def x_copy(c):
        rows = pl.ds(pl.multiple_of(c * ROWS, ROWS), ROWS)
        return pltpu.make_async_copy(x_in.at[rows], xs.at[rows], xsem.at[c])

    def out_copy(c):
        rows = pl.ds(c * ROWS, ROWS)
        return pltpu.make_async_copy(xs.at[rows], x_out.at[rows], osem.at[c])

    for c in range(chunks):
        x_copy(c).start()
    for g in range(SLOTS):
        w_start(jnp.int32(g))
    for g in range(KV_SLOTS):
        for cp in kv_copies(jnp.int32(g)):
            cp.start()
    for j in range(n_dn):
        wo_copy(0, j).start()

    barrier = pltpu.get_barrier_semaphore()
    for other in (sib, partner):
        pl.semaphore_signal(barrier, inc=1, device_id={"tp": other}, device_id_type=MESH)
    pl.semaphore_wait(barrier, 2)

    n_key = 8 * tok_rows
    lane = lax.broadcasted_iota(jnp.int32, (32, n_key), 1)
    row = lax.broadcasted_iota(jnp.int32, (32, n_key), 0)
    per = 2 * kv_heads
    match = (lax.div(lane, tok_rows) == lax.rem(row, 8)) & (lax.rem(lane, kv_heads) == lax.div(row, 16)) & (lax.rem(lane, per) < kv_heads)
    sidx[...] = jnp.where(match, lax.rem(lax.div(lane, per), seq), 2 * seq)

    def rope(y, base, dst, col, rows):
        cos, sin = cos_ref[rows], sin_ref[rows]
        for h in range(TILE // 256):
            first = y[:, h * 256:h * 256 + 128].astype(jnp.bfloat16).astype(jnp.float32)
            second = y[:, h * 256 + 128:h * 256 + 256].astype(jnp.bfloat16).astype(jnp.float32)
            at = col + h * 256
            dst[:, at:at + 128] = (first * cos - second * sin).astype(jnp.bfloat16).astype(jnp.float32)
            dst[:, at + 128:at + 256] = (second * cos + first * sin).astype(jnp.bfloat16).astype(jnp.float32)

    def dot(a, b):
        return jnp.dot(a, b, preferred_element_type=jnp.float32)

    scale = 1.0 / 16.0

    def roll(x, by):
        return jnp.concatenate([pltpu.roll(x[:, i:i + 128], by % 128, axis=1) for i in range(0, n_key, 128)], 1)

    def logits(slot, b, c, part):
        base = pl.multiple_of(b * KV_TOK + part * 8, 8)
        q8, k8 = q_s[pl.ds(base, 8)], k_s[pl.ds(base, 8)]
        q = jnp.concatenate([q8[:, h * 256:(h + 1) * 256] for h in range(4)], 0) * scale
        kn = jnp.concatenate([k8[:, (h // 2) * 256:(h // 2 + 1) * 256] for h in range(4)], 0)
        len8 = lens_ref[pl.ds(pl.multiple_of(c * ROWS + base, 8), 8), :]
        lens = jnp.concatenate([len8] * 4, 0)
        qq = jnp.concatenate([q[:, :128], q[:, 128:]], 0).astype(jnp.bfloat16)
        keys = kbuf[slot, pl.ds(part * n_key, n_key)]
        s2 = lax.dot_general(qq, keys, (((1,), (1,)), ((), ())), preferred_element_type=jnp.float32)
        s = s2[:32] + roll(s2[32:], -2)
        return jnp.where(sidx[...] < lens, s, -jnp.inf), jnp.sum(q * kn, axis=-1, keepdims=True)

    def mix(slot, b, part, s, self_logit):
        v8 = v_s[pl.ds(pl.multiple_of(b * KV_TOK + part * 8, 8), 8)]
        vn = jnp.concatenate([v8[:, (h // 2) * 256:(h // 2 + 1) * 256] for h in range(4)], 0)
        peak = jnp.maximum(jnp.max(s, axis=-1, keepdims=True), self_logit)
        w = jnp.exp(s - peak)
        sw = jnp.exp(self_logit - peak)
        inv = 1.0 / (jnp.sum(w, axis=-1, keepdims=True) + sw)
        p = w * inv
        sp = (sw * inv).astype(jnp.bfloat16).astype(jnp.float32)
        pp = jnp.concatenate([p, roll(p, 2)], 0).astype(jnp.bfloat16)
        o2 = dot(pp, vbuf[slot, pl.ds(part * n_key, n_key)])
        return jnp.concatenate([o2[:32], o2[32:]], 1) + sp * vn

    def swiglu(i):
        g = graw[...].astype(jnp.float32)
        u = uraw[...].astype(jnp.float32)
        u_s[:, pl.ds(pl.multiple_of(i * TILE, TILE), TILE)] = (g * (1.0 / (1.0 + jnp.exp(-g))) * u).astype(jnp.bfloat16)

    def stage(st, _):
        layer = lax.div(st, chunks)
        c = st - layer * chunks
        par = c
        rows = pl.ds(pl.multiple_of(c * ROWS, ROWS), ROWS)
        w0 = st * n_w

        @pl.when(st < chunks)
        def _():
            x_copy(c).wait()

        @pl.when(st >= chunks)
        def _():
            new_wait(par)

        gains = gain_ref[...].astype(jnp.float32)
        gain = gains[:1]
        for other in range(1, layers):
            gain = jnp.where(layer == other, gains[other:other + 1], gain)

        def norm(i, _):
            src = pl.ds(pl.multiple_of(c * ROWS + i * 16, 16), 16)
            dst = pl.ds(pl.multiple_of(i * 16, 16), 16)
            parts = range(0, width, 256)
            total = jnp.zeros((16, 256), jnp.float32)
            for p in parts:
                x = xs[src, p:p + 256].astype(jnp.float32)
                total = total + x * x
            inv = lax.rsqrt(jnp.sum(total, axis=-1, keepdims=True) / width + NORM_EPS)
            for p in parts:
                x = xs[src, p:p + 256].astype(jnp.float32)
                a_s[dst, p:p + 256] = (x * inv * gain[:, p:p + 256]).astype(jnp.bfloat16)
            return 0

        lax.fori_loop(0, ROWS // 16, norm, 0)

        @pl.when(st >= 1)
        def _():
            for j in range(n_dn - 2, n_dn):
                chip_sum(1 - par, j)

        s0, s1 = w_wait(w0), w_wait(w0 + 1)
        rope(dot(a_s[...], wbuf[s0]), 0, q_s, 0, rows)
        rope(dot(a_s[...], wbuf[s1]), 0, q_s, TILE, rows)
        s0, s1 = w_wait(w0 + 2), w_wait(w0 + 3)
        rope(dot(a_s[...], wbuf[s0]), 0, k_s, 0, rows)
        v_s[...] = dot(a_s[...], wbuf[s1]).astype(jnp.bfloat16).astype(jnp.float32)

        def block(b, _):
            gb = st * n_kv + b
            slot = lax.rem(gb, KV_SLOTS)
            for cp in kv_copies(gb):
                cp.wait()
            n_part = KV_TOK // 8
            ahead, outs = logits(slot, b, c, 0), []
            for g in range(n_part):
                now = ahead
                if g + 1 < n_part:
                    ahead = logits(slot, b, c, g + 1)
                outs.append(mix(slot, b, g, *now))
            t = pl.ds(pl.multiple_of(b * KV_TOK, KV_TOK), KV_TOK)
            for h in range(4):
                o = jnp.concatenate([part[h * 8:h * 8 + 8] for part in outs], 0)
                att_s[t, h * 256:(h + 1) * 256] = o.astype(jnp.bfloat16)

            @pl.when(gb + KV_SLOTS < all_kv)
            def _():
                for cp in kv_copies(gb + KV_SLOTS):
                    cp.start()

            @pl.when(b < n_q + 2)
            def _():
                w_next(w0 + b)

            return 0

        lax.fori_loop(0, n_kv, block, 0)

        def ff(i, _):
            gt = w0 + n_q + 2 + 2 * i
            s0, s1 = w_wait(gt), w_wait(gt + 1)
            swiglu(lax.rem(i + n_ff - 1, n_ff))
            graw[...] = dot(a_s[...], wbuf[s0]).astype(jnp.bfloat16)
            uraw[...] = dot(a_s[...], wbuf[s1]).astype(jnp.bfloat16)
            w_next(gt)
            w_next(gt + 1)
            return 0

        lax.fori_loop(0, n_ff, ff, 0)
        swiglu(n_ff - 1)

        @pl.when(st >= 1)
        def _():
            finish(1 - par)

        def down(j, _):
            gt = w0 + n_q + 2 + 2 * n_ff + j
            s0 = w_wait(gt)

            @pl.when(c == 0)
            def _():
                wo_copy(layer, j).wait()

            @pl.when(j >= 2)
            def _():
                chip_sum(par, j - 2)

            ybuf[j] = dot(u_s[...], wbuf[s0]) + dot(att_s[...], wobuf[j])
            chip_copy(par, j).start()
            w_next(gt)

            @pl.when((c == chunks - 1) & (layer < layers - 1))
            def _():
                wo_copy(layer + 1, j).start()

            return 0

        lax.fori_loop(0, n_dn, down, 0)
        return 0

    graw[...] = jnp.zeros_like(graw)
    uraw[...] = jnp.zeros_like(uraw)
    lax.fori_loop(0, stages, stage, 0)

    last = (stages - 1) % chunks
    for j in range(n_dn - 2, n_dn):
        chip_sum(last, j)
    new_wait(1 - last)
    out_copy(1 - last).start()
    finish(last)
    new_wait(last)
    out_copy(last).start()
    for c in range(chunks):
        out_copy(c).wait()


def solution(mesh):
    arg_specs = (P('dp', None), P('dp'), P(), P(None, None, 'tp'), P(None, None, 'tp'), P(None, None, 'tp'), P(None, 'tp', None), P(None, None, 'tp'), P(None, None, 'tp'), P(None, 'tp', None), P(None, 'dp', None, 'tp', None), P(None, 'dp', None, 'tp', None))

    def per_device(x_in, lengths, norm_gain, w_q, w_k, w_v, w_o, w_gate, w_up, w_down, k_cache, v_cache):
        layers, tokens, seq, kv_heads, head = k_cache.shape
        width = x_in.shape[1]
        half = head // 2
        inv_freq = 1.0 / (ROPE_BASE ** (jnp.arange(0, head, 2).astype(jnp.float32) / head))
        angles = lengths.astype(jnp.float32)[:, None] * inv_freq[None, :]
        cos, sin = jnp.cos(angles), jnp.sin(angles)

        def rows_of(cache):
            r = cache.reshape(layers * tokens * seq, kv_heads, 2, half).transpose(0, 2, 1, 3)
            return r.reshape(layers * tokens * seq * kv_heads * 2, half)

        tok_rows = seq * kv_heads * 2
        n_dn = width // TILE
        vm = pl.BlockSpec(memory_space=pltpu.VMEM)
        hbm = pl.BlockSpec(memory_space=pl.ANY)
        bf, f32 = jnp.bfloat16, jnp.float32
        dma = pltpu.SemaphoreType.DMA
        return pl.pallas_call(
            functools.partial(kernel, (layers, tokens, width, seq, kv_heads)),
            out_shape=jax.ShapeDtypeStruct(x_in.shape, bf),
            in_specs=[vm] * 4 + [hbm] * 10,
            out_specs=hbm,
            scratch_shapes=[
                pltpu.VMEM((tokens, width), bf),
                pltpu.VMEM((ROWS, width), bf),
                pltpu.VMEM((ROWS, w_q.shape[2]), f32),
                pltpu.VMEM((ROWS, w_k.shape[2]), f32),
                pltpu.VMEM((ROWS, w_v.shape[2]), f32),
                pltpu.VMEM((ROWS, w_q.shape[2]), bf),
                pltpu.VMEM((ROWS, w_gate.shape[2]), bf),
                pltpu.VMEM((ROWS, TILE), bf),
                pltpu.VMEM((ROWS, TILE), bf),
                pltpu.VMEM((32, 8 * tok_rows), jnp.int32),
                pltpu.VMEM((SLOTS, width, TILE), bf),
                pltpu.VMEM((n_dn, w_o.shape[1], TILE), bf),
                pltpu.VMEM((KV_SLOTS, KV_TOK * tok_rows, half), bf),
                pltpu.VMEM((KV_SLOTS, KV_TOK * tok_rows, half), bf),
                pltpu.VMEM((n_dn, ROWS, TILE), f32),
                pltpu.VMEM((2, n_dn, HALF, TILE), f32),
                pltpu.VMEM((n_dn, HALF, TILE), bf),
                pltpu.VMEM((2, n_dn, HALF, TILE), bf),
                dma((SLOTS,)), dma((n_dn,)), dma((2, KV_SLOTS)), dma((2,)),
                dma((n_dn,)), dma((2, n_dn)), dma((n_dn,)), dma((2, n_dn)), dma((2, n_dn)), dma((2, n_dn)), dma((2,)),
            ],
            compiler_params=pltpu.CompilerParams(
                collective_id=0, has_side_effects=True, vmem_limit_bytes=67_043_328),
            name="decoder",
        )(lengths[:, None], cos, sin, norm_gain, x_in, w_q, w_k, w_v, w_o, w_gate, w_up, w_down,
          rows_of(k_cache), rows_of(v_cache))

    return jax.shard_map(per_device, mesh=mesh, in_specs=arg_specs, out_specs=P('dp', None), check_vma=False)
```

```python
import functools

import jax
import jax.numpy as jnp
from jax import lax
from jax.experimental import pallas as pl
from jax.experimental.pallas import tpu as pltpu
from jax.sharding import PartitionSpec as P

NORM_EPS = 1e-5
ROPE_BASE = 500000.0
MESH = pl.DeviceIdType.MESH

ROWS = 256
HALF = 128
TILE = 512
SLOTS = 7
KV_SLOTS = 6
KV_TOK = 16


def kernel(cfg, lens_ref, cos_ref, sin_ref, gain_ref, x_in, wq, wk, wv, wo, wg, wu, wd, kc, vc, x_out,
           xs, a_s, q_s, k_s, v_s, att_s, u_s, raws, sidx, s_s, p_s, o_s, wbuf, wobuf, kbuf, vbuf, ybuf, irecv, rown, xrecv,
           wsem, wosem, kvsem, xsem, isend, irsem, xsend, xrsem, nsend, nrsem, osem):
    layers, tokens, width, seq, kv_heads = cfg
    tok_rows = seq * kv_heads * 2
    chunks = tokens // ROWS
    stages = layers * chunks
    n_dn = width // TILE
    n_ff = wg.shape[2] // TILE
    n_q = wq.shape[2] // TILE
    n_w = n_q + 2 + 2 * n_ff + n_dn
    n_kv = ROWS // KV_TOK
    all_w, all_kv = stages * n_w, stages * n_kv

    tp = lax.axis_index("tp")
    core = lax.rem(tp, 2)
    sib = tp + 1 - 2 * core
    partner = lax.rem(tp + 2, 4)
    own_row = pl.multiple_of(core * HALF, HALF)
    sib_row = pl.multiple_of((1 - core) * HALF, HALF)

    def w_start(gt):
        st = lax.div(gt, n_w)
        t = gt - st * n_w
        layer = lax.div(st, chunks)
        slot = lax.rem(gt, SLOTS)

        def put(src):
            pltpu.make_async_copy(src, wbuf.at[slot], wsem.at[slot]).start()

        def cols(i):
            return pl.ds(pl.multiple_of(i * TILE, TILE), TILE)

        f = t - (n_q + 2)

        @pl.when(t < n_q)
        def _():
            put(wq.at[layer, :, cols(t)])

        @pl.when(t == n_q)
        def _():
            put(wk.at[layer])

        @pl.when(t == n_q + 1)
        def _():
            put(wv.at[layer])

        @pl.when((f >= 0) & (f < 2 * n_ff) & (lax.rem(f + 2, 2) == 0))
        def _():
            put(wg.at[layer, :, cols(lax.div(f, 2))])

        @pl.when((f >= 0) & (f < 2 * n_ff) & (lax.rem(f + 2, 2) == 1))
        def _():
            put(wu.at[layer, :, cols(lax.div(f, 2))])

        @pl.when(f >= 2 * n_ff)
        def _():
            put(wd.at[layer, :, cols(f - 2 * n_ff)])

    def w_next(gt):
        @pl.when(gt + SLOTS < all_w)
        def _():
            w_start(gt + SLOTS)

    def w_wait(gt):
        slot = lax.rem(gt, SLOTS)
        pltpu.make_async_copy(wk.at[0], wbuf.at[slot], wsem.at[slot]).wait()
        return slot

    def wo_copy(layer, j):
        cols = pl.ds(pl.multiple_of(j * TILE, TILE), TILE)
        return pltpu.make_async_copy(wo.at[layer, :, cols], wobuf.at[j], wosem.at[j])

    def kv_copies(gb):
        st = lax.div(gb, n_kv)
        b = gb - st * n_kv
        layer = lax.div(st, chunks)
        tok = layer * tokens + (st - layer * chunks) * ROWS + b * KV_TOK
        slot = lax.rem(gb, KV_SLOTS)
        rows = pl.ds(pl.multiple_of(tok * tok_rows, KV_TOK * tok_rows), KV_TOK * tok_rows)
        return (pltpu.make_async_copy(kc.at[rows], kbuf.at[slot], kvsem.at[0, slot]),
                pltpu.make_async_copy(vc.at[rows], vbuf.at[slot], kvsem.at[1, slot]))

    def chip_copy(par, j):
        return pltpu.make_async_remote_copy(
            src_ref=ybuf.at[j, pl.ds(sib_row, HALF)], dst_ref=irecv.at[par, j], send_sem=isend.at[j],
            recv_sem=irsem.at[par, j], device_id={"tp": sib}, device_id_type=MESH)

    def link_copy(par, j):
        return pltpu.make_async_remote_copy(
            src_ref=rown.at[j], dst_ref=xrecv.at[par, j], send_sem=xsend.at[j],
            recv_sem=xrsem.at[par, j], device_id={"tp": partner}, device_id_type=MESH)

    def x_piece(par, row, j):
        return xs.at[pl.ds(pl.multiple_of(par * ROWS + row, HALF), HALF), pl.ds(pl.multiple_of(j * TILE, TILE), TILE)]

    def new_copy(par, j):
        piece = x_piece(par, own_row, j)
        return pltpu.make_async_remote_copy(
            src_ref=piece, dst_ref=piece, send_sem=nsend.at[par, j],
            recv_sem=nrsem.at[par, j], device_id={"tp": sib}, device_id_type=MESH)

    def chip_sum(par, j):
        chip_copy(par, j).wait_recv()
        rown[j] = (ybuf[j, pl.ds(own_row, HALF)] + irecv[par, j]).astype(jnp.bfloat16)
        link_copy(par, j).start()

    def finish(par):
        def step(j, _):
            link_copy(par, j).wait()
            chip_copy(par, j).wait_send()
            piece = x_piece(par, own_row, j)
            total = rown[j].astype(jnp.float32) + xrecv[par, j].astype(jnp.float32)
            piece[...] = (piece[...].astype(jnp.float32) + total).astype(jnp.bfloat16)
            new_copy(par, j).start()
            return 0

        lax.fori_loop(0, n_dn, step, 0)

    def new_wait(par):
        def step(j, _):
            new_copy(par, j).wait()
            return 0

        lax.fori_loop(0, n_dn, step, 0)

    def x_copy(c):
        rows = pl.ds(pl.multiple_of(c * ROWS, ROWS), ROWS)
        return pltpu.make_async_copy(x_in.at[rows], xs.at[rows], xsem.at[c])

    def out_copy(c):
        rows = pl.ds(c * ROWS, ROWS)
        return pltpu.make_async_copy(xs.at[rows], x_out.at[rows], osem.at[c])

    for c in range(chunks):
        x_copy(c).start()
    for g in range(SLOTS):
        w_start(jnp.int32(g))
    for g in range(KV_SLOTS):
        for cp in kv_copies(jnp.int32(g)):
            cp.start()
    for j in range(n_dn):
        wo_copy(0, j).start()

    barrier = pltpu.get_barrier_semaphore()
    for other in (sib, partner):
        pl.semaphore_signal(barrier, inc=1, device_id={"tp": other}, device_id_type=MESH)
    pl.semaphore_wait(barrier, 2)

    n_key = 8 * tok_rows
    lane = lax.broadcasted_iota(jnp.int32, (32, n_key), 1)
    row = lax.broadcasted_iota(jnp.int32, (32, n_key), 0)
    per = 2 * kv_heads
    match = (lax.div(lane, tok_rows) == lax.rem(row, 8)) & (lax.rem(lane, kv_heads) == lax.div(row, 16)) & (lax.rem(lane, per) < kv_heads)
    sidx[...] = jnp.where(match, lax.rem(lax.div(lane, per), seq), 2 * seq)

    def rope(y, dst, col, rows):
        cos, sin = cos_ref[rows], sin_ref[rows]
        for h in range(TILE // 256):
            first = y[:, h * 256:h * 256 + 128].astype(jnp.float32)
            second = y[:, h * 256 + 128:h * 256 + 256].astype(jnp.float32)
            at = col + h * 256
            dst[:, at:at + 128] = (first * cos - second * sin).astype(jnp.bfloat16).astype(jnp.float32)
            dst[:, at + 128:at + 256] = (second * cos + first * sin).astype(jnp.bfloat16).astype(jnp.float32)

    def dot(a, b):
        return jnp.dot(a, b, preferred_element_type=jnp.float32)

    scale = 1.0 / 16.0

    def roll(x, by):
        return jnp.concatenate([pltpu.roll(x[:, i:i + 128], by % 128, axis=1) for i in range(0, n_key, 128)], 1)

    n_part = KV_TOK // 8

    def spread(x8, group):
        return jnp.concatenate([x8[:, (h // group) * 256:(h // group + 1) * 256] for h in range(4)], 0)

    def logits(side, st, b):
        slot = lax.rem(st * n_kv + b, KV_SLOTS)
        for g in range(n_part):
            q = spread(q_s[pl.ds(pl.multiple_of(b * KV_TOK + g * 8, 8), 8)], 1) * scale
            qq = jnp.concatenate([q[:, :128], q[:, 128:]], 0).astype(jnp.bfloat16)
            keys = kbuf[slot, pl.ds(g * n_key, n_key)]
            s2 = lax.dot_general(qq, keys, (((1,), (1,)), ((), ())), preferred_element_type=jnp.float32)
            s_s[side][g] = s2

    def soft(side, c, b):
        for g in range(n_part):
            base = pl.multiple_of(b * KV_TOK + g * 8, 8)
            tok = pl.ds(base, 8)
            self_logit = jnp.sum(spread(q_s[tok], 1) * scale * spread(k_s[tok], 2), axis=-1, keepdims=True)
            lens = jnp.concatenate([lens_ref[pl.ds(pl.multiple_of(c * ROWS + base, 8), 8), :]] * 4, 0)
            s = jnp.where(sidx[...] < lens, s_s[side][g, :32] + roll(s_s[side][g, 32:], -2), -jnp.inf)
            peak = jnp.maximum(jnp.max(s, axis=-1, keepdims=True), self_logit)
            w = jnp.exp(s - peak)
            sw = jnp.exp(self_logit - peak)
            inv = 1.0 / (jnp.sum(w, axis=-1, keepdims=True) + sw)
            p = w * inv
            p_s[side][g, :32] = p.astype(jnp.bfloat16)
            p_s[side][g, 32:] = roll(p, 2).astype(jnp.bfloat16)
            o_s[side][g] = (sw * inv).astype(jnp.bfloat16).astype(jnp.float32) * spread(v_s[tok], 2)

    def mix(side, st, b):
        slot = lax.rem(st * n_kv + b, KV_SLOTS)
        outs = []
        for g in range(n_part):
            o2 = dot(p_s[side][g], vbuf[slot, pl.ds(g * n_key, n_key)])
            outs.append(jnp.concatenate([o2[:32], o2[32:]], 1) + o_s[side][g])
        t = pl.ds(pl.multiple_of(b * KV_TOK, KV_TOK), KV_TOK)
        for h in range(4):
            o = jnp.concatenate([part[h * 8:h * 8 + 8] for part in outs], 0)
            att_s[t, h * 256:(h + 1) * 256] = o.astype(jnp.bfloat16)

    def k_next(gb):
        @pl.when(gb + KV_SLOTS < all_kv)
        def _():
            kv_copies(gb + KV_SLOTS)[0].start()

    def v_next(gb):
        @pl.when(gb + KV_SLOTS < all_kv)
        def _():
            kv_copies(gb + KV_SLOTS)[1].start()

    def swiglu(side, i):
        g = raws[2 * side][...].astype(jnp.float32)
        u = raws[2 * side + 1][...].astype(jnp.float32)
        u_s[:, pl.ds(pl.multiple_of(i * TILE, TILE), TILE)] = (g * (1.0 / (1.0 + jnp.exp(-g))) * u).astype(jnp.bfloat16)

    def stage(st, _):
        layer = lax.div(st, chunks)
        c = st - layer * chunks
        par = c
        rows = pl.ds(pl.multiple_of(c * ROWS, ROWS), ROWS)
        w0 = st * n_w

        @pl.when(st < chunks)
        def _():
            x_copy(c).wait()

        @pl.when(st >= chunks)
        def _():
            new_wait(par)

        gains = gain_ref[...].astype(jnp.float32)
        gain = gains[:1]
        for other in range(1, layers):
            gain = jnp.where(layer == other, gains[other:other + 1], gain)

        def norm_rows(i):
            src = pl.ds(pl.multiple_of(c * ROWS + i * 16, 16), 16)
            dst = pl.ds(pl.multiple_of(i * 16, 16), 16)
            parts = range(0, width, 256)
            total = jnp.zeros((16, 256), jnp.float32)
            for p in parts:
                x = xs[src, p:p + 256].astype(jnp.float32)
                total = total + x * x
            inv = lax.rsqrt(jnp.sum(total, axis=-1, keepdims=True) / width + NORM_EPS)
            for p in parts:
                x = xs[src, p:p + 256].astype(jnp.float32)
                a_s[dst, p:p + 256] = (x * inv * gain[:, p:p + 256]).astype(jnp.bfloat16)

        def norm(i, _):
            norm_rows(2 * i)
            norm_rows(2 * i + 1)
            return 0

        lax.fori_loop(0, ROWS // 32, norm, 0)

        @pl.when(st >= 1)
        def _():
            for j in range(n_dn - 2, n_dn):
                chip_sum(1 - par, j)

        slots = [w_wait(w0), w_wait(w0 + 1)]
        for i in range(2):
            raws[i][...] = dot(a_s[...], wbuf[slots[i]]).astype(jnp.bfloat16)
        w_next(w0)
        w_next(w0 + 1)
        slots = [w_wait(w0 + 2), w_wait(w0 + 3)]
        raws[2][...] = dot(a_s[...], wbuf[slots[0]]).astype(jnp.bfloat16)
        rope(raws[0], q_s, 0, rows)
        rope(raws[1], q_s, TILE, rows)
        v_s[...] = dot(a_s[...], wbuf[slots[1]]).astype(jnp.bfloat16).astype(jnp.float32)
        rope(raws[2], k_s, 0, rows)

        b0 = st * n_kv
        kv_copies(b0)[0].wait()
        logits(0, st, 0)
        k_next(b0)
        kv_copies(b0 + 1)[0].wait()
        soft(0, c, 0)
        logits(1, st, 1)
        k_next(b0 + 1)

        def half(side, b):
            kv_copies(b0 + b - 1)[1].wait()
            kv_copies(b0 + b + 1)[0].wait()
            mix(1 - side, st, b - 1)
            soft(side, c, b)
            logits(1 - side, st, b + 1)
            v_next(b0 + b - 1)
            k_next(b0 + b + 1)

        def block(i, _):
            half(1, 2 * i + 1)

            @pl.when((i == 0) | (i == 2))
            def _():
                w_next(w0 + n_q + lax.div(i, 2))

            half(0, 2 * i + 2)
            return 0

        lax.fori_loop(0, n_kv // 2 - 1, block, 0)
        kv_copies(b0 + n_kv - 2)[1].wait()
        mix(0, st, n_kv - 2)
        soft(1, c, n_kv - 1)
        v_next(b0 + n_kv - 2)
        kv_copies(b0 + n_kv - 1)[1].wait()
        mix(1, st, n_kv - 1)
        v_next(b0 + n_kv - 1)

        def ff_tile(side, i):
            gt = w0 + n_q + 2 + 2 * i
            s0, s1 = w_wait(gt), w_wait(gt + 1)
            swiglu(1 - side, lax.rem(i + n_ff - 1, n_ff))
            raws[2 * side][...] = dot(a_s[...], wbuf[s0]).astype(jnp.bfloat16)
            raws[2 * side + 1][...] = dot(a_s[...], wbuf[s1]).astype(jnp.bfloat16)
            w_next(gt)
            w_next(gt + 1)

        def ff(i, _):
            ff_tile(0, 2 * i)
            ff_tile(1, 2 * i + 1)
            return 0

        lax.fori_loop(0, n_ff // 2, ff, 0)
        if n_ff % 2:
            ff_tile(0, n_ff - 1)
        swiglu((n_ff - 1) % 2, n_ff - 1)

        @pl.when(st >= 1)
        def _():
            finish(1 - par)

        def down(j, _):
            gt = w0 + n_q + 2 + 2 * n_ff + j
            s0 = w_wait(gt)

            @pl.when(c == 0)
            def _():
                wo_copy(layer, j).wait()

            @pl.when(j >= 2)
            def _():
                chip_sum(par, j - 2)

            ybuf[j] = dot(u_s[...], wbuf[s0]) + dot(att_s[...], wobuf[j])
            chip_copy(par, j).start()
            w_next(gt)

            @pl.when((c == chunks - 1) & (layer < layers - 1))
            def _():
                wo_copy(layer + 1, j).start()

            return 0

        lax.fori_loop(0, n_dn, down, 0)
        return 0

    for raw in raws:
        raw[...] = jnp.zeros_like(raw)
    lax.fori_loop(0, stages, stage, 0)

    last = (stages - 1) % chunks
    for j in range(n_dn - 2, n_dn):
        chip_sum(last, j)
    new_wait(1 - last)
    out_copy(1 - last).start()
    finish(last)
    new_wait(last)
    out_copy(last).start()
    for c in range(chunks):
        out_copy(c).wait()


def solution(mesh):
    arg_specs = (P('dp', None), P('dp'), P(), P(None, None, 'tp'), P(None, None, 'tp'), P(None, None, 'tp'), P(None, 'tp', None), P(None, None, 'tp'), P(None, None, 'tp'), P(None, 'tp', None), P(None, 'dp', None, 'tp', None), P(None, 'dp', None, 'tp', None))

    def per_device(x_in, lengths, norm_gain, w_q, w_k, w_v, w_o, w_gate, w_up, w_down, k_cache, v_cache):
        layers, tokens, seq, kv_heads, head = k_cache.shape
        width = x_in.shape[1]
        half = head // 2
        inv_freq = 1.0 / (ROPE_BASE ** (jnp.arange(0, head, 2).astype(jnp.float32) / head))
        angles = lengths.astype(jnp.float32)[:, None] * inv_freq[None, :]
        cos, sin = jnp.cos(angles), jnp.sin(angles)

        def rows_of(cache):
            r = cache.reshape(layers * tokens * seq, kv_heads, 2, half).transpose(0, 2, 1, 3)
            return r.reshape(layers * tokens * seq * kv_heads * 2, half)

        tok_rows = seq * kv_heads * 2
        n_dn = width // TILE
        vm = pl.BlockSpec(memory_space=pltpu.VMEM)
        hbm = pl.BlockSpec(memory_space=pl.ANY)
        bf, f32 = jnp.bfloat16, jnp.float32
        dma = pltpu.SemaphoreType.DMA
        return pl.pallas_call(
            functools.partial(kernel, (layers, tokens, width, seq, kv_heads)),
            out_shape=jax.ShapeDtypeStruct(x_in.shape, bf),
            in_specs=[vm] * 4 + [hbm] * 10,
            out_specs=hbm,
            scratch_shapes=[
                pltpu.VMEM((tokens, width), bf),
                pltpu.VMEM((ROWS, width), bf),
                pltpu.VMEM((ROWS, w_q.shape[2]), f32),
                pltpu.VMEM((ROWS, w_k.shape[2]), f32),
                pltpu.VMEM((ROWS, w_v.shape[2]), f32),
                pltpu.VMEM((ROWS, w_q.shape[2]), bf),
                pltpu.VMEM((ROWS, w_gate.shape[2]), bf),
                [pltpu.VMEM((ROWS, TILE), bf)] * 4,
                pltpu.VMEM((32, 8 * tok_rows), jnp.int32),
                [pltpu.VMEM((KV_TOK // 8, 64, 8 * tok_rows), f32)] * 2,
                [pltpu.VMEM((KV_TOK // 8, 64, 8 * tok_rows), bf)] * 2,
                [pltpu.VMEM((KV_TOK // 8, 32, head), f32)] * 2,
                pltpu.VMEM((SLOTS, width, TILE), bf),
                pltpu.VMEM((n_dn, w_o.shape[1], TILE), bf),
                pltpu.VMEM((KV_SLOTS, KV_TOK * tok_rows, half), bf),
                pltpu.VMEM((KV_SLOTS, KV_TOK * tok_rows, half), bf),
                pltpu.VMEM((n_dn, ROWS, TILE), f32),
                pltpu.VMEM((2, n_dn, HALF, TILE), f32),
                pltpu.VMEM((n_dn, HALF, TILE), bf),
                pltpu.VMEM((2, n_dn, HALF, TILE), bf),
                dma((SLOTS,)), dma((n_dn,)), dma((2, KV_SLOTS)), dma((2,)),
                dma((n_dn,)), dma((2, n_dn)), dma((n_dn,)), dma((2, n_dn)), dma((2, n_dn)), dma((2, n_dn)), dma((2,)),
            ],
            compiler_params=pltpu.CompilerParams(
                collective_id=0, has_side_effects=True, vmem_limit_bytes=67_043_328),
            name="decoder",
        )(lengths[:, None], cos, sin, norm_gain, x_in, w_q, w_k, w_v, w_o, w_gate, w_up, w_down,
          rows_of(k_cache), rows_of(v_cache))

    return jax.shard_map(per_device, mesh=mesh, in_specs=arg_specs, out_specs=P('dp', None), check_vma=False)
```

```python
import functools

import jax
import jax.numpy as jnp
import numpy as np
from jax import lax
from jax.experimental import pallas as pl
from jax.experimental.pallas import tpu as pltpu
from jax.sharding import PartitionSpec as P

NORM_EPS = 1e-5
ROPE_BASE = 500000.0
MESH = pl.DeviceIdType.MESH

ROWS = 256
HALF = 128
TILE = 512
SLOTS = 7
KV_SLOTS = 9
X_SLOTS = 4
KV_TOK = 16


def kernel(cfg, lens_ref, table_ref, gain_ref, x_in, wq, wk, wv, wo, wg, wu, wd, kc, vc, x_out,
           xs, a_s, q_s, k_s, v_s, att_s, u_s, raws, cos_ref, sin_ref, len_s, sidx, s_s, p_s, o_s, wbuf, wobuf, kbuf, vbuf, ybuf, irecv, rown, xrecv,
           wsem, wosem, kvsem, xsem, isend, irsem, xsend, xrsem, nsend, nrsem, osem):
    layers, tokens, width, seq, kv_heads = cfg
    tok_rows = seq * kv_heads * 2
    chunks = tokens // ROWS
    stages = layers * chunks
    n_dn = width // TILE
    n_ff = wg.shape[2] // TILE
    n_q = wq.shape[2] // TILE
    n_w = n_q + 2 + 2 * n_ff + n_dn
    n_kv = ROWS // KV_TOK
    all_w, all_kv = stages * n_w, stages * n_kv

    tp = lax.axis_index("tp")
    core = lax.rem(tp, 2)
    sib = tp + 1 - 2 * core
    partner = lax.rem(tp + 2, 4)
    own_row = pl.multiple_of(core * HALF, HALF)
    sib_row = pl.multiple_of((1 - core) * HALF, HALF)

    def w_start(gt):
        st = lax.div(gt, n_w)
        t = gt - st * n_w
        layer = lax.div(st, chunks)
        slot = lax.rem(gt, SLOTS)

        def put(src):
            pltpu.make_async_copy(src, wbuf.at[slot], wsem.at[slot]).start()

        def cols(i):
            return pl.ds(pl.multiple_of(i * TILE, TILE), TILE)

        f = t - (n_q + 2)

        @pl.when(t < n_q)
        def _():
            put(wq.at[layer, :, cols(t)])

        @pl.when(t == n_q)
        def _():
            put(wk.at[layer])

        @pl.when(t == n_q + 1)
        def _():
            put(wv.at[layer])

        @pl.when((f >= 0) & (f < 2 * n_ff) & (lax.rem(f + 2, 2) == 0))
        def _():
            put(wg.at[layer, :, cols(lax.div(f, 2))])

        @pl.when((f >= 0) & (f < 2 * n_ff) & (lax.rem(f + 2, 2) == 1))
        def _():
            put(wu.at[layer, :, cols(lax.div(f, 2))])

        @pl.when(f >= 2 * n_ff)
        def _():
            put(wd.at[layer, :, cols(f - 2 * n_ff)])

    def w_next(gt):
        @pl.when(gt + SLOTS < all_w)
        def _():
            w_start(gt + SLOTS)

    def w_wait(gt):
        slot = lax.rem(gt, SLOTS)
        pltpu.make_async_copy(wk.at[0], wbuf.at[slot], wsem.at[slot]).wait()
        return slot

    def wo_copy(layer, j):
        cols = pl.ds(pl.multiple_of(j * TILE, TILE), TILE)
        return pltpu.make_async_copy(wo.at[layer, :, cols], wobuf.at[j], wosem.at[j])

    def kv_copies(gb):
        st = lax.div(gb, n_kv)
        b = gb - st * n_kv
        layer = lax.div(st, chunks)
        tok = layer * tokens + (st - layer * chunks) * ROWS + b * KV_TOK
        slot = lax.rem(gb, KV_SLOTS)
        rows = pl.ds(pl.multiple_of(tok * tok_rows, KV_TOK * tok_rows), KV_TOK * tok_rows)
        return (pltpu.make_async_copy(kc.at[rows], kbuf.at[slot], kvsem.at[0, slot]),
                pltpu.make_async_copy(vc.at[rows], vbuf.at[slot], kvsem.at[1, slot]))

    def chip_copy(gj):
        slot = lax.rem(gj, X_SLOTS)
        return pltpu.make_async_remote_copy(
            src_ref=ybuf.at[slot, pl.ds(sib_row, HALF)], dst_ref=irecv.at[slot], send_sem=isend.at[slot],
            recv_sem=irsem.at[slot], device_id={"tp": sib}, device_id_type=MESH)

    def link_copy(par, j):
        return pltpu.make_async_remote_copy(
            src_ref=rown.at[j], dst_ref=xrecv.at[par, j], send_sem=xsend.at[j],
            recv_sem=xrsem.at[par, j], device_id={"tp": partner}, device_id_type=MESH)

    def x_piece(par, row, j):
        return xs.at[pl.ds(pl.multiple_of(par * ROWS + row, HALF), HALF), pl.ds(pl.multiple_of(j * TILE, TILE), TILE)]

    def new_copy(par, j):
        piece = x_piece(par, own_row, j)
        return pltpu.make_async_remote_copy(
            src_ref=piece, dst_ref=piece, send_sem=nsend.at[par, j],
            recv_sem=nrsem.at[par, j], device_id={"tp": sib}, device_id_type=MESH)

    def chip_sum(st, j):
        gj = st * n_dn + j
        slot = lax.rem(gj, X_SLOTS)
        chip_copy(gj).wait()
        rown[j] = (ybuf[slot, pl.ds(own_row, HALF)] + irecv[slot]).astype(jnp.bfloat16)
        link_copy(lax.rem(st, chunks), j).start()

    def finish(par):
        def step(j, _):
            link_copy(par, j).wait()
            piece = x_piece(par, own_row, j)
            total = rown[j].astype(jnp.float32) + xrecv[par, j].astype(jnp.float32)
            piece[...] = (piece[...].astype(jnp.float32) + total).astype(jnp.bfloat16)
            new_copy(par, j).start()
            return 0

        lax.fori_loop(0, n_dn, step, 0)

    def new_wait(par):
        def step(j, _):
            new_copy(par, j).wait()
            return 0

        lax.fori_loop(0, n_dn, step, 0)

    def x_copy(c):
        rows = pl.ds(pl.multiple_of(c * ROWS, ROWS), ROWS)
        return pltpu.make_async_copy(x_in.at[rows], xs.at[rows], xsem.at[c])

    def out_copy(c):
        rows = pl.ds(c * ROWS, ROWS)
        return pltpu.make_async_copy(xs.at[rows], x_out.at[rows], osem.at[c])

    x_copy(0).start()
    for g in range(SLOTS):
        w_start(jnp.int32(g))
    for g in range(KV_SLOTS):
        for cp in kv_copies(jnp.int32(g)):
            cp.start()
    for j in range(n_dn):
        wo_copy(0, j).start()
    for c in range(1, chunks):
        x_copy(c).start()

    barrier = pltpu.get_barrier_semaphore()
    for other in (sib, partner):
        pl.semaphore_signal(barrier, inc=1, device_id={"tp": other}, device_id_type=MESH)
    pl.semaphore_wait(barrier, 2)

    n_key = 8 * tok_rows
    lane = lax.broadcasted_iota(jnp.int32, (32, n_key), 1)
    row = lax.broadcasted_iota(jnp.int32, (32, n_key), 0)
    per = 2 * kv_heads
    match = (lax.div(lane, tok_rows) == lax.rem(row, 8)) & (lax.rem(lane, kv_heads) == lax.div(row, 16)) & (lax.rem(lane, per) < kv_heads)
    sidx[...] = jnp.where(match, lax.rem(lax.div(lane, per), seq), 2 * seq).astype(jnp.float32)
    pick = lax.broadcasted_iota(jnp.int32, (seq, tokens), 0) == lens_ref[...]
    angles = lax.dot_general(pick.astype(jnp.float32), table_ref[...], (((0,), (0,)), ((), ())),
                             precision=lax.Precision.HIGHEST, preferred_element_type=jnp.float32)
    half = angles.shape[1] // 3
    cos_ref[...], sin_ref[...], len_s[...] = angles[:, :half], angles[:, half:2 * half], angles[:, 2 * half:]

    def rope(y, dst, col, rows):
        cos, sin = cos_ref[rows], sin_ref[rows]
        for h in range(TILE // 256):
            first = y[:, h * 256:h * 256 + 128].astype(jnp.float32)
            second = y[:, h * 256 + 128:h * 256 + 256].astype(jnp.float32)
            at = col + h * 256
            dst[:, at:at + 128] = (first * cos - second * sin).astype(jnp.bfloat16).astype(jnp.float32)
            dst[:, at + 128:at + 256] = (second * cos + first * sin).astype(jnp.bfloat16).astype(jnp.float32)

    def dot(a, b):
        return jnp.dot(a, b, preferred_element_type=jnp.float32)

    scale = 1.0 / 16.0

    def roll(x, by):
        return jnp.concatenate([pltpu.roll(x[:, i:i + 128], by % 128, axis=1) for i in range(0, n_key, 128)], 1)

    n_part = KV_TOK // 8

    def spread(x8, group):
        return jnp.concatenate([x8[:, (h // group) * 256:(h // group + 1) * 256] for h in range(4)], 0)

    def logits(side, st, b):
        slot = lax.rem(st * n_kv + b, KV_SLOTS)
        for g in range(n_part):
            q = spread(q_s[pl.ds(pl.multiple_of(b * KV_TOK + g * 8, 8), 8)], 1) * scale
            qq = jnp.concatenate([q[:, :128], q[:, 128:]], 0).astype(jnp.bfloat16)
            keys = kbuf[slot, pl.ds(g * n_key, n_key)]
            s2 = lax.dot_general(qq, keys, (((1,), (1,)), ((), ())), preferred_element_type=jnp.float32)
            s_s[side][g] = s2

    def soft(side, c, b):
        for g in range(n_part):
            base = pl.multiple_of(b * KV_TOK + g * 8, 8)
            tok = pl.ds(base, 8)
            self_logit = jnp.sum(spread(q_s[tok], 1) * scale * spread(k_s[tok], 2), axis=-1, keepdims=True)
            lens = jnp.concatenate([len_s[pl.ds(pl.multiple_of(c * ROWS + base, 8), 8), :1]] * 4, 0)
            s = jnp.where(sidx[...] < lens, s_s[side][g, :32] + roll(s_s[side][g, 32:], -2), -jnp.inf)
            peak = jnp.maximum(jnp.max(s, axis=-1, keepdims=True), self_logit)
            w = jnp.exp(s - peak)
            sw = jnp.exp(self_logit - peak)
            inv = 1.0 / (jnp.sum(w, axis=-1, keepdims=True) + sw)
            p = w * inv
            p_s[side][g, :32] = p.astype(jnp.bfloat16)
            p_s[side][g, 32:] = roll(p, 2).astype(jnp.bfloat16)
            o_s[side][g] = (sw * inv).astype(jnp.bfloat16).astype(jnp.float32) * spread(v_s[tok], 2)

    def mix(side, st, b):
        slot = lax.rem(st * n_kv + b, KV_SLOTS)
        outs = []
        for g in range(n_part):
            o2 = dot(p_s[side][g], vbuf[slot, pl.ds(g * n_key, n_key)])
            outs.append(jnp.concatenate([o2[:32], o2[32:]], 1) + o_s[side][g])
        t = pl.ds(pl.multiple_of(b * KV_TOK, KV_TOK), KV_TOK)
        for h in range(4):
            o = jnp.concatenate([part[h * 8:h * 8 + 8] for part in outs], 0)
            att_s[t, h * 256:(h + 1) * 256] = o.astype(jnp.bfloat16)

    def k_next(gb):
        @pl.when(gb + KV_SLOTS < all_kv)
        def _():
            kv_copies(gb + KV_SLOTS)[0].start()

    def v_next(gb):
        @pl.when(gb + KV_SLOTS < all_kv)
        def _():
            kv_copies(gb + KV_SLOTS)[1].start()

    def swiglu(side, i):
        g = raws[2 * side][...].astype(jnp.float32)
        u = raws[2 * side + 1][...].astype(jnp.float32)
        u_s[:, pl.ds(pl.multiple_of(i * TILE, TILE), TILE)] = (g * (1.0 / (1.0 + jnp.exp(-g))) * u).astype(jnp.bfloat16)

    def stage(st, _):
        layer = lax.div(st, chunks)
        c = st - layer * chunks
        par = c
        rows = pl.ds(pl.multiple_of(c * ROWS, ROWS), ROWS)
        w0 = st * n_w

        @pl.when(st < chunks)
        def _():
            x_copy(c).wait()

        @pl.when(st >= chunks)
        def _():
            new_wait(par)

        gains = gain_ref[...].astype(jnp.float32)
        gain = gains[:1]
        for other in range(1, layers):
            gain = jnp.where(layer == other, gains[other:other + 1], gain)

        def norm_rows(i):
            src = pl.ds(pl.multiple_of(c * ROWS + i * 16, 16), 16)
            dst = pl.ds(pl.multiple_of(i * 16, 16), 16)
            parts = range(0, width, 256)
            total = jnp.zeros((16, 256), jnp.float32)
            for p in parts:
                x = xs[src, p:p + 256].astype(jnp.float32)
                total = total + x * x
            inv = lax.rsqrt(jnp.sum(total, axis=-1, keepdims=True) / width + NORM_EPS)
            for p in parts:
                x = xs[src, p:p + 256].astype(jnp.float32)
                a_s[dst, p:p + 256] = (x * inv * gain[:, p:p + 256]).astype(jnp.bfloat16)

        def norm(i, _):
            norm_rows(2 * i)
            norm_rows(2 * i + 1)
            return 0

        lax.fori_loop(0, ROWS // 32, norm, 0)

        @pl.when(st >= 1)
        def _():
            for j in range(n_dn - 2, n_dn):
                chip_sum(st - 1, j)

        slots = [w_wait(w0), w_wait(w0 + 1)]
        for i in range(2):
            raws[i][...] = dot(a_s[...], wbuf[slots[i]]).astype(jnp.bfloat16)
        w_next(w0)
        w_next(w0 + 1)
        slots = [w_wait(w0 + 2), w_wait(w0 + 3)]
        raws[2][...] = dot(a_s[...], wbuf[slots[0]]).astype(jnp.bfloat16)
        rope(raws[0], q_s, 0, rows)
        rope(raws[1], q_s, TILE, rows)
        v_s[...] = dot(a_s[...], wbuf[slots[1]]).astype(jnp.bfloat16).astype(jnp.float32)
        rope(raws[2], k_s, 0, rows)

        b0 = st * n_kv
        kv_copies(b0)[0].wait()
        logits(0, st, 0)
        k_next(b0)
        kv_copies(b0 + 1)[0].wait()
        soft(0, c, 0)
        logits(1, st, 1)
        k_next(b0 + 1)

        def half(side, b):
            kv_copies(b0 + b - 1)[1].wait()
            kv_copies(b0 + b + 1)[0].wait()
            mix(1 - side, st, b - 1)
            soft(side, c, b)
            logits(1 - side, st, b + 1)
            v_next(b0 + b - 1)
            k_next(b0 + b + 1)

        def block(i, _):
            half(1, 2 * i + 1)

            @pl.when((i == 0) | (i == 2))
            def _():
                w_next(w0 + n_q + lax.div(i, 2))

            half(0, 2 * i + 2)
            return 0

        lax.fori_loop(0, n_kv // 2 - 1, block, 0)
        kv_copies(b0 + n_kv - 2)[1].wait()
        mix(0, st, n_kv - 2)
        soft(1, c, n_kv - 1)
        v_next(b0 + n_kv - 2)
        kv_copies(b0 + n_kv - 1)[1].wait()
        mix(1, st, n_kv - 1)
        v_next(b0 + n_kv - 1)

        def ff_tile(side, i):
            gt = w0 + n_q + 2 + 2 * i
            s0, s1 = w_wait(gt), w_wait(gt + 1)
            swiglu(1 - side, lax.rem(i + n_ff - 1, n_ff))
            raws[2 * side][...] = dot(a_s[...], wbuf[s0]).astype(jnp.bfloat16)
            raws[2 * side + 1][...] = dot(a_s[...], wbuf[s1]).astype(jnp.bfloat16)
            w_next(gt)
            w_next(gt + 1)

        def ff(i, _):
            ff_tile(0, 2 * i)
            ff_tile(1, 2 * i + 1)
            return 0

        lax.fori_loop(0, n_ff // 2, ff, 0)
        if n_ff % 2:
            ff_tile(0, n_ff - 1)
        swiglu((n_ff - 1) % 2, n_ff - 1)

        @pl.when(st >= 1)
        def _():
            finish(1 - par)

        def down(j, _):
            gt = w0 + n_q + 2 + 2 * n_ff + j
            s0 = w_wait(gt)

            @pl.when(c == 0)
            def _():
                wo_copy(layer, j).wait()

            @pl.when(j >= 2)
            def _():
                chip_sum(st, j - 2)

            gj = st * n_dn + j
            ybuf[lax.rem(gj, X_SLOTS)] = dot(u_s[...], wbuf[s0]) + dot(att_s[...], wobuf[j])
            chip_copy(gj).start()
            w_next(gt)

            @pl.when((c == chunks - 1) & (layer < layers - 1))
            def _():
                wo_copy(layer + 1, j).start()

            return 0

        lax.fori_loop(0, n_dn, down, 0)
        return 0

    for raw in raws:
        raw[...] = jnp.zeros_like(raw)
    lax.fori_loop(0, stages, stage, 0)

    last = (stages - 1) % chunks
    for j in range(n_dn - 2, n_dn):
        chip_sum(stages - 1, j)
    new_wait(1 - last)
    out_copy(1 - last).start()
    finish(last)
    new_wait(last)
    out_copy(last).start()
    for c in range(chunks):
        out_copy(c).wait()


def solution(mesh):
    arg_specs = (P('dp', None), P('dp'), P(), P(None, None, 'tp'), P(None, None, 'tp'), P(None, None, 'tp'), P(None, 'tp', None), P(None, None, 'tp'), P(None, None, 'tp'), P(None, 'tp', None), P(None, 'dp', None, 'tp', None), P(None, 'dp', None, 'tp', None))

    def per_device(x_in, lengths, norm_gain, w_q, w_k, w_v, w_o, w_gate, w_up, w_down, k_cache, v_cache):
        layers, tokens, seq, kv_heads, head = k_cache.shape
        width = x_in.shape[1]
        half = head // 2
        inv_freq = 1.0 / (np.float32(ROPE_BASE) ** (np.arange(0, head, 2).astype(np.float32) / np.float32(head)))
        pos = np.arange(seq).astype(np.float32)[:, None]
        angles = pos * inv_freq[None, :].astype(np.float32)
        table = np.concatenate([np.cos(angles), np.sin(angles), pos + 0 * angles], 1).astype(np.float32)

        def rows_of(cache):
            r = cache.reshape(layers * tokens * seq, kv_heads, 2, half).transpose(0, 2, 1, 3)
            return r.reshape(layers * tokens * seq * kv_heads * 2, half)

        tok_rows = seq * kv_heads * 2
        n_dn = width // TILE
        vm = pl.BlockSpec(memory_space=pltpu.VMEM)
        hbm = pl.BlockSpec(memory_space=pl.ANY)
        bf, f32 = jnp.bfloat16, jnp.float32
        dma = pltpu.SemaphoreType.DMA
        return pl.pallas_call(
            functools.partial(kernel, (layers, tokens, width, seq, kv_heads)),
            out_shape=jax.ShapeDtypeStruct(x_in.shape, bf),
            in_specs=[vm] * 3 + [hbm] * 10,
            out_specs=hbm,
            scratch_shapes=[
                pltpu.VMEM((tokens, width), bf),
                pltpu.VMEM((ROWS, width), bf),
                pltpu.VMEM((ROWS, w_q.shape[2]), f32),
                pltpu.VMEM((ROWS, w_k.shape[2]), f32),
                pltpu.VMEM((ROWS, w_v.shape[2]), f32),
                pltpu.VMEM((ROWS, w_q.shape[2]), bf),
                pltpu.VMEM((ROWS, w_gate.shape[2]), bf),
                [pltpu.VMEM((ROWS, TILE), bf)] * 4,
                pltpu.VMEM((tokens, half), f32),
                pltpu.VMEM((tokens, half), f32),
                pltpu.VMEM((tokens, half), f32),
                pltpu.VMEM((32, 8 * tok_rows), f32),
                [pltpu.VMEM((KV_TOK // 8, 64, 8 * tok_rows), f32)] * 2,
                [pltpu.VMEM((KV_TOK // 8, 64, 8 * tok_rows), bf)] * 2,
                [pltpu.VMEM((KV_TOK // 8, 32, head), f32)] * 2,
                pltpu.VMEM((SLOTS, width, TILE), bf),
                pltpu.VMEM((n_dn, w_o.shape[1], TILE), bf),
                pltpu.VMEM((KV_SLOTS, KV_TOK * tok_rows, half), bf),
                pltpu.VMEM((KV_SLOTS, KV_TOK * tok_rows, half), bf),
                pltpu.VMEM((X_SLOTS, ROWS, TILE), f32),
                pltpu.VMEM((X_SLOTS, HALF, TILE), f32),
                pltpu.VMEM((n_dn, HALF, TILE), bf),
                pltpu.VMEM((2, n_dn, HALF, TILE), bf),
                dma((SLOTS,)), dma((n_dn,)), dma((2, KV_SLOTS)), dma((2,)),
                dma((X_SLOTS,)), dma((X_SLOTS,)), dma((n_dn,)), dma((2, n_dn)), dma((2, n_dn)), dma((2, n_dn)), dma((2,)),
            ],
            compiler_params=pltpu.CompilerParams(
                collective_id=0, has_side_effects=True, vmem_limit_bytes=67_043_328),
            name="decoder",
        )(lengths.reshape(1, tokens), jnp.asarray(table), norm_gain, x_in, w_q, w_k, w_v, w_o, w_gate, w_up, w_down,
          rows_of(k_cache), rows_of(v_cache))

    return jax.shard_map(per_device, mesh=mesh, in_specs=arg_specs, out_specs=P('dp', None), check_vma=False)
```

```python
import functools

import jax
import jax.numpy as jnp
import numpy as np
from jax import lax
from jax.experimental import pallas as pl
from jax.experimental.pallas import tpu as pltpu
from jax.sharding import PartitionSpec as P

NORM_EPS = 1e-5
ROPE_BASE = 500000.0
MESH = pl.DeviceIdType.MESH

ROWS = 256
HALF = 128
TILE = 512
SLOTS = 7
KV_SLOTS = 7
X_SLOTS = 4
KV_TOK = 16


def kernel(cfg, lens_ref, table_ref, gain_ref, x_in, wq, wk, wv, wo, wg, wu, wd, kc, vc, x_out,
           xs, a_s, q_s, k_s, v_s, att_s, u_s, raws, cos_ref, sin_ref, len_s, len4, sidx, s_s, p_s, o_s, wbuf, wobuf, kbuf, vbuf, ybuf, irecv, rown, xrecv,
           wsem, wosem, kvsem, xsem, isend, irsem, xsend, xrsem, nsend, nrsem, osem):
    layers, tokens, width, seq, kv_heads = cfg
    tok_rows = seq * kv_heads * 2
    chunks = tokens // ROWS
    stages = layers * chunks
    n_dn = width // TILE
    n_ff = wg.shape[2] // TILE
    n_q = wq.shape[2] // TILE
    n_w = n_q + 2 + 2 * n_ff + n_dn
    n_kv = ROWS // KV_TOK
    all_w, all_kv = stages * n_w, stages * n_kv

    tp = lax.axis_index("tp")
    core = lax.rem(tp, 2)
    sib = tp + 1 - 2 * core
    partner = lax.rem(tp + 2, 4)
    own_row = pl.multiple_of(core * HALF, HALF)
    sib_row = pl.multiple_of((1 - core) * HALF, HALF)

    def w_start(gt):
        st = lax.div(gt, n_w)
        t = gt - st * n_w
        layer = lax.div(st, chunks)
        slot = lax.rem(gt, SLOTS)

        def put(src):
            pltpu.make_async_copy(src, wbuf.at[slot], wsem.at[slot]).start()

        def cols(i):
            return pl.ds(pl.multiple_of(i * TILE, TILE), TILE)

        f = t - (n_q + 2)

        @pl.when(t < n_q)
        def _():
            put(wq.at[layer, :, cols(t)])

        @pl.when(t == n_q)
        def _():
            put(wk.at[layer])

        @pl.when(t == n_q + 1)
        def _():
            put(wv.at[layer])

        @pl.when((f >= 0) & (f < 2 * n_ff) & (lax.rem(f + 2, 2) == 0))
        def _():
            put(wg.at[layer, :, cols(lax.div(f, 2))])

        @pl.when((f >= 0) & (f < 2 * n_ff) & (lax.rem(f + 2, 2) == 1))
        def _():
            put(wu.at[layer, :, cols(lax.div(f, 2))])

        @pl.when(f >= 2 * n_ff)
        def _():
            put(wd.at[layer, :, cols(f - 2 * n_ff)])

    def w_next(gt):
        @pl.when(gt + SLOTS < all_w)
        def _():
            w_start(gt + SLOTS)

    def w_wait(gt):
        slot = lax.rem(gt, SLOTS)
        pltpu.make_async_copy(wk.at[0], wbuf.at[slot], wsem.at[slot]).wait()
        return slot

    def wo_copy(layer, j):
        cols = pl.ds(pl.multiple_of(j * TILE, TILE), TILE)
        return pltpu.make_async_copy(wo.at[layer, :, cols], wobuf.at[j], wosem.at[j])

    def kv_copies(gb):
        st = lax.div(gb, n_kv)
        b = gb - st * n_kv
        layer = lax.div(st, chunks)
        tok = layer * tokens + (st - layer * chunks) * ROWS + b * KV_TOK
        slot = lax.rem(gb, KV_SLOTS)
        rows = pl.ds(pl.multiple_of(tok * tok_rows, KV_TOK * tok_rows), KV_TOK * tok_rows)
        return (pltpu.make_async_copy(kc.at[rows], kbuf.at[slot], kvsem.at[0, slot]),
                pltpu.make_async_copy(vc.at[rows], vbuf.at[slot], kvsem.at[1, slot]))

    def chip_copy(gj):
        slot = lax.rem(gj, X_SLOTS)
        return pltpu.make_async_remote_copy(
            src_ref=ybuf.at[slot, pl.ds(sib_row, HALF)], dst_ref=irecv.at[slot], send_sem=isend.at[slot],
            recv_sem=irsem.at[slot], device_id={"tp": sib}, device_id_type=MESH)

    def link_copy(par, j):
        return pltpu.make_async_remote_copy(
            src_ref=rown.at[j], dst_ref=xrecv.at[par, j], send_sem=xsend.at[j],
            recv_sem=xrsem.at[par, j], device_id={"tp": partner}, device_id_type=MESH)

    def x_piece(par, row, j):
        return xs.at[pl.ds(pl.multiple_of(par * ROWS + row, HALF), HALF), pl.ds(pl.multiple_of(j * TILE, TILE), TILE)]

    def new_copy(par, j):
        piece = x_piece(par, own_row, j)
        return pltpu.make_async_remote_copy(
            src_ref=piece, dst_ref=piece, send_sem=nsend.at[par, j],
            recv_sem=nrsem.at[par, j], device_id={"tp": sib}, device_id_type=MESH)

    def chip_sum(st, j):
        gj = st * n_dn + j
        slot = lax.rem(gj, X_SLOTS)
        chip_copy(gj).wait()
        rown[j] = (ybuf[slot, pl.ds(own_row, HALF)] + irecv[slot]).astype(jnp.bfloat16)
        link_copy(lax.rem(st, chunks), j).start()

    def finish(par):
        def step(j, _):
            link_copy(par, j).wait()
            piece = x_piece(par, own_row, j)
            total = rown[j].astype(jnp.float32) + xrecv[par, j].astype(jnp.float32)
            piece[...] = (piece[...].astype(jnp.float32) + total).astype(jnp.bfloat16)
            new_copy(par, j).start()
            return 0

        lax.fori_loop(0, n_dn, step, 0)

    def new_wait(par):
        def step(j, _):
            new_copy(par, j).wait()
            return 0

        lax.fori_loop(0, n_dn, step, 0)

    def x_copy(c):
        rows = pl.ds(pl.multiple_of(c * ROWS, ROWS), ROWS)
        return pltpu.make_async_copy(x_in.at[rows], xs.at[rows], xsem.at[c])

    def out_copy(c):
        rows = pl.ds(c * ROWS, ROWS)
        return pltpu.make_async_copy(xs.at[rows], x_out.at[rows], osem.at[c])

    x_copy(0).start()
    for g in range(SLOTS):
        w_start(jnp.int32(g))
    for g in range(KV_SLOTS):
        for cp in kv_copies(jnp.int32(g)):
            cp.start()
    for j in range(n_dn):
        wo_copy(0, j).start()
    for c in range(1, chunks):
        x_copy(c).start()

    barrier = pltpu.get_barrier_semaphore()
    for other in (sib, partner):
        pl.semaphore_signal(barrier, inc=1, device_id={"tp": other}, device_id_type=MESH)
    pl.semaphore_wait(barrier, 2)

    n_key = 2 * tok_rows
    lane = lax.broadcasted_iota(jnp.int32, (KV_TOK * 4, n_key), 1)
    row = lax.rem(lax.broadcasted_iota(jnp.int32, (KV_TOK * 4, n_key), 0), 8)
    per = 2 * kv_heads
    match = (lax.div(lane, tok_rows) == lax.div(row, 4)) & (lax.rem(lane, kv_heads) == lax.div(lax.rem(row, 4), 2)) & (lax.rem(lane, per) < kv_heads)
    sidx[...] = jnp.where(match, lax.rem(lax.div(lane, per), seq), 2 * seq).astype(jnp.float32)
    pick = lax.broadcasted_iota(jnp.int32, (seq, tokens), 0) == lens_ref[...]
    angles = lax.dot_general(pick.astype(jnp.float32), table_ref[...], (((0,), (0,)), ((), ())),
                             precision=lax.Precision.HIGHEST, preferred_element_type=jnp.float32)
    half = angles.shape[1] // 3
    cos_ref[...], sin_ref[...], len_s[...] = angles[:, :half], angles[:, half:2 * half], angles[:, 2 * half:]

    def rope(y, dst, first_head, copies, rows):
        cos, sin = cos_ref[rows], sin_ref[rows]
        for h in range(TILE // 256):
            first = y[:, h * 256:h * 256 + 128].astype(jnp.float32)
            second = y[:, h * 256 + 128:h * 256 + 256].astype(jnp.float32)
            lo = (first * cos - second * sin).astype(jnp.bfloat16).astype(jnp.float32)
            hi = (second * cos + first * sin).astype(jnp.bfloat16).astype(jnp.float32)
            for i in range(copies):
                at = pl.ds((first_head + h) * copies + i, ROWS, 4)
                dst[0, at] = lo
                dst[1, at] = hi

    def dot(a, b):
        return jnp.dot(a, b, preferred_element_type=jnp.float32)

    scale = 1.0 / 16.0
    n_pair = KV_TOK // 2
    n_row = KV_TOK * 4

    def roll(x, by):
        return jnp.concatenate([pltpu.roll(x[:, i:i + 128], by % 128, axis=1) for i in (0, 128)], 1)

    def block_rows(b):
        return pl.ds(pl.multiple_of(b * n_row, n_row), n_row)

    def logits(side, st, b):
        slot = lax.rem(st * n_kv + b, KV_SLOTS)
        q = [(q_s[j, block_rows(b)] * scale).reshape(n_pair, 8, 128) for j in range(2)]
        qq = jnp.concatenate(q, 1).astype(jnp.bfloat16)
        for g in range(n_pair):
            keys = kbuf[slot, pl.ds(g * n_key, n_key)]
            s_s[side][g * 16:g * 16 + 16] = lax.dot_general(
                qq[g], keys, (((1,), (1,)), ((), ())), preferred_element_type=jnp.float32)

    def soft(side, c, b):
        s2 = s_s[side][...].reshape(n_pair, 2, 8, n_key)
        s = s2[:, 0].reshape(n_row, n_key) + roll(s2[:, 1].reshape(n_row, n_key), -2)
        r = block_rows(b)
        self_logit = jnp.sum(q_s[0, r] * k_s[0, r] + q_s[1, r] * k_s[1, r], axis=-1, keepdims=True) * scale
        keep = sidx[...] < len4[r, :1]
        s = jnp.where(keep, s, -jnp.inf)
        peak = jnp.maximum(jnp.max(s, axis=-1, keepdims=True), self_logit)
        w = jnp.exp(s - peak)
        sw = jnp.exp(self_logit - peak)
        inv = 1.0 / (jnp.sum(w, axis=-1, keepdims=True) + sw)
        p = w * inv
        pp = jnp.concatenate([p.reshape(n_pair, 8, n_key), roll(p, 2).reshape(n_pair, 8, n_key)], 1)
        p_s[side][...] = pp.reshape(2 * n_row, n_key).astype(jnp.bfloat16)
        sp = (sw * inv).astype(jnp.bfloat16).astype(jnp.float32)
        for j in range(2):
            o_s[side][j] = sp * v_s[j, r]

    def mix(side, st, b):
        slot = lax.rem(st * n_kv + b, KV_SLOTS)
        base = pl.multiple_of(b * n_row, n_row)
        for g in range(n_pair):
            o2 = dot(p_s[side][g * 16:g * 16 + 16], vbuf[slot, pl.ds(g * n_key, n_key)])
            for j in range(2):
                q_s[j, pl.ds(base + g * 8, 8)] = o2[j * 8:j * 8 + 8] + o_s[side][j, g * 8:g * 8 + 8]

    def k_next(gb):
        @pl.when(gb + KV_SLOTS < all_kv)
        def _():
            kv_copies(gb + KV_SLOTS)[0].start()

    def v_next(gb):
        @pl.when(gb + KV_SLOTS < all_kv)
        def _():
            kv_copies(gb + KV_SLOTS)[1].start()

    def swiglu(side, i):
        g = raws[2 * side][...].astype(jnp.float32)
        u = raws[2 * side + 1][...].astype(jnp.float32)
        u_s[:, pl.ds(pl.multiple_of(i * TILE, TILE), TILE)] = (g * (1.0 / (1.0 + jnp.exp(-g))) * u).astype(jnp.bfloat16)

    def stage(st, _):
        layer = lax.div(st, chunks)
        c = st - layer * chunks
        par = c
        rows = pl.ds(pl.multiple_of(c * ROWS, ROWS), ROWS)
        w0 = st * n_w

        @pl.when(st < chunks)
        def _():
            x_copy(c).wait()

        @pl.when(st >= chunks)
        def _():
            new_wait(par)

        gains = gain_ref[...].astype(jnp.float32)
        gain = gains[:1]
        for other in range(1, layers):
            gain = jnp.where(layer == other, gains[other:other + 1], gain)

        def norm_rows(i):
            src = pl.ds(pl.multiple_of(c * ROWS + i * 16, 16), 16)
            dst = pl.ds(pl.multiple_of(i * 16, 16), 16)
            parts = range(0, width, 256)
            total = jnp.zeros((16, 256), jnp.float32)
            for p in parts:
                x = xs[src, p:p + 256].astype(jnp.float32)
                total = total + x * x
            inv = lax.rsqrt(jnp.sum(total, axis=-1, keepdims=True) / width + NORM_EPS)
            for p in parts:
                x = xs[src, p:p + 256].astype(jnp.float32)
                a_s[dst, p:p + 256] = (x * inv * gain[:, p:p + 256]).astype(jnp.bfloat16)

        def norm(i, _):
            norm_rows(2 * i)
            norm_rows(2 * i + 1)
            return 0

        lax.fori_loop(0, ROWS // 32, norm, 0)

        @pl.when(st >= 1)
        def _():
            for j in range(n_dn - 2, n_dn):
                chip_sum(st - 1, j)

        slots = [w_wait(w0), w_wait(w0 + 1)]
        for i in range(2):
            raws[i][...] = dot(a_s[...], wbuf[slots[i]]).astype(jnp.bfloat16)
        w_next(w0)
        w_next(w0 + 1)
        slots = [w_wait(w0 + 2), w_wait(w0 + 3)]
        raws[2][...] = dot(a_s[...], wbuf[slots[0]]).astype(jnp.bfloat16)
        rope(raws[0], q_s, 0, 1, rows)
        rope(raws[1], q_s, 2, 1, rows)
        v = dot(a_s[...], wbuf[slots[1]]).astype(jnp.bfloat16).astype(jnp.float32)
        rope(raws[2], k_s, 0, 2, rows)
        for h in range(4):
            for j in range(2):
                v_s[j, pl.ds(h, ROWS, 4)] = v[:, (h // 2) * 256 + j * 128:(h // 2) * 256 + j * 128 + 128]
            len4[pl.ds(h, ROWS, 4)] = len_s[rows]

        b0 = st * n_kv
        kv_copies(b0)[0].wait()
        logits(0, st, 0)
        k_next(b0)
        kv_copies(b0 + 1)[0].wait()
        soft(0, c, 0)
        logits(1, st, 1)
        k_next(b0 + 1)

        def half(side, b):
            kv_copies(b0 + b - 1)[1].wait()
            kv_copies(b0 + b + 1)[0].wait()
            mix(1 - side, st, b - 1)
            soft(side, c, b)
            logits(1 - side, st, b + 1)
            v_next(b0 + b - 1)
            k_next(b0 + b + 1)

        def block(i, _):
            half(1, 2 * i + 1)

            @pl.when((i == 0) | (i == 2))
            def _():
                w_next(w0 + n_q + lax.div(i, 2))

            half(0, 2 * i + 2)
            return 0

        lax.fori_loop(0, n_kv // 2 - 1, block, 0)
        kv_copies(b0 + n_kv - 2)[1].wait()
        mix(0, st, n_kv - 2)
        soft(1, c, n_kv - 1)
        v_next(b0 + n_kv - 2)
        kv_copies(b0 + n_kv - 1)[1].wait()
        mix(1, st, n_kv - 1)
        v_next(b0 + n_kv - 1)
        for h in range(4):
            for j in range(2):
                at = h * 256 + j * 128
                att_s[:, at:at + 128] = q_s[j, pl.ds(h, ROWS, 4)].astype(jnp.bfloat16)

        def ff_tile(side, i):
            gt = w0 + n_q + 2 + 2 * i
            s0, s1 = w_wait(gt), w_wait(gt + 1)
            swiglu(1 - side, lax.rem(i + n_ff - 1, n_ff))
            raws[2 * side][...] = dot(a_s[...], wbuf[s0]).astype(jnp.bfloat16)
            raws[2 * side + 1][...] = dot(a_s[...], wbuf[s1]).astype(jnp.bfloat16)
            w_next(gt)
            w_next(gt + 1)

        def ff(i, _):
            ff_tile(0, 2 * i)
            ff_tile(1, 2 * i + 1)
            return 0

        lax.fori_loop(0, n_ff // 2, ff, 0)
        if n_ff % 2:
            ff_tile(0, n_ff - 1)
        swiglu((n_ff - 1) % 2, n_ff - 1)

        @pl.when(st >= 1)
        def _():
            finish(1 - par)

        def down(j, _):
            gt = w0 + n_q + 2 + 2 * n_ff + j
            s0 = w_wait(gt)

            @pl.when(c == 0)
            def _():
                wo_copy(layer, j).wait()

            @pl.when(j >= 2)
            def _():
                chip_sum(st, j - 2)

            gj = st * n_dn + j
            ybuf[lax.rem(gj, X_SLOTS)] = dot(u_s[...], wbuf[s0]) + dot(att_s[...], wobuf[j])
            chip_copy(gj).start()
            w_next(gt)

            @pl.when((c == chunks - 1) & (layer < layers - 1))
            def _():
                wo_copy(layer + 1, j).start()

            return 0

        lax.fori_loop(0, n_dn, down, 0)
        return 0

    for raw in raws:
        raw[...] = jnp.zeros_like(raw)
    lax.fori_loop(0, stages, stage, 0)

    last = (stages - 1) % chunks
    for j in range(n_dn - 2, n_dn):
        chip_sum(stages - 1, j)
    new_wait(1 - last)
    out_copy(1 - last).start()
    finish(last)
    new_wait(last)
    out_copy(last).start()
    for c in range(chunks):
        out_copy(c).wait()


def solution(mesh):
    arg_specs = (P('dp', None), P('dp'), P(), P(None, None, 'tp'), P(None, None, 'tp'), P(None, None, 'tp'), P(None, 'tp', None), P(None, None, 'tp'), P(None, None, 'tp'), P(None, 'tp', None), P(None, 'dp', None, 'tp', None), P(None, 'dp', None, 'tp', None))

    def per_device(x_in, lengths, norm_gain, w_q, w_k, w_v, w_o, w_gate, w_up, w_down, k_cache, v_cache):
        layers, tokens, seq, kv_heads, head = k_cache.shape
        width = x_in.shape[1]
        half = head // 2
        inv_freq = 1.0 / (np.float32(ROPE_BASE) ** (np.arange(0, head, 2).astype(np.float32) / np.float32(head)))
        pos = np.arange(seq).astype(np.float32)[:, None]
        angles = pos * inv_freq[None, :].astype(np.float32)
        table = np.concatenate([np.cos(angles), np.sin(angles), pos + 0 * angles], 1).astype(np.float32)

        def rows_of(cache):
            r = cache.reshape(layers * tokens * seq, kv_heads, 2, half).transpose(0, 2, 1, 3)
            return r.reshape(layers * tokens * seq * kv_heads * 2, half)

        tok_rows = seq * kv_heads * 2
        n_dn = width // TILE
        vm = pl.BlockSpec(memory_space=pltpu.VMEM)
        hbm = pl.BlockSpec(memory_space=pl.ANY)
        bf, f32 = jnp.bfloat16, jnp.float32
        dma = pltpu.SemaphoreType.DMA
        return pl.pallas_call(
            functools.partial(kernel, (layers, tokens, width, seq, kv_heads)),
            out_shape=jax.ShapeDtypeStruct(x_in.shape, bf),
            in_specs=[vm] * 3 + [hbm] * 10,
            out_specs=hbm,
            scratch_shapes=[
                pltpu.VMEM((tokens, width), bf),
                pltpu.VMEM((ROWS, width), bf),
                pltpu.VMEM((2, 4 * ROWS, half), f32),
                pltpu.VMEM((2, 4 * ROWS, half), f32),
                pltpu.VMEM((2, 4 * ROWS, half), f32),
                pltpu.VMEM((ROWS, w_q.shape[2]), bf),
                pltpu.VMEM((ROWS, w_gate.shape[2]), bf),
                [pltpu.VMEM((ROWS, TILE), bf)] * 4,
                pltpu.VMEM((tokens, half), f32),
                pltpu.VMEM((tokens, half), f32),
                pltpu.VMEM((tokens, half), f32),
                pltpu.VMEM((4 * ROWS, half), f32),
                pltpu.VMEM((4 * KV_TOK, 2 * tok_rows), f32),
                [pltpu.VMEM((8 * KV_TOK, 2 * tok_rows), f32)] * 2,
                [pltpu.VMEM((8 * KV_TOK, 2 * tok_rows), bf)] * 2,
                [pltpu.VMEM((2, 4 * KV_TOK, half), f32)] * 2,
                pltpu.VMEM((SLOTS, width, TILE), bf),
                pltpu.VMEM((n_dn, w_o.shape[1], TILE), bf),
                pltpu.VMEM((KV_SLOTS, KV_TOK * tok_rows, half), bf),
                pltpu.VMEM((KV_SLOTS, KV_TOK * tok_rows, half), bf),
                pltpu.VMEM((X_SLOTS, ROWS, TILE), f32),
                pltpu.VMEM((X_SLOTS, HALF, TILE), f32),
                pltpu.VMEM((n_dn, HALF, TILE), bf),
                pltpu.VMEM((2, n_dn, HALF, TILE), bf),
                dma((SLOTS,)), dma((n_dn,)), dma((2, KV_SLOTS)), dma((2,)),
                dma((X_SLOTS,)), dma((X_SLOTS,)), dma((n_dn,)), dma((2, n_dn)), dma((2, n_dn)), dma((2, n_dn)), dma((2,)),
            ],
            compiler_params=pltpu.CompilerParams(
                collective_id=0, has_side_effects=True, vmem_limit_bytes=67_043_328),
            name="decoder",
        )(lengths.reshape(1, tokens), jnp.asarray(table), norm_gain, x_in, w_q, w_k, w_v, w_o, w_gate, w_up, w_down,
          rows_of(k_cache), rows_of(v_cache))

    return jax.shard_map(per_device, mesh=mesh, in_specs=arg_specs, out_specs=P('dp', None), check_vma=False)
```

```python
import functools

import jax
import jax.numpy as jnp
import numpy as np
from jax import lax
from jax.experimental import pallas as pl
from jax.experimental.pallas import tpu as pltpu
from jax.sharding import PartitionSpec as P

NORM_EPS = 1e-5
ROPE_BASE = 500000.0
MESH = pl.DeviceIdType.MESH

ROWS = 256
HALF = 128
TILE = 512
SLOTS = 7
KV_SLOTS = 4
X_SLOTS = 4
KV_TOK = 32


def kernel(cfg, lens_ref, table_ref, gain_ref, x_in, wq, wk, wv, wo, wg, wu, wd, kc, vc, x_out,
           xs, a_s, q_s, k_s, v_s, att_s, u_s, raws, cos_ref, sin_ref, len_s, len4, sidx, s_s, p_s, o_s, wbuf, wobuf, kbuf, vbuf, ybuf, irecv, rown, xrecv,
           wsem, wosem, kvsem, xsem, isend, irsem, xsend, xrsem, nsend, nrsem, osem):
    layers, tokens, width, seq, kv_heads = cfg
    tok_rows = seq * kv_heads * 2
    chunks = tokens // ROWS
    stages = layers * chunks
    n_dn = width // TILE
    n_ff = wg.shape[2] // TILE
    n_q = wq.shape[2] // TILE
    n_w = n_q + 2 + 2 * n_ff + n_dn
    n_kv = ROWS // KV_TOK
    all_w, all_kv = stages * n_w, stages * n_kv

    tp = lax.axis_index("tp")
    core = lax.rem(tp, 2)
    sib = tp + 1 - 2 * core
    partner = lax.rem(tp + 2, 4)
    own_row = pl.multiple_of(core * HALF, HALF)
    sib_row = pl.multiple_of((1 - core) * HALF, HALF)

    def w_start(gt):
        st = lax.div(gt, n_w)
        t = gt - st * n_w
        layer = lax.div(st, chunks)
        slot = lax.rem(gt, SLOTS)

        def put(src):
            pltpu.make_async_copy(src, wbuf.at[slot], wsem.at[slot]).start()

        def cols(i):
            return pl.ds(pl.multiple_of(i * TILE, TILE), TILE)

        f = t - (n_q + 2)

        @pl.when(t < n_q)
        def _():
            put(wq.at[layer, :, cols(t)])

        @pl.when(t == n_q)
        def _():
            put(wk.at[layer])

        @pl.when(t == n_q + 1)
        def _():
            put(wv.at[layer])

        @pl.when((f >= 0) & (f < 2 * n_ff) & (lax.rem(f + 2, 2) == 0))
        def _():
            put(wg.at[layer, :, cols(lax.div(f, 2))])

        @pl.when((f >= 0) & (f < 2 * n_ff) & (lax.rem(f + 2, 2) == 1))
        def _():
            put(wu.at[layer, :, cols(lax.div(f, 2))])

        @pl.when(f >= 2 * n_ff)
        def _():
            put(wd.at[layer, :, cols(f - 2 * n_ff)])

    def w_next(gt):
        @pl.when(gt + SLOTS < all_w)
        def _():
            w_start(gt + SLOTS)

    def w_wait(gt):
        slot = lax.rem(gt, SLOTS)
        pltpu.make_async_copy(wk.at[0], wbuf.at[slot], wsem.at[slot]).wait()
        return slot

    def wo_copy(layer, j):
        cols = pl.ds(pl.multiple_of(j * TILE, TILE), TILE)
        return pltpu.make_async_copy(wo.at[layer, :, cols], wobuf.at[j], wosem.at[j])

    def kv_copies(gb):
        st = lax.div(gb, n_kv)
        b = gb - st * n_kv
        layer = lax.div(st, chunks)
        tok = layer * tokens + (st - layer * chunks) * ROWS + b * KV_TOK
        slot = lax.rem(gb, KV_SLOTS)
        rows = pl.ds(pl.multiple_of(tok * tok_rows, KV_TOK * tok_rows), KV_TOK * tok_rows)
        return (pltpu.make_async_copy(kc.at[rows], kbuf.at[slot], kvsem.at[0, slot]),
                pltpu.make_async_copy(vc.at[rows], vbuf.at[slot], kvsem.at[1, slot]))

    def chip_copy(gj):
        slot = lax.rem(gj, X_SLOTS)
        return pltpu.make_async_remote_copy(
            src_ref=ybuf.at[slot, pl.ds(sib_row, HALF)], dst_ref=irecv.at[slot], send_sem=isend.at[slot],
            recv_sem=irsem.at[slot], device_id={"tp": sib}, device_id_type=MESH)

    def link_copy(par, j):
        return pltpu.make_async_remote_copy(
            src_ref=rown.at[j], dst_ref=xrecv.at[par, j], send_sem=xsend.at[j],
            recv_sem=xrsem.at[par, j], device_id={"tp": partner}, device_id_type=MESH)

    def x_piece(par, row, j):
        return xs.at[pl.ds(pl.multiple_of(par * ROWS + row, HALF), HALF), pl.ds(pl.multiple_of(j * TILE, TILE), TILE)]

    def new_copy(par, j):
        piece = x_piece(par, own_row, j)
        return pltpu.make_async_remote_copy(
            src_ref=piece, dst_ref=piece, send_sem=nsend.at[par, j],
            recv_sem=nrsem.at[par, j], device_id={"tp": sib}, device_id_type=MESH)

    def chip_sum(st, j):
        gj = st * n_dn + j
        slot = lax.rem(gj, X_SLOTS)
        chip_copy(gj).wait()
        rown[j] = (ybuf[slot, pl.ds(own_row, HALF)] + irecv[slot]).astype(jnp.bfloat16)
        link_copy(lax.rem(st, chunks), j).start()

    def finish(par):
        def step(j, _):
            link_copy(par, j).wait()
            piece = x_piece(par, own_row, j)
            total = rown[j].astype(jnp.float32) + xrecv[par, j].astype(jnp.float32)
            piece[...] = (piece[...].astype(jnp.float32) + total).astype(jnp.bfloat16)
            new_copy(par, j).start()
            return 0

        lax.fori_loop(0, n_dn, step, 0)

    def new_wait(par):
        def step(j, _):
            new_copy(par, j).wait()
            return 0

        lax.fori_loop(0, n_dn, step, 0)

    def x_copy(c):
        rows = pl.ds(pl.multiple_of(c * ROWS, ROWS), ROWS)
        return pltpu.make_async_copy(x_in.at[rows], xs.at[rows], xsem.at[c])

    def out_copy(c):
        rows = pl.ds(c * ROWS, ROWS)
        return pltpu.make_async_copy(xs.at[rows], x_out.at[rows], osem.at[c])

    x_copy(0).start()
    for g in range(SLOTS):
        w_start(jnp.int32(g))
    for g in range(KV_SLOTS):
        for cp in kv_copies(jnp.int32(g)):
            cp.start()
    for j in range(n_dn):
        wo_copy(0, j).start()
    for c in range(1, chunks):
        x_copy(c).start()

    barrier = pltpu.get_barrier_semaphore()
    for other in (sib, partner):
        pl.semaphore_signal(barrier, inc=1, device_id={"tp": other}, device_id_type=MESH)
    pl.semaphore_wait(barrier, 2)

    n_key = 2 * tok_rows
    lane = lax.broadcasted_iota(jnp.int32, (KV_TOK * 4, n_key), 1)
    row = lax.rem(lax.broadcasted_iota(jnp.int32, (KV_TOK * 4, n_key), 0), 8)
    per = 2 * kv_heads
    match = (lax.div(lane, tok_rows) == lax.div(row, 4)) & (lax.rem(lane, kv_heads) == lax.div(lax.rem(row, 4), 2)) & (lax.rem(lane, per) < kv_heads)
    sidx[...] = jnp.where(match, lax.rem(lax.div(lane, per), seq), 2 * seq).astype(jnp.float32)
    pick = lax.broadcasted_iota(jnp.int32, (seq, tokens), 0) == lens_ref[...]
    angles = lax.dot_general(pick.astype(jnp.float32), table_ref[...], (((0,), (0,)), ((), ())),
                             precision=lax.Precision.HIGHEST, preferred_element_type=jnp.float32)
    half = angles.shape[1] // 3
    cos_ref[...], sin_ref[...], len_s[...] = angles[:, :half], angles[:, half:2 * half], angles[:, 2 * half:]

    def rope(y, dst, first_head, copies, rows):
        cos, sin = cos_ref[rows], sin_ref[rows]
        for h in range(TILE // 256):
            first = y[:, h * 256:h * 256 + 128].astype(jnp.float32)
            second = y[:, h * 256 + 128:h * 256 + 256].astype(jnp.float32)
            lo = (first * cos - second * sin).astype(jnp.bfloat16).astype(jnp.float32)
            hi = (second * cos + first * sin).astype(jnp.bfloat16).astype(jnp.float32)
            for i in range(copies):
                at = pl.ds((first_head + h) * copies + i, ROWS, 4)
                dst[0, at] = lo
                dst[1, at] = hi

    def dot(a, b):
        return jnp.dot(a, b, preferred_element_type=jnp.float32)

    scale = 1.0 / 16.0
    n_pair = KV_TOK // 2
    n_row = KV_TOK * 4

    def roll(x, by):
        return jnp.concatenate([pltpu.roll(x[:, i:i + 128], by % 128, axis=1) for i in (0, 128)], 1)

    def block_rows(b):
        return pl.ds(pl.multiple_of(b * n_row, n_row), n_row)

    def logits(side, st, b):
        slot = lax.rem(st * n_kv + b, KV_SLOTS)
        q = [(q_s[j, block_rows(b)] * scale).reshape(n_pair, 8, 128) for j in range(2)]
        qq = jnp.concatenate(q, 1).astype(jnp.bfloat16)
        for g in range(n_pair):
            keys = kbuf[slot, pl.ds(g * n_key, n_key)]
            s_s[side][g * 16:g * 16 + 16] = lax.dot_general(
                qq[g], keys, (((1,), (1,)), ((), ())), preferred_element_type=jnp.float32)

    def soft(side, c, b):
        s2 = s_s[side][...].reshape(n_pair, 2, 8, n_key)
        s = s2[:, 0].reshape(n_row, n_key) + roll(s2[:, 1].reshape(n_row, n_key), -2)
        r = block_rows(b)
        self_logit = jnp.sum(q_s[0, r] * k_s[0, r] + q_s[1, r] * k_s[1, r], axis=-1, keepdims=True) * scale
        keep = sidx[...] < len4[r, :1]
        s = jnp.where(keep, s, -jnp.inf)
        peak = jnp.maximum(jnp.max(s, axis=-1, keepdims=True), self_logit)
        w = jnp.exp(s - peak)
        sw = jnp.exp(self_logit - peak)
        inv = 1.0 / (jnp.sum(w, axis=-1, keepdims=True) + sw)
        p = w * inv
        pp = jnp.concatenate([p.reshape(n_pair, 8, n_key), roll(p, 2).reshape(n_pair, 8, n_key)], 1)
        p_s[side][...] = pp.reshape(2 * n_row, n_key).astype(jnp.bfloat16)
        sp = (sw * inv).astype(jnp.bfloat16).astype(jnp.float32)
        for j in range(2):
            o_s[side][j] = sp * v_s[j, r]

    def mix(side, st, b):
        slot = lax.rem(st * n_kv + b, KV_SLOTS)
        base = pl.multiple_of(b * n_row, n_row)
        for g in range(n_pair):
            o2 = dot(p_s[side][g * 16:g * 16 + 16], vbuf[slot, pl.ds(g * n_key, n_key)])
            for j in range(2):
                q_s[j, pl.ds(base + g * 8, 8)] = o2[j * 8:j * 8 + 8] + o_s[side][j, g * 8:g * 8 + 8]

    def k_next(gb):
        @pl.when(gb + KV_SLOTS < all_kv)
        def _():
            kv_copies(gb + KV_SLOTS)[0].start()

    def v_next(gb):
        @pl.when(gb + KV_SLOTS < all_kv)
        def _():
            kv_copies(gb + KV_SLOTS)[1].start()

    def swiglu(side, i):
        g = raws[2 * side][...].astype(jnp.float32)
        u = raws[2 * side + 1][...].astype(jnp.float32)
        u_s[:, pl.ds(pl.multiple_of(i * TILE, TILE), TILE)] = (g * (1.0 / (1.0 + jnp.exp(-g))) * u).astype(jnp.bfloat16)

    def norm_rows(chunk, layer, i):
        gains = gain_ref[...].astype(jnp.float32)
        gain = gains[:1]
        for other in range(1, layers):
            gain = jnp.where(layer == other, gains[other:other + 1], gain)
        src = pl.ds(pl.multiple_of(chunk * ROWS + i * 16, 16), 16)
        dst = pl.ds(pl.multiple_of(i * 16, 16), 16)
        parts = range(0, width, 256)
        total = jnp.zeros((16, 256), jnp.float32)
        for p in parts:
            x = xs[src, p:p + 256].astype(jnp.float32)
            total = total + x * x
        inv = lax.rsqrt(jnp.sum(total, axis=-1, keepdims=True) / width + NORM_EPS)
        for p in parts:
            x = xs[src, p:p + 256].astype(jnp.float32)
            a_s[dst, p:p + 256] = (x * inv * gain[:, p:p + 256]).astype(jnp.bfloat16)

    def stage(st, _):
        layer = lax.div(st, chunks)
        c = st - layer * chunks
        par = c
        rows = pl.ds(pl.multiple_of(c * ROWS, ROWS), ROWS)
        w0 = st * n_w

        slots = [w_wait(w0), w_wait(w0 + 1)]
        for i in range(2):
            raws[i][...] = dot(a_s[...], wbuf[slots[i]]).astype(jnp.bfloat16)
        w_next(w0)
        w_next(w0 + 1)

        @pl.when(st >= 1)
        def _():
            for j in range(n_dn - 2, n_dn):
                chip_sum(st - 1, j)

        b0 = st * n_kv
        slots = [w_wait(w0 + 2), w_wait(w0 + 3)]
        kv_copies(b0)[0].wait()
        kv_copies(b0 + 1)[0].wait()
        raws[2][...] = dot(a_s[...], wbuf[slots[0]]).astype(jnp.bfloat16)
        rope(raws[0], q_s, 0, 1, rows)
        rope(raws[1], q_s, 2, 1, rows)
        v = dot(a_s[...], wbuf[slots[1]]).astype(jnp.bfloat16).astype(jnp.float32)
        logits(0, st, 0)
        rope(raws[2], k_s, 0, 2, rows)
        for h in range(4):
            for j in range(2):
                v_s[j, pl.ds(h, ROWS, 4)] = v[:, (h // 2) * 256 + j * 128:(h // 2) * 256 + j * 128 + 128]
            len4[pl.ds(h, ROWS, 4)] = len_s[rows]
        soft(0, c, 0)
        logits(1, st, 1)
        k_next(b0)
        k_next(b0 + 1)

        def half(side, b):
            kv_copies(b0 + b - 1)[1].wait()
            kv_copies(b0 + b + 1)[0].wait()
            mix(1 - side, st, b - 1)
            soft(side, c, b)
            logits(1 - side, st, b + 1)
            v_next(b0 + b - 1)
            k_next(b0 + b + 1)

        def block(i, _):
            half(1, 2 * i + 1)

            @pl.when((i == 0) | (i == 2))
            def _():
                w_next(w0 + n_q + lax.div(i, 2))

            half(0, 2 * i + 2)
            return 0

        lax.fori_loop(0, n_kv // 2 - 1, block, 0)
        kv_copies(b0 + n_kv - 2)[1].wait()
        kv_copies(b0 + n_kv - 1)[1].wait()
        mix(0, st, n_kv - 2)
        soft(1, c, n_kv - 1)
        mix(1, st, n_kv - 1)
        for h in range(4):
            for j in range(2):
                at = h * 256 + j * 128
                att_s[:, at:at + 128] = q_s[j, pl.ds(h, ROWS, 4)].astype(jnp.bfloat16)
        v_next(b0 + n_kv - 2)
        v_next(b0 + n_kv - 1)

        def ff_tile(side, i):
            gt = w0 + n_q + 2 + 2 * i
            s0, s1 = w_wait(gt), w_wait(gt + 1)
            swiglu(1 - side, lax.rem(i + n_ff - 1, n_ff))
            raws[2 * side][...] = dot(a_s[...], wbuf[s0]).astype(jnp.bfloat16)
            raws[2 * side + 1][...] = dot(a_s[...], wbuf[s1]).astype(jnp.bfloat16)
            w_next(gt)
            w_next(gt + 1)

        def ff(i, _):
            ff_tile(0, 2 * i)
            ff_tile(1, 2 * i + 1)
            return 0

        lax.fori_loop(0, n_ff // 2, ff, 0)
        if n_ff % 2:
            ff_tile(0, n_ff - 1)
        swiglu((n_ff - 1) % 2, n_ff - 1)

        @pl.when(st >= 1)
        def _():
            finish(1 - par)

        following = st + 1
        turn = lax.rem(following, chunks)
        source = turn + lax.div(following, stages) * (c - turn)
        n_norm = 4
        groups = ROWS // 16 // n_norm

        def down(j, with_norm):
            gt = w0 + n_q + 2 + 2 * n_ff + j
            s0 = w_wait(gt)

            @pl.when(c == 0)
            def _():
                wo_copy(layer, j).wait()

            @pl.when(j >= 2)
            def _():
                chip_sum(st, j - 2)

            gj = st * n_dn + j
            if with_norm:
                for i in range(groups):
                    norm_rows(source, lax.div(following, chunks), (j - (n_dn - n_norm)) * groups + i)
            ybuf[lax.rem(gj, X_SLOTS)] = dot(u_s[...], wbuf[s0]) + dot(att_s[...], wobuf[j])
            chip_copy(gj).start()
            w_next(gt)

            @pl.when((c == chunks - 1) & (layer < layers - 1))
            def _():
                wo_copy(layer + 1, j).start()

        def down_plain(j, _):
            down(j, False)
            return 0

        def down_norm(j, _):
            down(j, True)
            return 0

        lax.fori_loop(0, n_dn - n_norm, down_plain, 0)

        @pl.when(following < chunks)
        def _():
            x_copy(turn).wait()

        @pl.when((following >= chunks) & (following < stages))
        def _():
            new_wait(turn)

        lax.fori_loop(n_dn - n_norm, n_dn, down_norm, 0)
        return 0

    x_copy(0).wait()

    def first(i, _):
        norm_rows(0, 0, 2 * i)
        norm_rows(0, 0, 2 * i + 1)
        return 0

    lax.fori_loop(0, ROWS // 32, first, 0)
    for raw in raws:
        raw[...] = jnp.zeros_like(raw)
    lax.fori_loop(0, stages, stage, 0)

    last = (stages - 1) % chunks
    for j in range(n_dn - 2, n_dn):
        chip_sum(stages - 1, j)
    new_wait(1 - last)
    out_copy(1 - last).start()
    finish(last)
    new_wait(last)
    out_copy(last).start()
    for c in range(chunks):
        out_copy(c).wait()


def solution(mesh):
    arg_specs = (P('dp', None), P('dp'), P(), P(None, None, 'tp'), P(None, None, 'tp'), P(None, None, 'tp'), P(None, 'tp', None), P(None, None, 'tp'), P(None, None, 'tp'), P(None, 'tp', None), P(None, 'dp', None, 'tp', None), P(None, 'dp', None, 'tp', None))

    def per_device(x_in, lengths, norm_gain, w_q, w_k, w_v, w_o, w_gate, w_up, w_down, k_cache, v_cache):
        layers, tokens, seq, kv_heads, head = k_cache.shape
        width = x_in.shape[1]
        half = head // 2
        inv_freq = 1.0 / (np.float32(ROPE_BASE) ** (np.arange(0, head, 2).astype(np.float32) / np.float32(head)))
        pos = np.arange(seq).astype(np.float32)[:, None]
        angles = pos * inv_freq[None, :].astype(np.float32)
        table = np.concatenate([np.cos(angles), np.sin(angles), pos + 0 * angles], 1).astype(np.float32)

        def rows_of(cache):
            r = cache.reshape(layers * tokens * seq, kv_heads, 2, half).transpose(0, 2, 1, 3)
            return r.reshape(layers * tokens * seq * kv_heads * 2, half)

        tok_rows = seq * kv_heads * 2
        n_dn = width // TILE
        vm = pl.BlockSpec(memory_space=pltpu.VMEM)
        hbm = pl.BlockSpec(memory_space=pl.ANY)
        bf, f32 = jnp.bfloat16, jnp.float32
        dma = pltpu.SemaphoreType.DMA
        return pl.pallas_call(
            functools.partial(kernel, (layers, tokens, width, seq, kv_heads)),
            out_shape=jax.ShapeDtypeStruct(x_in.shape, bf),
            in_specs=[vm] * 3 + [hbm] * 10,
            out_specs=hbm,
            scratch_shapes=[
                pltpu.VMEM((tokens, width), bf),
                pltpu.VMEM((ROWS, width), bf),
                pltpu.VMEM((2, 4 * ROWS, half), f32),
                pltpu.VMEM((2, 4 * ROWS, half), f32),
                pltpu.VMEM((2, 4 * ROWS, half), f32),
                pltpu.VMEM((ROWS, w_q.shape[2]), bf),
                pltpu.VMEM((ROWS, w_gate.shape[2]), bf),
                [pltpu.VMEM((ROWS, TILE), bf)] * 4,
                pltpu.VMEM((tokens, half), f32),
                pltpu.VMEM((tokens, half), f32),
                pltpu.VMEM((tokens, half), f32),
                pltpu.VMEM((4 * ROWS, half), f32),
                pltpu.VMEM((4 * KV_TOK, 2 * tok_rows), f32),
                [pltpu.VMEM((8 * KV_TOK, 2 * tok_rows), f32)] * 2,
                [pltpu.VMEM((8 * KV_TOK, 2 * tok_rows), bf)] * 2,
                [pltpu.VMEM((2, 4 * KV_TOK, half), f32)] * 2,
                pltpu.VMEM((SLOTS, width, TILE), bf),
                pltpu.VMEM((n_dn, w_o.shape[1], TILE), bf),
                pltpu.VMEM((KV_SLOTS, KV_TOK * tok_rows, half), bf),
                pltpu.VMEM((KV_SLOTS, KV_TOK * tok_rows, half), bf),
                pltpu.VMEM((X_SLOTS, ROWS, TILE), f32),
                pltpu.VMEM((X_SLOTS, HALF, TILE), f32),
                pltpu.VMEM((n_dn, HALF, TILE), bf),
                pltpu.VMEM((2, n_dn, HALF, TILE), bf),
                dma((SLOTS,)), dma((n_dn,)), dma((2, KV_SLOTS)), dma((2,)),
                dma((X_SLOTS,)), dma((X_SLOTS,)), dma((n_dn,)), dma((2, n_dn)), dma((2, n_dn)), dma((2, n_dn)), dma((2,)),
            ],
            compiler_params=pltpu.CompilerParams(
                collective_id=0, has_side_effects=True, vmem_limit_bytes=67_043_328),
            name="decoder",
        )(lengths.reshape(1, tokens), jnp.asarray(table), norm_gain, x_in, w_q, w_k, w_v, w_o, w_gate, w_up, w_down,
          rows_of(k_cache), rows_of(v_cache))

    return jax.shard_map(per_device, mesh=mesh, in_specs=arg_specs, out_specs=P('dp', None), check_vma=False)
```

```python
import functools

import jax
import jax.numpy as jnp
import numpy as np
from jax import lax
from jax.experimental import pallas as pl
from jax.experimental.pallas import tpu as pltpu
from jax.sharding import PartitionSpec as P

NORM_EPS = 1e-5
ROPE_BASE = 500000.0
MESH = pl.DeviceIdType.MESH

ROWS = 256
HALF = 128
TILE = 512
SLOTS = 6
KV_SLOTS = 5
X_SLOTS = 4
KV_TOK = 32


def kernel(cfg, lens_ref, table_ref, gain_ref, x_in, wq, wk, wv, wo, wg, wu, wd, kc, vc, x_out,
           xs, a_s, q_s, k_s, v_s, att_s, u_s, raws, saved, cos_ref, sin_ref, len_s, len4, sidx, s_s, p_s, o_s, wbuf, wobuf, kbuf, vbuf, ybuf, irecv, rown, xrecv,
           wsem, wosem, kvsem, xsem, isend, irsem, xsend, xrsem, nsend, nrsem, osem):
    layers, tokens, width, seq, kv_heads = cfg
    tok_rows = seq * kv_heads * 2
    chunks = tokens // ROWS
    stages = layers * chunks
    n_dn = width // TILE
    n_ff = wg.shape[2] // TILE
    n_q = wq.shape[2] // TILE
    n_w = n_q + 2 + 2 * n_ff + n_dn
    n_kv = ROWS // KV_TOK
    n_qkv = n_q + 2
    all_w, all_kv = stages * n_w - n_qkv, stages * n_kv

    tp = lax.axis_index("tp")
    core = lax.rem(tp, 2)
    sib = tp + 1 - 2 * core
    partner = lax.rem(tp + 2, 4)
    own_row = pl.multiple_of(core * HALF, HALF)
    sib_row = pl.multiple_of((1 - core) * HALF, HALF)

    def w_start(gt):
        t = gt + n_qkv * lax.div(lax.div(gt, n_w) + stages - 1, stages)
        st = lax.div(t, n_w)
        t = t - st * n_w
        layer = lax.div(st, chunks)
        slot = lax.rem(gt, SLOTS)

        def put(src):
            pltpu.make_async_copy(src, wbuf.at[slot], wsem.at[slot]).start()

        def cols(i):
            return pl.ds(pl.multiple_of(i * TILE, TILE), TILE)

        f = t - (n_q + 2)

        @pl.when(t < n_q)
        def _():
            put(wq.at[layer, :, cols(t)])

        @pl.when(t == n_q)
        def _():
            put(wk.at[layer])

        @pl.when(t == n_q + 1)
        def _():
            put(wv.at[layer])

        @pl.when((f >= 0) & (f < 2 * n_ff) & (lax.rem(f + 2, 2) == 0))
        def _():
            put(wg.at[layer, :, cols(lax.div(f, 2))])

        @pl.when((f >= 0) & (f < 2 * n_ff) & (lax.rem(f + 2, 2) == 1))
        def _():
            put(wu.at[layer, :, cols(lax.div(f, 2))])

        @pl.when(f >= 2 * n_ff)
        def _():
            put(wd.at[layer, :, cols(f - 2 * n_ff)])

    def w_next(gt):
        @pl.when(gt + SLOTS < all_w)
        def _():
            w_start(gt + SLOTS)

    def w_wait(gt):
        slot = lax.rem(gt, SLOTS)
        pltpu.make_async_copy(wk.at[0], wbuf.at[slot], wsem.at[slot]).wait()
        return slot

    def wo_copy(layer, j):
        cols = pl.ds(pl.multiple_of(j * TILE, TILE), TILE)
        return pltpu.make_async_copy(wo.at[layer, :, cols], wobuf.at[j], wosem.at[j])

    def kv_copies(gb):
        st = lax.div(gb, n_kv)
        b = gb - st * n_kv
        layer = lax.div(st, chunks)
        tok = layer * tokens + (st - layer * chunks) * ROWS + b * KV_TOK
        slot = lax.rem(gb, KV_SLOTS)
        rows = pl.ds(pl.multiple_of(tok * tok_rows, KV_TOK * tok_rows), KV_TOK * tok_rows)
        return (pltpu.make_async_copy(kc.at[rows], kbuf.at[slot], kvsem.at[0, slot]),
                pltpu.make_async_copy(vc.at[rows], vbuf.at[slot], kvsem.at[1, slot]))

    def chip_copy(gj):
        slot = lax.rem(gj, X_SLOTS)
        return pltpu.make_async_remote_copy(
            src_ref=ybuf.at[slot, pl.ds(sib_row, HALF)], dst_ref=irecv.at[slot], send_sem=isend.at[slot],
            recv_sem=irsem.at[slot], device_id={"tp": sib}, device_id_type=MESH)

    def link_copy(par, j):
        return pltpu.make_async_remote_copy(
            src_ref=rown.at[j], dst_ref=xrecv.at[par, j], send_sem=xsend.at[j],
            recv_sem=xrsem.at[par, j], device_id={"tp": partner}, device_id_type=MESH)

    def x_piece(par, row, j):
        return xs.at[pl.ds(pl.multiple_of(par * ROWS + row, HALF), HALF), pl.ds(pl.multiple_of(j * TILE, TILE), TILE)]

    def new_copy(par, j):
        piece = x_piece(par, own_row, j)
        return pltpu.make_async_remote_copy(
            src_ref=piece, dst_ref=piece, send_sem=nsend.at[par, j],
            recv_sem=nrsem.at[par, j], device_id={"tp": sib}, device_id_type=MESH)

    def chip_sum(st, j):
        gj = st * n_dn + j
        slot = lax.rem(gj, X_SLOTS)
        chip_copy(gj).wait()
        rown[j] = (ybuf[slot, pl.ds(own_row, HALF)] + irecv[slot]).astype(jnp.bfloat16)
        link_copy(lax.rem(st, chunks), j).start()

    def finish(par):
        def step(j, _):
            link_copy(par, j).wait()
            piece = x_piece(par, own_row, j)
            total = rown[j].astype(jnp.float32) + xrecv[par, j].astype(jnp.float32)
            piece[...] = (piece[...].astype(jnp.float32) + total).astype(jnp.bfloat16)
            new_copy(par, j).start()
            return 0

        lax.fori_loop(0, n_dn, step, 0)

    def new_wait(par):
        def step(j, _):
            new_copy(par, j).wait()
            return 0

        lax.fori_loop(0, n_dn, step, 0)

    def x_copy(c):
        rows = pl.ds(pl.multiple_of(c * ROWS, ROWS), ROWS)
        return pltpu.make_async_copy(x_in.at[rows], xs.at[rows], xsem.at[c])

    def out_copy(c):
        rows = pl.ds(c * ROWS, ROWS)
        return pltpu.make_async_copy(xs.at[rows], x_out.at[rows], osem.at[c])

    for c in range(chunks):
        x_copy(c).start()
    for g in range(n_qkv):
        w_start(jnp.int32(g))
    for g in range(KV_SLOTS):
        for cp in kv_copies(jnp.int32(g)):
            cp.start()
    for g in range(n_qkv, SLOTS):
        w_start(jnp.int32(g))

    barrier = pltpu.get_barrier_semaphore()
    for other in (sib, partner):
        pl.semaphore_signal(barrier, inc=1, device_id={"tp": other}, device_id_type=MESH)
    pl.semaphore_wait(barrier, 2)

    n_key = 2 * tok_rows
    lane = lax.broadcasted_iota(jnp.int32, (KV_TOK * 4, n_key), 1)
    row = lax.rem(lax.broadcasted_iota(jnp.int32, (KV_TOK * 4, n_key), 0), 8)
    per = 2 * kv_heads
    match = (lax.div(lane, tok_rows) == lax.div(row, 4)) & (lax.rem(lane, kv_heads) == lax.div(lax.rem(row, 4), 2)) & (lax.rem(lane, per) < kv_heads)
    sidx[...] = jnp.where(match, lax.rem(lax.div(lane, per), seq), 2 * seq).astype(jnp.float32)
    pick = lax.broadcasted_iota(jnp.int32, (seq, tokens), 0) == lens_ref[...]
    angles = lax.dot_general(pick.astype(jnp.float32), table_ref[...], (((0,), (0,)), ((), ())),
                             precision=lax.Precision.HIGHEST, preferred_element_type=jnp.float32)
    half = angles.shape[1] // 3
    cos_ref[...], sin_ref[...], len_s[...] = angles[:, :half], angles[:, half:2 * half], angles[:, 2 * half:]

    def rope(y, dst, first_head, copies, rows):
        cos, sin = cos_ref[rows], sin_ref[rows]
        for h in range(TILE // 256):
            first = y[:, h * 256:h * 256 + 128].astype(jnp.float32)
            second = y[:, h * 256 + 128:h * 256 + 256].astype(jnp.float32)
            lo = (first * cos - second * sin).astype(jnp.bfloat16).astype(jnp.float32)
            hi = (second * cos + first * sin).astype(jnp.bfloat16).astype(jnp.float32)
            for i in range(copies):
                at = pl.ds((first_head + h) * copies + i, ROWS, 4)
                dst[0, at] = lo
                dst[1, at] = hi

    def dot(a, b):
        return jnp.dot(a, b, preferred_element_type=jnp.float32)

    scale = 1.0 / 16.0
    n_pair = KV_TOK // 2
    n_row = KV_TOK * 4

    def roll(x, by):
        return jnp.concatenate([pltpu.roll(x[:, i:i + 128], by % 128, axis=1) for i in (0, 128)], 1)

    def block_rows(b):
        return pl.ds(pl.multiple_of(b * n_row, n_row), n_row)

    def logits(side, st, b):
        slot = lax.rem(st * n_kv + b, KV_SLOTS)
        q = [(q_s[j, block_rows(b)] * scale).reshape(n_pair, 8, 128) for j in range(2)]
        qq = jnp.concatenate(q, 1).astype(jnp.bfloat16)
        for g in range(n_pair):
            keys = kbuf[slot, pl.ds(g * n_key, n_key)]
            s_s[side][g * 16:g * 16 + 16] = lax.dot_general(
                qq[g], keys, (((1,), (1,)), ((), ())), preferred_element_type=jnp.float32)

    def soft(side, c, b):
        s2 = s_s[side][...].reshape(n_pair, 2, 8, n_key)
        s = s2[:, 0].reshape(n_row, n_key) + roll(s2[:, 1].reshape(n_row, n_key), -2)
        r = block_rows(b)
        self_logit = jnp.sum(q_s[0, r] * k_s[0, r] + q_s[1, r] * k_s[1, r], axis=-1, keepdims=True) * scale
        keep = sidx[...] < len4[r, :1]
        s = jnp.where(keep, s, -jnp.inf)
        peak = jnp.maximum(jnp.max(s, axis=-1, keepdims=True), self_logit)
        w = jnp.exp(s - peak)
        sw = jnp.exp(self_logit - peak)
        inv = 1.0 / (jnp.sum(w, axis=-1, keepdims=True) + sw)
        p = w * inv
        pp = jnp.concatenate([p.reshape(n_pair, 8, n_key), roll(p, 2).reshape(n_pair, 8, n_key)], 1)
        p_s[side][...] = pp.reshape(2 * n_row, n_key).astype(jnp.bfloat16)
        sp = (sw * inv).astype(jnp.bfloat16).astype(jnp.float32)
        for j in range(2):
            o_s[side][j] = sp * v_s[j, r]

    def mix(side, st, b):
        slot = lax.rem(st * n_kv + b, KV_SLOTS)
        base = pl.multiple_of(b * n_row, n_row)
        for g in range(n_pair):
            o2 = dot(p_s[side][g * 16:g * 16 + 16], vbuf[slot, pl.ds(g * n_key, n_key)])
            for j in range(2):
                q_s[j, pl.ds(base + g * 8, 8)] = o2[j * 8:j * 8 + 8] + o_s[side][j, g * 8:g * 8 + 8]

    def k_next(gb):
        @pl.when(gb + KV_SLOTS < all_kv)
        def _():
            kv_copies(gb + KV_SLOTS)[0].start()

    def v_next(gb):
        @pl.when(gb + KV_SLOTS < all_kv)
        def _():
            kv_copies(gb + KV_SLOTS)[1].start()

    def swiglu(side, i):
        g = raws[2 * side][...].astype(jnp.float32)
        u = raws[2 * side + 1][...].astype(jnp.float32)
        u_s[:, pl.ds(pl.multiple_of(i * TILE, TILE), TILE)] = (g * (1.0 / (1.0 + jnp.exp(-g))) * u).astype(jnp.bfloat16)

    def norm_rows(to, chunk, layer, i):
        gains = gain_ref[...].astype(jnp.float32)
        gain = gains[:1]
        for other in range(1, layers):
            gain = jnp.where(layer == other, gains[other:other + 1], gain)
        src = pl.ds(pl.multiple_of(chunk * ROWS + i * 16, 16), 16)
        dst = pl.ds(pl.multiple_of(i * 16, 16), 16)
        parts = range(0, width, 256)
        total = jnp.zeros((16, 256), jnp.float32)
        for p in parts:
            x = xs[src, p:p + 256].astype(jnp.float32)
            total = total + x * x
        inv = lax.rsqrt(jnp.sum(total, axis=-1, keepdims=True) / width + NORM_EPS)
        for p in parts:
            x = xs[src, p:p + 256].astype(jnp.float32)
            to[dst, p:p + 256] = (x * inv * gain[:, p:p + 256]).astype(jnp.bfloat16)

    def stage(st, _):
        layer = lax.div(st, chunks)
        c = st - layer * chunks
        par = c
        rows = pl.ds(pl.multiple_of(c * ROWS, ROWS), ROWS)
        wf0 = st * n_w + n_qkv * (1 - lax.div(st + stages - 1, stages))
        w0 = wf0 - n_qkv

        def products(a, first, to):
            for i in range(2):
                to[first + i][...] = dot(a[...], wbuf[lax.rem(w0 + first + i, SLOTS)]).astype(jnp.bfloat16)

        def rope_q():
            rope(raws[0], q_s, 0, 1, rows)
            rope(raws[1], q_s, 2, 1, rows)

        @pl.when(st != 1)
        def _():
            for i in range(2):
                w_wait(w0 + i)
            products(a_s, 0, raws)

            @pl.when(st == 0)
            def _():
                products(u_s, 0, saved)

            w_next(w0)
            w_next(w0 + 1)

        @pl.when(st >= 1)
        def _():
            for j in range(n_dn - 2, n_dn):
                chip_sum(st - 1, j)

        @pl.when(st != 1)
        def _():
            for i in range(2, 4):
                w_wait(w0 + i)
            rope_q()
            products(a_s, 2, raws)

            @pl.when(st == 0)
            def _():
                products(u_s, 2, saved)

        @pl.when(st == 1)
        def _():
            for i in range(4):
                raws[i][...] = saved[i][...]
            rope_q()

        b0 = st * n_kv
        kv_copies(b0)[0].wait()
        kv_copies(b0 + 1)[0].wait()
        logits(0, st, 0)
        rope(raws[2], k_s, 0, 2, rows)
        v = raws[3][...].astype(jnp.float32)
        for h in range(4):
            for j in range(2):
                v_s[j, pl.ds(h, ROWS, 4)] = v[:, (h // 2) * 256 + j * 128:(h // 2) * 256 + j * 128 + 128]
            len4[pl.ds(h, ROWS, 4)] = len_s[rows]
        soft(0, c, 0)
        logits(1, st, 1)
        k_next(b0)
        k_next(b0 + 1)

        def half(side, b):
            kv_copies(b0 + b - 1)[1].wait()
            kv_copies(b0 + b + 1)[0].wait()
            mix(1 - side, st, b - 1)
            soft(side, c, b)
            logits(1 - side, st, b + 1)
            v_next(b0 + b - 1)
            k_next(b0 + b + 1)

        def block(i, _):
            for side, at in ((1, 1), (0, 2)):
                half(side, 2 * i + at)

                @pl.when((i == n_kv // 2 - 2) & (st != 1))
                def _():
                    w_next(w0 + n_q + at - 1)

            return 0

        lax.fori_loop(0, n_kv // 2 - 1, block, 0)
        kv_copies(b0 + n_kv - 2)[1].wait()
        kv_copies(b0 + n_kv - 1)[1].wait()
        mix(0, st, n_kv - 2)
        soft(1, c, n_kv - 1)
        mix(1, st, n_kv - 1)
        for h in range(4):
            for j in range(2):
                at = h * 256 + j * 128
                att_s[:, at:at + 128] = q_s[j, pl.ds(h, ROWS, 4)].astype(jnp.bfloat16)
        v_next(b0 + n_kv - 2)
        v_next(b0 + n_kv - 1)

        def ff_tile(side, i):
            gt = wf0 + 2 * i
            s0, s1 = w_wait(gt), w_wait(gt + 1)
            swiglu(1 - side, lax.rem(i + n_ff - 1, n_ff))
            raws[2 * side][...] = dot(a_s[...], wbuf[s0]).astype(jnp.bfloat16)
            raws[2 * side + 1][...] = dot(a_s[...], wbuf[s1]).astype(jnp.bfloat16)
            w_next(gt)
            w_next(gt + 1)

            @pl.when(st == 0)
            def _():
                wo_copy(0, i).start()

        def ff(i, _):
            ff_tile(0, 2 * i)
            ff_tile(1, 2 * i + 1)
            return 0

        lax.fori_loop(0, n_ff // 2, ff, 0)
        if n_ff % 2:
            ff_tile(0, n_ff - 1)
        swiglu((n_ff - 1) % 2, n_ff - 1)

        @pl.when(st >= 1)
        def _():
            finish(1 - par)

        following = st + 1
        turn = lax.rem(following, chunks)
        source = turn + lax.div(following, stages) * (c - turn)
        n_norm = 4
        groups = ROWS // 16 // n_norm

        def down(j, with_norm):
            gt = wf0 + 2 * n_ff + j
            s0 = w_wait(gt)

            @pl.when(c == 0)
            def _():
                wo_copy(layer, j).wait()

            @pl.when(j >= 2)
            def _():
                chip_sum(st, j - 2)

            gj = st * n_dn + j
            if with_norm:
                for i in range(groups):
                    norm_rows(a_s, source, lax.div(following, chunks), (j - (n_dn - n_norm)) * groups + i)
            ybuf[lax.rem(gj, X_SLOTS)] = dot(u_s[...], wbuf[s0]) + dot(att_s[...], wobuf[j])
            chip_copy(gj).start()
            w_next(gt)

            @pl.when((c == chunks - 1) & (layer < layers - 1))
            def _():
                wo_copy(layer + 1, j).start()

        def down_plain(j, _):
            down(j, False)
            return 0

        def down_norm(j, _):
            down(j, True)
            return 0

        lax.fori_loop(0, n_dn - n_norm, down_plain, 0)

        @pl.when((following >= chunks) & (following < stages))
        def _():
            new_wait(turn)

        lax.fori_loop(n_dn - n_norm, n_dn, down_norm, 0)
        return 0

    for c, to in enumerate((a_s, u_s)):
        x_copy(c).wait()

        def first(i, _):
            norm_rows(to, c, 0, 2 * i)
            norm_rows(to, c, 0, 2 * i + 1)
            return 0

        lax.fori_loop(0, ROWS // 32, first, 0)
    for raw in raws:
        raw[...] = jnp.zeros_like(raw)
    lax.fori_loop(0, stages, stage, 0)

    last = (stages - 1) % chunks
    for j in range(n_dn - 2, n_dn):
        chip_sum(stages - 1, j)
    new_wait(1 - last)
    out_copy(1 - last).start()
    finish(last)
    new_wait(last)
    out_copy(last).start()
    for c in range(chunks):
        out_copy(c).wait()


def solution(mesh):
    arg_specs = (P('dp', None), P('dp'), P(), P(None, None, 'tp'), P(None, None, 'tp'), P(None, None, 'tp'), P(None, 'tp', None), P(None, None, 'tp'), P(None, None, 'tp'), P(None, 'tp', None), P(None, 'dp', None, 'tp', None), P(None, 'dp', None, 'tp', None))

    def per_device(x_in, lengths, norm_gain, w_q, w_k, w_v, w_o, w_gate, w_up, w_down, k_cache, v_cache):
        layers, tokens, seq, kv_heads, head = k_cache.shape
        width = x_in.shape[1]
        half = head // 2
        inv_freq = 1.0 / (np.float32(ROPE_BASE) ** (np.arange(0, head, 2).astype(np.float32) / np.float32(head)))
        pos = np.arange(seq).astype(np.float32)[:, None]
        angles = pos * inv_freq[None, :].astype(np.float32)
        table = np.concatenate([np.cos(angles), np.sin(angles), pos + 0 * angles], 1).astype(np.float32)

        def rows_of(cache):
            r = cache.reshape(layers * tokens * seq, kv_heads, 2, half).transpose(0, 2, 1, 3)
            return r.reshape(layers * tokens * seq * kv_heads * 2, half)

        tok_rows = seq * kv_heads * 2
        n_dn = width // TILE
        vm = pl.BlockSpec(memory_space=pltpu.VMEM)
        hbm = pl.BlockSpec(memory_space=pl.ANY)
        bf, f32 = jnp.bfloat16, jnp.float32
        dma = pltpu.SemaphoreType.DMA
        return pl.pallas_call(
            functools.partial(kernel, (layers, tokens, width, seq, kv_heads)),
            out_shape=jax.ShapeDtypeStruct(x_in.shape, bf),
            in_specs=[vm] * 3 + [hbm] * 10,
            out_specs=hbm,
            scratch_shapes=[
                pltpu.VMEM((tokens, width), bf),
                pltpu.VMEM((ROWS, width), bf),
                pltpu.VMEM((2, 4 * ROWS, half), f32),
                pltpu.VMEM((2, 4 * ROWS, half), f32),
                pltpu.VMEM((2, 4 * ROWS, half), f32),
                pltpu.VMEM((ROWS, w_q.shape[2]), bf),
                pltpu.VMEM((ROWS, w_gate.shape[2]), bf),
                [pltpu.VMEM((ROWS, TILE), bf)] * 4,
                [pltpu.VMEM((ROWS, TILE), bf)] * 4,
                pltpu.VMEM((tokens, half), f32),
                pltpu.VMEM((tokens, half), f32),
                pltpu.VMEM((tokens, half), f32),
                pltpu.VMEM((4 * ROWS, half), f32),
                pltpu.VMEM((4 * KV_TOK, 2 * tok_rows), f32),
                [pltpu.VMEM((8 * KV_TOK, 2 * tok_rows), f32)] * 2,
                [pltpu.VMEM((8 * KV_TOK, 2 * tok_rows), bf)] * 2,
                [pltpu.VMEM((2, 4 * KV_TOK, half), f32)] * 2,
                pltpu.VMEM((SLOTS, width, TILE), bf),
                pltpu.VMEM((n_dn, w_o.shape[1], TILE), bf),
                pltpu.VMEM((KV_SLOTS, KV_TOK * tok_rows, half), bf),
                pltpu.VMEM((KV_SLOTS, KV_TOK * tok_rows, half), bf),
                pltpu.VMEM((X_SLOTS, ROWS, TILE), f32),
                pltpu.VMEM((X_SLOTS, HALF, TILE), f32),
                pltpu.VMEM((n_dn, HALF, TILE), bf),
                pltpu.VMEM((2, n_dn, HALF, TILE), bf),
                dma((SLOTS,)), dma((n_dn,)), dma((2, KV_SLOTS)), dma((2,)),
                dma((X_SLOTS,)), dma((X_SLOTS,)), dma((n_dn,)), dma((2, n_dn)), dma((2, n_dn)), dma((2, n_dn)), dma((2,)),
            ],
            compiler_params=pltpu.CompilerParams(
                collective_id=0, has_side_effects=True, vmem_limit_bytes=67_043_328),
            name="decoder",
        )(lengths.reshape(1, tokens), jnp.asarray(table), norm_gain, x_in, w_q, w_k, w_v, w_o, w_gate, w_up, w_down,
          rows_of(k_cache), rows_of(v_cache))

    return jax.shard_map(per_device, mesh=mesh, in_specs=arg_specs, out_specs=P('dp', None), check_vma=False)
```

```python
import functools

import jax
import jax.numpy as jnp
import numpy as np
from jax import lax
from jax.experimental import pallas as pl
from jax.experimental.pallas import tpu as pltpu
from jax.sharding import PartitionSpec as P

NORM_EPS = 1e-5
ROPE_BASE = 500000.0
MESH = pl.DeviceIdType.MESH

ROWS = 256
HALF = 128
TILE = 512
SLOTS = 7
KV_SLOTS = 4
X_SLOTS = 4
KV_TOK = 32


def kernel(cfg, lens_ref, table_ref, gain_ref, x_in, wq, wk, wv, wo, wg, wu, wd, kc, vc, x_out,
           xs, a_s, q_s, k_s, v_s, att_s, u_s, raws, cos_ref, sin_ref, len_s, len4, sidx, s_s, p_s, o_s, wbuf, wobuf, kbuf, vbuf, ybuf, irecv, rown, xrecv,
           wsem, wosem, kvsem, xsem, isend, irsem, xsend, xrsem, nsend, nrsem, osem):
    layers, tokens, width, seq, kv_heads = cfg
    tok_rows = seq * kv_heads * 2
    chunks = tokens // ROWS
    stages = layers * chunks
    n_dn = width // TILE
    n_ff = wg.shape[2] // TILE
    n_q = wq.shape[2] // TILE
    n_w = n_q + 2 + 2 * n_ff + n_dn
    n_kv = ROWS // KV_TOK
    all_w, all_kv = stages * n_w, stages * n_kv

    tp = lax.axis_index("tp")
    core = lax.rem(tp, 2)
    sib = tp + 1 - 2 * core
    partner = lax.rem(tp + 2, 4)
    own_row = pl.multiple_of(core * HALF, HALF)
    sib_row = pl.multiple_of((1 - core) * HALF, HALF)

    def w_start(gt):
        st = lax.div(gt, n_w)
        t = gt - st * n_w
        layer = lax.div(st, chunks)
        slot = lax.rem(gt, SLOTS)

        def put(src):
            pltpu.make_async_copy(src, wbuf.at[slot], wsem.at[slot]).start()

        def cols(i):
            return pl.ds(pl.multiple_of(i * TILE, TILE), TILE)

        f = t - (n_q + 2)

        @pl.when(t < n_q)
        def _():
            put(wq.at[layer, :, cols(t)])

        @pl.when(t == n_q)
        def _():
            put(wk.at[layer])

        @pl.when(t == n_q + 1)
        def _():
            put(wv.at[layer])

        @pl.when((f >= 0) & (f < 2 * n_ff) & (lax.rem(f + 2, 2) == 0))
        def _():
            put(wg.at[layer, :, cols(lax.div(f, 2))])

        @pl.when((f >= 0) & (f < 2 * n_ff) & (lax.rem(f + 2, 2) == 1))
        def _():
            put(wu.at[layer, :, cols(lax.div(f, 2))])

        @pl.when(f >= 2 * n_ff)
        def _():
            put(wd.at[layer, :, cols(f - 2 * n_ff)])

    def w_next(gt):
        @pl.when(gt + SLOTS < all_w)
        def _():
            w_start(gt + SLOTS)

    def w_wait(gt):
        slot = lax.rem(gt, SLOTS)
        pltpu.make_async_copy(wk.at[0], wbuf.at[slot], wsem.at[slot]).wait()
        return slot

    def wo_copy(layer, j):
        cols = pl.ds(pl.multiple_of(j * TILE, TILE), TILE)
        return pltpu.make_async_copy(wo.at[layer, :, cols], wobuf.at[j], wosem.at[j])

    def kv_copies(gb):
        st = lax.div(gb, n_kv)
        b = gb - st * n_kv
        layer = lax.div(st, chunks)
        tok = layer * tokens + (st - layer * chunks) * ROWS + b * KV_TOK
        slot = lax.rem(gb, KV_SLOTS)
        rows = pl.ds(pl.multiple_of(tok * tok_rows, KV_TOK * tok_rows), KV_TOK * tok_rows)
        return (pltpu.make_async_copy(kc.at[rows], kbuf.at[slot], kvsem.at[0, slot]),
                pltpu.make_async_copy(vc.at[rows], vbuf.at[slot], kvsem.at[1, slot]))

    def chip_copy(gj):
        slot = lax.rem(gj, X_SLOTS)
        return pltpu.make_async_remote_copy(
            src_ref=ybuf.at[slot, pl.ds(sib_row, HALF)], dst_ref=irecv.at[slot], send_sem=isend.at[slot],
            recv_sem=irsem.at[slot], device_id={"tp": sib}, device_id_type=MESH)

    def link_copy(par, j):
        return pltpu.make_async_remote_copy(
            src_ref=rown.at[j], dst_ref=xrecv.at[par, j], send_sem=xsend.at[j],
            recv_sem=xrsem.at[par, j], device_id={"tp": partner}, device_id_type=MESH)

    def x_piece(par, row, j):
        return xs.at[pl.ds(pl.multiple_of(par * ROWS + row, HALF), HALF), pl.ds(pl.multiple_of(j * TILE, TILE), TILE)]

    def new_copy(par, j):
        piece = x_piece(par, own_row, j)
        return pltpu.make_async_remote_copy(
            src_ref=piece, dst_ref=piece, send_sem=nsend.at[par, j],
            recv_sem=nrsem.at[par, j], device_id={"tp": sib}, device_id_type=MESH)

    def chip_sum(st, j):
        gj = st * n_dn + j
        slot = lax.rem(gj, X_SLOTS)
        chip_copy(gj).wait()
        rown[j] = (ybuf[slot, pl.ds(own_row, HALF)] + irecv[slot]).astype(jnp.bfloat16)
        link_copy(lax.rem(st, chunks), j).start()

    def finish(par):
        def step(j, _):
            link_copy(par, j).wait()
            piece = x_piece(par, own_row, j)
            total = rown[j].astype(jnp.float32) + xrecv[par, j].astype(jnp.float32)
            piece[...] = (piece[...].astype(jnp.float32) + total).astype(jnp.bfloat16)
            new_copy(par, j).start()
            return 0

        lax.fori_loop(0, n_dn, step, 0)

    def new_wait(par):
        def step(j, _):
            new_copy(par, j).wait()
            return 0

        lax.fori_loop(0, n_dn, step, 0)

    def x_copy(c):
        rows = pl.ds(pl.multiple_of(c * ROWS, ROWS), ROWS)
        return pltpu.make_async_copy(x_in.at[rows], xs.at[rows], xsem.at[c])

    def out_copy(c):
        rows = pl.ds(c * ROWS, ROWS)
        return pltpu.make_async_copy(xs.at[rows], x_out.at[rows], osem.at[c])

    x_copy(0).start()
    for g in range(SLOTS):
        w_start(jnp.int32(g))
    for g in range(KV_SLOTS):
        for cp in kv_copies(jnp.int32(g)):
            cp.start()
    for j in range(n_dn):
        wo_copy(0, j).start()
    for c in range(1, chunks):
        x_copy(c).start()

    barrier = pltpu.get_barrier_semaphore()
    for other in (sib, partner):
        pl.semaphore_signal(barrier, inc=1, device_id={"tp": other}, device_id_type=MESH)
    pl.semaphore_wait(barrier, 2)

    n_key = 2 * tok_rows
    lane = lax.broadcasted_iota(jnp.int32, (KV_TOK * 4, n_key), 1)
    row = lax.rem(lax.broadcasted_iota(jnp.int32, (KV_TOK * 4, n_key), 0), 8)
    per = 2 * kv_heads
    match = (lax.div(lane, tok_rows) == lax.div(row, 4)) & (lax.rem(lane, kv_heads) == lax.div(lax.rem(row, 4), 2)) & (lax.rem(lane, per) < kv_heads)
    sidx[...] = jnp.where(match, lax.rem(lax.div(lane, per), seq), 2 * seq).astype(jnp.float32)
    pick = lax.broadcasted_iota(jnp.int32, (seq, tokens), 0) == lens_ref[...]
    angles = lax.dot_general(pick.astype(jnp.float32), table_ref[...], (((0,), (0,)), ((), ())),
                             precision=lax.Precision.HIGHEST, preferred_element_type=jnp.float32)
    half = angles.shape[1] // 3
    cos_ref[...], sin_ref[...], len_s[...] = angles[:, :half], angles[:, half:2 * half], angles[:, 2 * half:]

    def rope(y, dst, first_head, copies, rows):
        cos, sin = cos_ref[rows], sin_ref[rows]
        for h in range(TILE // 256):
            first = y[:, h * 256:h * 256 + 128].astype(jnp.float32)
            second = y[:, h * 256 + 128:h * 256 + 256].astype(jnp.float32)
            lo = (first * cos - second * sin).astype(jnp.bfloat16).astype(jnp.float32)
            hi = (second * cos + first * sin).astype(jnp.bfloat16).astype(jnp.float32)
            for i in range(copies):
                at = pl.ds((first_head + h) * copies + i, ROWS, 4)
                dst[0, at] = lo
                dst[1, at] = hi

    def dot(a, b):
        return jnp.dot(a, b, preferred_element_type=jnp.float32)

    scale = 1.0 / 16.0
    n_pair = KV_TOK // 2
    n_row = KV_TOK * 4

    def roll(x, by):
        return jnp.concatenate([pltpu.roll(x[:, i:i + 128], by % 128, axis=1) for i in (0, 128)], 1)

    def block_rows(b):
        return pl.ds(pl.multiple_of(b * n_row, n_row), n_row)

    def logits(side, st, b):
        slot = lax.rem(st * n_kv + b, KV_SLOTS)
        q = [(q_s[j, block_rows(b)] * scale).reshape(n_pair, 8, 128) for j in range(2)]
        qq = jnp.concatenate(q, 1).astype(jnp.bfloat16)
        for g in range(n_pair):
            keys = kbuf[slot, pl.ds(g * n_key, n_key)]
            s_s[side][g * 16:g * 16 + 16] = lax.dot_general(
                qq[g], keys, (((1,), (1,)), ((), ())), preferred_element_type=jnp.float32)

    def soft(side, c, b):
        s2 = s_s[side][...].reshape(n_pair, 2, 8, n_key)
        s = s2[:, 0].reshape(n_row, n_key) + roll(s2[:, 1].reshape(n_row, n_key), -2)
        r = block_rows(b)
        self_logit = jnp.sum(q_s[0, r] * k_s[0, r] + q_s[1, r] * k_s[1, r], axis=-1, keepdims=True) * scale
        keep = sidx[...] < len4[r, :1]
        s = jnp.where(keep, s, -jnp.inf)
        peak = jnp.maximum(jnp.max(s, axis=-1, keepdims=True), self_logit)
        w = jnp.exp(s - peak)
        sw = jnp.exp(self_logit - peak)
        inv = 1.0 / (jnp.sum(w, axis=-1, keepdims=True) + sw)
        p = w * inv
        pp = jnp.concatenate([p.reshape(n_pair, 8, n_key), roll(p, 2).reshape(n_pair, 8, n_key)], 1)
        p_s[side][...] = pp.reshape(2 * n_row, n_key).astype(jnp.bfloat16)
        sp = (sw * inv).astype(jnp.bfloat16).astype(jnp.float32)
        for j in range(2):
            o_s[side][j] = sp * v_s[j, r]

    def mix(side, st, b):
        slot = lax.rem(st * n_kv + b, KV_SLOTS)
        base = pl.multiple_of(b * n_row, n_row)
        for g in range(n_pair):
            o2 = dot(p_s[side][g * 16:g * 16 + 16], vbuf[slot, pl.ds(g * n_key, n_key)])
            for j in range(2):
                q_s[j, pl.ds(base + g * 8, 8)] = o2[j * 8:j * 8 + 8] + o_s[side][j, g * 8:g * 8 + 8]

    def k_next(gb):
        @pl.when(gb + KV_SLOTS < all_kv)
        def _():
            kv_copies(gb + KV_SLOTS)[0].start()

    def v_next(gb):
        @pl.when(gb + KV_SLOTS < all_kv)
        def _():
            kv_copies(gb + KV_SLOTS)[1].start()

    def swiglu(side, i):
        g = raws[2 * side][...].astype(jnp.float32)
        u = raws[2 * side + 1][...].astype(jnp.float32)
        u_s[:, pl.ds(pl.multiple_of(i * TILE, TILE), TILE)] = (g * (1.0 / (1.0 + jnp.exp(-g))) * u).astype(jnp.bfloat16)

    def norm_rows(chunk, layer, i):
        gains = gain_ref[...].astype(jnp.float32)
        gain = gains[:1]
        for other in range(1, layers):
            gain = jnp.where(layer == other, gains[other:other + 1], gain)
        src = pl.ds(pl.multiple_of(chunk * ROWS + i * 16, 16), 16)
        dst = pl.ds(pl.multiple_of(i * 16, 16), 16)
        parts = range(0, width, 256)
        total = jnp.zeros((16, 256), jnp.float32)
        for p in parts:
            x = xs[src, p:p + 256].astype(jnp.float32)
            total = total + x * x
        inv = lax.rsqrt(jnp.sum(total, axis=-1, keepdims=True) / width + NORM_EPS)
        for p in parts:
            x = xs[src, p:p + 256].astype(jnp.float32)
            a_s[dst, p:p + 256] = (x * inv * gain[:, p:p + 256]).astype(jnp.bfloat16)

    def stage(st, _):
        layer = lax.div(st, chunks)
        c = st - layer * chunks
        par = c
        rows = pl.ds(pl.multiple_of(c * ROWS, ROWS), ROWS)
        w0 = st * n_w

        slots = [w_wait(w0), w_wait(w0 + 1)]
        for i in range(2):
            raws[i][...] = dot(a_s[...], wbuf[slots[i]]).astype(jnp.bfloat16)
        w_next(w0)
        w_next(w0 + 1)

        @pl.when(st >= 1)
        def _():
            for j in range(n_dn - 2, n_dn):
                chip_sum(st - 1, j)

        b0 = st * n_kv
        slots = [w_wait(w0 + 2), w_wait(w0 + 3)]
        kv_copies(b0)[0].wait()
        kv_copies(b0 + 1)[0].wait()
        raws[2][...] = dot(a_s[...], wbuf[slots[0]]).astype(jnp.bfloat16)
        rope(raws[0], q_s, 0, 1, rows)
        rope(raws[1], q_s, 2, 1, rows)
        v = dot(a_s[...], wbuf[slots[1]]).astype(jnp.bfloat16).astype(jnp.float32)
        logits(0, st, 0)
        rope(raws[2], k_s, 0, 2, rows)
        for h in range(4):
            for j in range(2):
                v_s[j, pl.ds(h, ROWS, 4)] = v[:, (h // 2) * 256 + j * 128:(h // 2) * 256 + j * 128 + 128]
            len4[pl.ds(h, ROWS, 4)] = len_s[rows]
        soft(0, c, 0)
        logits(1, st, 1)
        k_next(b0)
        k_next(b0 + 1)

        def half(side, b):
            kv_copies(b0 + b - 1)[1].wait()
            kv_copies(b0 + b + 1)[0].wait()
            mix(1 - side, st, b - 1)
            soft(side, c, b)
            logits(1 - side, st, b + 1)
            v_next(b0 + b - 1)
            k_next(b0 + b + 1)

        def block(i, _):
            half(1, 2 * i + 1)

            @pl.when((i == 0) | (i == 2))
            def _():
                w_next(w0 + n_q + lax.div(i, 2))

            half(0, 2 * i + 2)
            return 0

        lax.fori_loop(0, n_kv // 2 - 1, block, 0)
        kv_copies(b0 + n_kv - 2)[1].wait()
        kv_copies(b0 + n_kv - 1)[1].wait()
        mix(0, st, n_kv - 2)
        soft(1, c, n_kv - 1)
        mix(1, st, n_kv - 1)
        for h in range(4):
            for j in range(2):
                at = h * 256 + j * 128
                att_s[:, at:at + 128] = q_s[j, pl.ds(h, ROWS, 4)].astype(jnp.bfloat16)
        v_next(b0 + n_kv - 2)
        v_next(b0 + n_kv - 1)

        def ff_dots(side, i):
            gt = w0 + n_q + 2 + 2 * i
            raws[2 * side][...] = dot(a_s[...], wbuf[lax.rem(gt, SLOTS)]).astype(jnp.bfloat16)
            raws[2 * side + 1][...] = dot(a_s[...], wbuf[lax.rem(gt + 1, SLOTS)]).astype(jnp.bfloat16)

        def ff(i, _):
            gt = w0 + n_q + 2 + 4 * i
            for k in range(4):
                w_wait(gt + k)
            swiglu(1, lax.rem(2 * i + n_ff - 1, n_ff))
            ff_dots(0, 2 * i)
            swiglu(0, 2 * i)
            ff_dots(1, 2 * i + 1)
            for k in range(4):
                w_next(gt + k)
            return 0

        lax.fori_loop(0, n_ff // 2, ff, 0)
        if n_ff % 2:
            gt = w0 + n_q + 2 + 2 * (n_ff - 1)
            w_wait(gt)
            w_wait(gt + 1)
            swiglu(1, n_ff - 2)
            ff_dots(0, n_ff - 1)
            w_next(gt)
            w_next(gt + 1)
        swiglu((n_ff - 1) % 2, n_ff - 1)

        @pl.when(st >= 1)
        def _():
            finish(1 - par)

        following = st + 1
        turn = lax.rem(following, chunks)
        source = turn + lax.div(following, stages) * (c - turn)
        n_norm = 4
        groups = ROWS // 16 // n_norm

        def down(j, with_norm):
            gt = w0 + n_q + 2 + 2 * n_ff + j
            s0 = w_wait(gt)

            @pl.when(c == 0)
            def _():
                wo_copy(layer, j).wait()

            @pl.when(j >= 2)
            def _():
                chip_sum(st, j - 2)

            gj = st * n_dn + j
            if with_norm:
                for i in range(groups):
                    norm_rows(source, lax.div(following, chunks), (j - (n_dn - n_norm)) * groups + i)
            ybuf[lax.rem(gj, X_SLOTS)] = dot(u_s[...], wbuf[s0]) + dot(att_s[...], wobuf[j])
            chip_copy(gj).start()
            w_next(gt)

            @pl.when((c == chunks - 1) & (layer < layers - 1))
            def _():
                wo_copy(layer + 1, j).start()

        def down_plain(j, _):
            down(j, False)
            return 0

        def down_norm(j, _):
            down(j, True)
            return 0

        lax.fori_loop(0, n_dn - n_norm, down_plain, 0)

        @pl.when(following < chunks)
        def _():
            x_copy(turn).wait()

        @pl.when((following >= chunks) & (following < stages))
        def _():
            new_wait(turn)

        lax.fori_loop(n_dn - n_norm, n_dn, down_norm, 0)
        return 0

    x_copy(0).wait()

    def first(i, _):
        norm_rows(0, 0, 2 * i)
        norm_rows(0, 0, 2 * i + 1)
        return 0

    lax.fori_loop(0, ROWS // 32, first, 0)
    for raw in raws:
        raw[...] = jnp.zeros_like(raw)
    lax.fori_loop(0, stages, stage, 0)

    last = (stages - 1) % chunks
    for j in range(n_dn - 2, n_dn):
        chip_sum(stages - 1, j)
    new_wait(1 - last)
    out_copy(1 - last).start()
    finish(last)
    new_wait(last)
    out_copy(last).start()
    for c in range(chunks):
        out_copy(c).wait()


def solution(mesh):
    arg_specs = (P('dp', None), P('dp'), P(), P(None, None, 'tp'), P(None, None, 'tp'), P(None, None, 'tp'), P(None, 'tp', None), P(None, None, 'tp'), P(None, None, 'tp'), P(None, 'tp', None), P(None, 'dp', None, 'tp', None), P(None, 'dp', None, 'tp', None))

    def per_device(x_in, lengths, norm_gain, w_q, w_k, w_v, w_o, w_gate, w_up, w_down, k_cache, v_cache):
        layers, tokens, seq, kv_heads, head = k_cache.shape
        width = x_in.shape[1]
        half = head // 2
        inv_freq = 1.0 / (np.float32(ROPE_BASE) ** (np.arange(0, head, 2).astype(np.float32) / np.float32(head)))
        pos = np.arange(seq).astype(np.float32)[:, None]
        angles = pos * inv_freq[None, :].astype(np.float32)
        table = np.concatenate([np.cos(angles), np.sin(angles), pos + 0 * angles], 1).astype(np.float32)

        def rows_of(cache):
            r = cache.reshape(layers * tokens * seq, kv_heads, 2, half).transpose(0, 2, 1, 3)
            return r.reshape(layers * tokens * seq * kv_heads * 2, half)

        tok_rows = seq * kv_heads * 2
        n_dn = width // TILE
        vm = pl.BlockSpec(memory_space=pltpu.VMEM)
        hbm = pl.BlockSpec(memory_space=pl.ANY)
        bf, f32 = jnp.bfloat16, jnp.float32
        dma = pltpu.SemaphoreType.DMA
        return pl.pallas_call(
            functools.partial(kernel, (layers, tokens, width, seq, kv_heads)),
            out_shape=jax.ShapeDtypeStruct(x_in.shape, bf),
            in_specs=[vm] * 3 + [hbm] * 10,
            out_specs=hbm,
            scratch_shapes=[
                pltpu.VMEM((tokens, width), bf),
                pltpu.VMEM((ROWS, width), bf),
                pltpu.VMEM((2, 4 * ROWS, half), f32),
                pltpu.VMEM((2, 4 * ROWS, half), f32),
                pltpu.VMEM((2, 4 * ROWS, half), f32),
                pltpu.VMEM((ROWS, w_q.shape[2]), bf),
                pltpu.VMEM((ROWS, w_gate.shape[2]), bf),
                [pltpu.VMEM((ROWS, TILE), bf)] * 4,
                pltpu.VMEM((tokens, half), f32),
                pltpu.VMEM((tokens, half), f32),
                pltpu.VMEM((tokens, half), f32),
                pltpu.VMEM((4 * ROWS, half), f32),
                pltpu.VMEM((4 * KV_TOK, 2 * tok_rows), f32),
                [pltpu.VMEM((8 * KV_TOK, 2 * tok_rows), f32)] * 2,
                [pltpu.VMEM((8 * KV_TOK, 2 * tok_rows), bf)] * 2,
                [pltpu.VMEM((2, 4 * KV_TOK, half), f32)] * 2,
                pltpu.VMEM((SLOTS, width, TILE), bf),
                pltpu.VMEM((n_dn, w_o.shape[1], TILE), bf),
                pltpu.VMEM((KV_SLOTS, KV_TOK * tok_rows, half), bf),
                pltpu.VMEM((KV_SLOTS, KV_TOK * tok_rows, half), bf),
                pltpu.VMEM((X_SLOTS, ROWS, TILE), f32),
                pltpu.VMEM((X_SLOTS, HALF, TILE), f32),
                pltpu.VMEM((n_dn, HALF, TILE), bf),
                pltpu.VMEM((2, n_dn, HALF, TILE), bf),
                dma((SLOTS,)), dma((n_dn,)), dma((2, KV_SLOTS)), dma((2,)),
                dma((X_SLOTS,)), dma((X_SLOTS,)), dma((n_dn,)), dma((2, n_dn)), dma((2, n_dn)), dma((2, n_dn)), dma((2,)),
            ],
            compiler_params=pltpu.CompilerParams(
                collective_id=0, has_side_effects=True, vmem_limit_bytes=67_043_328),
            name="decoder",
        )(lengths.reshape(1, tokens), jnp.asarray(table), norm_gain, x_in, w_q, w_k, w_v, w_o, w_gate, w_up, w_down,
          rows_of(k_cache), rows_of(v_cache))

    return jax.shard_map(per_device, mesh=mesh, in_specs=arg_specs, out_specs=P('dp', None), check_vma=False)
```

```python
import functools

import jax
import jax.numpy as jnp
import numpy as np
from jax import lax
from jax.experimental import pallas as pl
from jax.experimental.pallas import tpu as pltpu
from jax.sharding import PartitionSpec as P

NORM_EPS = 1e-5
ROPE_BASE = 500000.0
MESH = pl.DeviceIdType.MESH

ROWS = 256
HALF = 128
TILE = 512
SLOTS = 6
KV_SLOTS = 5
X_SLOTS = 4
KV_TOK = 32


def kernel(cfg, lens_ref, table_ref, gain_ref, x_in, wq, wk, wv, wo, wg, wu, wd, kc, vc, x_out,
           xs, a_s, q_s, k_s, v_s, att_s, u_s, raws, cos_ref, sin_ref, len_s, len4, sidx, s_s, p_s, o_s, wbuf, wobuf, kbuf, vbuf, ybuf, irecv, rown, xrecv,
           wsem, wosem, kvsem, xsem, isend, irsem, xsend, xrsem, nsend, nrsem, osem):
    layers, tokens, width, seq, kv_heads = cfg
    tok_rows = seq * kv_heads * 2
    chunks = tokens // ROWS
    stages = layers * chunks
    n_dn = width // TILE
    n_ff = wg.shape[2] // TILE
    n_q = wq.shape[2] // TILE
    n_w = n_q + 2 + 2 * n_ff + n_dn
    n_kv = ROWS // KV_TOK
    all_w, all_kv = stages * n_w, stages * n_kv

    tp = lax.axis_index("tp")
    core = lax.rem(tp, 2)
    sib = tp + 1 - 2 * core
    partner = lax.rem(tp + 2, 4)
    own_row = pl.multiple_of(core * HALF, HALF)
    sib_row = pl.multiple_of((1 - core) * HALF, HALF)

    def w_start(gt):
        st = lax.div(gt, n_w)
        t = gt - st * n_w
        layer = lax.div(st, chunks)
        slot = lax.rem(gt, SLOTS)

        def put(src):
            pltpu.make_async_copy(src, wbuf.at[slot], wsem.at[slot]).start()

        def cols(i):
            return pl.ds(pl.multiple_of(i * TILE, TILE), TILE)

        f = t - (n_q + 2)

        @pl.when(t < n_q)
        def _():
            put(wq.at[layer, :, cols(t)])

        @pl.when(t == n_q)
        def _():
            put(wk.at[layer])

        @pl.when(t == n_q + 1)
        def _():
            put(wv.at[layer])

        @pl.when((f >= 0) & (f < 2 * n_ff) & (lax.rem(f + 2, 2) == 0))
        def _():
            put(wg.at[layer, :, cols(lax.div(f, 2))])

        @pl.when((f >= 0) & (f < 2 * n_ff) & (lax.rem(f + 2, 2) == 1))
        def _():
            put(wu.at[layer, :, cols(lax.div(f, 2))])

        @pl.when(f >= 2 * n_ff)
        def _():
            put(wd.at[layer, :, cols(f - 2 * n_ff)])

    def w_next(gt):
        @pl.when(gt + SLOTS < all_w)
        def _():
            w_start(gt + SLOTS)

    def w_wait(gt):
        slot = lax.rem(gt, SLOTS)
        pltpu.make_async_copy(wk.at[0], wbuf.at[slot], wsem.at[slot]).wait()
        return slot

    def wo_copy(layer, j):
        cols = pl.ds(pl.multiple_of(j * TILE, TILE), TILE)
        return pltpu.make_async_copy(wo.at[layer, :, cols], wobuf.at[j], wosem.at[j])

    def kv_copies(gb):
        st = lax.div(gb, n_kv)
        b = gb - st * n_kv
        layer = lax.div(st, chunks)
        tok = layer * tokens + (st - layer * chunks) * ROWS + b * KV_TOK
        slot = lax.rem(gb, KV_SLOTS)
        rows = pl.ds(pl.multiple_of(tok * tok_rows, KV_TOK * tok_rows), KV_TOK * tok_rows)
        return (pltpu.make_async_copy(kc.at[rows], kbuf.at[slot], kvsem.at[0, slot]),
                pltpu.make_async_copy(vc.at[rows], vbuf.at[slot], kvsem.at[1, slot]))

    def chip_copy(gj):
        slot = lax.rem(gj, X_SLOTS)
        return pltpu.make_async_remote_copy(
            src_ref=ybuf.at[slot, pl.ds(sib_row, HALF)], dst_ref=irecv.at[slot], send_sem=isend.at[slot],
            recv_sem=irsem.at[slot], device_id={"tp": sib}, device_id_type=MESH)

    def link_copy(par, j):
        return pltpu.make_async_remote_copy(
            src_ref=rown.at[j], dst_ref=xrecv.at[par, j], send_sem=xsend.at[j],
            recv_sem=xrsem.at[par, j], device_id={"tp": partner}, device_id_type=MESH)

    def x_piece(par, row, j):
        return xs.at[pl.ds(pl.multiple_of(par * ROWS + row, HALF), HALF), pl.ds(pl.multiple_of(j * TILE, TILE), TILE)]

    def new_copy(par, j):
        piece = x_piece(par, own_row, j)
        return pltpu.make_async_remote_copy(
            src_ref=piece, dst_ref=piece, send_sem=nsend.at[par, j],
            recv_sem=nrsem.at[par, j], device_id={"tp": sib}, device_id_type=MESH)

    def chip_sum(st, j):
        gj = st * n_dn + j
        slot = lax.rem(gj, X_SLOTS)
        chip_copy(gj).wait()
        rown[j] = (ybuf[slot, pl.ds(own_row, HALF)] + irecv[slot]).astype(jnp.bfloat16)
        link_copy(lax.rem(st, chunks), j).start()

    def finish(par):
        def step(j, _):
            link_copy(par, j).wait()
            piece = x_piece(par, own_row, j)
            total = rown[j].astype(jnp.float32) + xrecv[par, j].astype(jnp.float32)
            piece[...] = (piece[...].astype(jnp.float32) + total).astype(jnp.bfloat16)
            new_copy(par, j).start()
            return 0

        lax.fori_loop(0, n_dn, step, 0)

    def new_wait(par):
        def step(j, _):
            new_copy(par, j).wait()
            return 0

        lax.fori_loop(0, n_dn, step, 0)

    def x_copy(c):
        rows = pl.ds(pl.multiple_of(c * ROWS, ROWS), ROWS)
        return pltpu.make_async_copy(x_in.at[rows], xs.at[rows], xsem.at[c])

    def out_copy(c):
        rows = pl.ds(c * ROWS, ROWS)
        return pltpu.make_async_copy(xs.at[rows], x_out.at[rows], osem.at[c])

    x_copy(0).start()
    for g in range(n_q + 2):
        w_start(jnp.int32(g))
    for g in range(KV_SLOTS):
        for cp in kv_copies(jnp.int32(g)):
            cp.start()
    for g in range(n_q + 2, SLOTS):
        w_start(jnp.int32(g))
    for c in range(1, chunks):
        x_copy(c).start()

    barrier = pltpu.get_barrier_semaphore()
    for other in (sib, partner):
        pl.semaphore_signal(barrier, inc=1, device_id={"tp": other}, device_id_type=MESH)
    pl.semaphore_wait(barrier, 2)

    n_key = 2 * tok_rows
    lane = lax.broadcasted_iota(jnp.int32, (KV_TOK * 4, n_key), 1)
    row = lax.rem(lax.broadcasted_iota(jnp.int32, (KV_TOK * 4, n_key), 0), 8)
    per = 2 * kv_heads
    match = (lax.div(lane, tok_rows) == lax.div(row, 4)) & (lax.rem(lane, kv_heads) == lax.div(lax.rem(row, 4), 2)) & (lax.rem(lane, per) < kv_heads)
    sidx[...] = jnp.where(match, lax.rem(lax.div(lane, per), seq), 2 * seq).astype(jnp.float32)
    pick = lax.broadcasted_iota(jnp.int32, (seq, tokens), 0) == lens_ref[...]
    angles = lax.dot_general(pick.astype(jnp.float32), table_ref[...], (((0,), (0,)), ((), ())),
                             precision=lax.Precision.HIGHEST, preferred_element_type=jnp.float32)
    half = angles.shape[1] // 3
    cos_ref[...], sin_ref[...], len_s[...] = angles[:, :half], angles[:, half:2 * half], angles[:, 2 * half:]

    def rope(y, dst, first_head, copies, rows):
        cos, sin = cos_ref[rows], sin_ref[rows]
        for h in range(TILE // 256):
            first = y[:, h * 256:h * 256 + 128].astype(jnp.float32)
            second = y[:, h * 256 + 128:h * 256 + 256].astype(jnp.float32)
            lo = (first * cos - second * sin).astype(jnp.bfloat16).astype(jnp.float32)
            hi = (second * cos + first * sin).astype(jnp.bfloat16).astype(jnp.float32)
            for i in range(copies):
                at = pl.ds((first_head + h) * copies + i, ROWS, 4)
                dst[0, at] = lo
                dst[1, at] = hi

    def dot(a, b):
        return jnp.dot(a, b, preferred_element_type=jnp.float32)

    scale = 1.0 / 16.0
    n_pair = KV_TOK // 2
    n_row = KV_TOK * 4

    def roll(x, by):
        return jnp.concatenate([pltpu.roll(x[:, i:i + 128], by % 128, axis=1) for i in (0, 128)], 1)

    def block_rows(b):
        return pl.ds(pl.multiple_of(b * n_row, n_row), n_row)

    def logits(side, st, b):
        slot = lax.rem(st * n_kv + b, KV_SLOTS)
        q = [(q_s[j, block_rows(b)] * scale).reshape(n_pair, 8, 128) for j in range(2)]
        qq = jnp.concatenate(q, 1).astype(jnp.bfloat16)
        for g in range(n_pair):
            keys = kbuf[slot, pl.ds(g * n_key, n_key)]
            s_s[side][g * 16:g * 16 + 16] = lax.dot_general(
                qq[g], keys, (((1,), (1,)), ((), ())), preferred_element_type=jnp.float32)

    def soft(side, c, b):
        s2 = s_s[side][...].reshape(n_pair, 2, 8, n_key)
        s = s2[:, 0].reshape(n_row, n_key) + roll(s2[:, 1].reshape(n_row, n_key), -2)
        r = block_rows(b)
        self_logit = jnp.sum(q_s[0, r] * k_s[0, r] + q_s[1, r] * k_s[1, r], axis=-1, keepdims=True) * scale
        keep = sidx[...] < len4[r, :1]
        s = jnp.where(keep, s, -jnp.inf)
        peak = jnp.maximum(jnp.max(s, axis=-1, keepdims=True), self_logit)
        w = jnp.exp(s - peak)
        sw = jnp.exp(self_logit - peak)
        inv = 1.0 / (jnp.sum(w, axis=-1, keepdims=True) + sw)
        p = w * inv
        pp = jnp.concatenate([p.reshape(n_pair, 8, n_key), roll(p, 2).reshape(n_pair, 8, n_key)], 1)
        p_s[side][...] = pp.reshape(2 * n_row, n_key).astype(jnp.bfloat16)
        sp = (sw * inv).astype(jnp.bfloat16).astype(jnp.float32)
        for j in range(2):
            o_s[side][j] = sp * v_s[j, r]

    def mix(side, st, b):
        slot = lax.rem(st * n_kv + b, KV_SLOTS)
        base = pl.multiple_of(b * n_row, n_row)
        for g in range(n_pair):
            o2 = dot(p_s[side][g * 16:g * 16 + 16], vbuf[slot, pl.ds(g * n_key, n_key)])
            for j in range(2):
                q_s[j, pl.ds(base + g * 8, 8)] = o2[j * 8:j * 8 + 8] + o_s[side][j, g * 8:g * 8 + 8]

    def k_next(gb):
        @pl.when(gb + KV_SLOTS < all_kv)
        def _():
            kv_copies(gb + KV_SLOTS)[0].start()

    def v_next(gb):
        @pl.when(gb + KV_SLOTS < all_kv)
        def _():
            kv_copies(gb + KV_SLOTS)[1].start()

    def swiglu(side, i):
        g = raws[2 * side][...].astype(jnp.float32)
        u = raws[2 * side + 1][...].astype(jnp.float32)
        u_s[:, pl.ds(pl.multiple_of(i * TILE, TILE), TILE)] = (g * (1.0 / (1.0 + jnp.exp(-g))) * u).astype(jnp.bfloat16)

    def norm_rows(chunk, layer, i):
        gains = gain_ref[...].astype(jnp.float32)
        gain = gains[:1]
        for other in range(1, layers):
            gain = jnp.where(layer == other, gains[other:other + 1], gain)
        src = pl.ds(pl.multiple_of(chunk * ROWS + i * 16, 16), 16)
        dst = pl.ds(pl.multiple_of(i * 16, 16), 16)
        parts = range(0, width, 256)
        total = jnp.zeros((16, 256), jnp.float32)
        for p in parts:
            x = xs[src, p:p + 256].astype(jnp.float32)
            total = total + x * x
        inv = lax.rsqrt(jnp.sum(total, axis=-1, keepdims=True) / width + NORM_EPS)
        for p in parts:
            x = xs[src, p:p + 256].astype(jnp.float32)
            a_s[dst, p:p + 256] = (x * inv * gain[:, p:p + 256]).astype(jnp.bfloat16)

    def stage(st, _):
        layer = lax.div(st, chunks)
        c = st - layer * chunks
        par = c
        rows = pl.ds(pl.multiple_of(c * ROWS, ROWS), ROWS)
        w0 = st * n_w

        slots = [w_wait(w0), w_wait(w0 + 1)]
        for i in range(2):
            raws[i][...] = dot(a_s[...], wbuf[slots[i]]).astype(jnp.bfloat16)
        w_next(w0)
        w_next(w0 + 1)

        @pl.when(st >= 1)
        def _():
            for j in range(n_dn - 2, n_dn):
                chip_sum(st - 1, j)

        b0 = st * n_kv
        slots = [w_wait(w0 + 2), w_wait(w0 + 3)]
        kv_copies(b0)[0].wait()
        kv_copies(b0 + 1)[0].wait()
        raws[2][...] = dot(a_s[...], wbuf[slots[0]]).astype(jnp.bfloat16)
        rope(raws[0], q_s, 0, 1, rows)
        rope(raws[1], q_s, 2, 1, rows)
        v = dot(a_s[...], wbuf[slots[1]]).astype(jnp.bfloat16).astype(jnp.float32)
        logits(0, st, 0)
        rope(raws[2], k_s, 0, 2, rows)
        for h in range(4):
            for j in range(2):
                v_s[j, pl.ds(h, ROWS, 4)] = v[:, (h // 2) * 256 + j * 128:(h // 2) * 256 + j * 128 + 128]
            len4[pl.ds(h, ROWS, 4)] = len_s[rows]
        soft(0, c, 0)
        logits(1, st, 1)
        k_next(b0)
        k_next(b0 + 1)

        def half(side, b):
            kv_copies(b0 + b - 1)[1].wait()
            kv_copies(b0 + b + 1)[0].wait()
            mix(1 - side, st, b - 1)
            soft(side, c, b)
            logits(1 - side, st, b + 1)
            v_next(b0 + b - 1)
            k_next(b0 + b + 1)

        def block(i, _):
            for side, at in ((1, 1), (0, 2)):
                half(side, 2 * i + at)

                @pl.when(i == n_kv // 2 - 2)
                def _():
                    w_next(w0 + n_q + at - 1)

            return 0

        lax.fori_loop(0, n_kv // 2 - 1, block, 0)
        kv_copies(b0 + n_kv - 2)[1].wait()
        kv_copies(b0 + n_kv - 1)[1].wait()
        mix(0, st, n_kv - 2)
        soft(1, c, n_kv - 1)
        mix(1, st, n_kv - 1)
        for h in range(4):
            for j in range(2):
                at = h * 256 + j * 128
                att_s[:, at:at + 128] = q_s[j, pl.ds(h, ROWS, 4)].astype(jnp.bfloat16)
        v_next(b0 + n_kv - 2)
        v_next(b0 + n_kv - 1)

        def ff_tile(side, i):
            gt = w0 + n_q + 2 + 2 * i
            s0, s1 = w_wait(gt), w_wait(gt + 1)
            swiglu(1 - side, lax.rem(i + n_ff - 1, n_ff))
            raws[2 * side][...] = dot(a_s[...], wbuf[s0]).astype(jnp.bfloat16)
            raws[2 * side + 1][...] = dot(a_s[...], wbuf[s1]).astype(jnp.bfloat16)
            w_next(gt)
            w_next(gt + 1)

            @pl.when(st == 0)
            def _():
                wo_copy(0, i).start()

        def ff(i, _):
            ff_tile(0, 2 * i)
            ff_tile(1, 2 * i + 1)
            return 0

        lax.fori_loop(0, n_ff // 2, ff, 0)
        if n_ff % 2:
            ff_tile(0, n_ff - 1)
        swiglu((n_ff - 1) % 2, n_ff - 1)

        @pl.when(st >= 1)
        def _():
            finish(1 - par)

        following = st + 1
        turn = lax.rem(following, chunks)
        source = turn + lax.div(following, stages) * (c - turn)
        n_norm = 4
        groups = ROWS // 16 // n_norm

        def down(j, with_norm):
            gt = w0 + n_q + 2 + 2 * n_ff + j
            s0 = w_wait(gt)

            @pl.when(c == 0)
            def _():
                wo_copy(layer, j).wait()

            @pl.when(j >= 2)
            def _():
                chip_sum(st, j - 2)

            gj = st * n_dn + j
            if with_norm:
                for i in range(groups):
                    norm_rows(source, lax.div(following, chunks), (j - (n_dn - n_norm)) * groups + i)
            ybuf[lax.rem(gj, X_SLOTS)] = dot(u_s[...], wbuf[s0]) + dot(att_s[...], wobuf[j])
            chip_copy(gj).start()
            w_next(gt)

            @pl.when((c == chunks - 1) & (layer < layers - 1))
            def _():
                wo_copy(layer + 1, j).start()

        def down_plain(j, _):
            down(j, False)
            return 0

        def down_norm(j, _):
            down(j, True)
            return 0

        lax.fori_loop(0, n_dn - n_norm, down_plain, 0)

        @pl.when(following < chunks)
        def _():
            x_copy(turn).wait()

        @pl.when((following >= chunks) & (following < stages))
        def _():
            new_wait(turn)

        lax.fori_loop(n_dn - n_norm, n_dn, down_norm, 0)
        return 0

    x_copy(0).wait()

    def first(i, _):
        norm_rows(0, 0, 2 * i)
        norm_rows(0, 0, 2 * i + 1)
        return 0

    lax.fori_loop(0, ROWS // 32, first, 0)
    for raw in raws:
        raw[...] = jnp.zeros_like(raw)
    lax.fori_loop(0, stages, stage, 0)

    last = (stages - 1) % chunks
    for j in range(n_dn - 2, n_dn):
        chip_sum(stages - 1, j)
    new_wait(1 - last)
    out_copy(1 - last).start()
    finish(last)
    new_wait(last)
    out_copy(last).start()
    for c in range(chunks):
        out_copy(c).wait()


def solution(mesh):
    arg_specs = (P('dp', None), P('dp'), P(), P(None, None, 'tp'), P(None, None, 'tp'), P(None, None, 'tp'), P(None, 'tp', None), P(None, None, 'tp'), P(None, None, 'tp'), P(None, 'tp', None), P(None, 'dp', None, 'tp', None), P(None, 'dp', None, 'tp', None))

    def per_device(x_in, lengths, norm_gain, w_q, w_k, w_v, w_o, w_gate, w_up, w_down, k_cache, v_cache):
        layers, tokens, seq, kv_heads, head = k_cache.shape
        width = x_in.shape[1]
        half = head // 2
        inv_freq = 1.0 / (np.float32(ROPE_BASE) ** (np.arange(0, head, 2).astype(np.float32) / np.float32(head)))
        pos = np.arange(seq).astype(np.float32)[:, None]
        angles = pos * inv_freq[None, :].astype(np.float32)
        table = np.concatenate([np.cos(angles), np.sin(angles), pos + 0 * angles], 1).astype(np.float32)

        def rows_of(cache):
            r = cache.reshape(layers * tokens * seq, kv_heads, 2, half).transpose(0, 2, 1, 3)
            return r.reshape(layers * tokens * seq * kv_heads * 2, half)

        tok_rows = seq * kv_heads * 2
        n_dn = width // TILE
        vm = pl.BlockSpec(memory_space=pltpu.VMEM)
        hbm = pl.BlockSpec(memory_space=pl.ANY)
        bf, f32 = jnp.bfloat16, jnp.float32
        dma = pltpu.SemaphoreType.DMA
        return pl.pallas_call(
            functools.partial(kernel, (layers, tokens, width, seq, kv_heads)),
            out_shape=jax.ShapeDtypeStruct(x_in.shape, bf),
            in_specs=[vm] * 3 + [hbm] * 10,
            out_specs=hbm,
            scratch_shapes=[
                pltpu.VMEM((tokens, width), bf),
                pltpu.VMEM((ROWS, width), bf),
                pltpu.VMEM((2, 4 * ROWS, half), f32),
                pltpu.VMEM((2, 4 * ROWS, half), f32),
                pltpu.VMEM((2, 4 * ROWS, half), f32),
                pltpu.VMEM((ROWS, w_q.shape[2]), bf),
                pltpu.VMEM((ROWS, w_gate.shape[2]), bf),
                [pltpu.VMEM((ROWS, TILE), bf)] * 4,
                pltpu.VMEM((tokens, half), f32),
                pltpu.VMEM((tokens, half), f32),
                pltpu.VMEM((tokens, half), f32),
                pltpu.VMEM((4 * ROWS, half), f32),
                pltpu.VMEM((4 * KV_TOK, 2 * tok_rows), f32),
                [pltpu.VMEM((8 * KV_TOK, 2 * tok_rows), f32)] * 2,
                [pltpu.VMEM((8 * KV_TOK, 2 * tok_rows), bf)] * 2,
                [pltpu.VMEM((2, 4 * KV_TOK, half), f32)] * 2,
                pltpu.VMEM((SLOTS, width, TILE), bf),
                pltpu.VMEM((n_dn, w_o.shape[1], TILE), bf),
                pltpu.VMEM((KV_SLOTS, KV_TOK * tok_rows, half), bf),
                pltpu.VMEM((KV_SLOTS, KV_TOK * tok_rows, half), bf),
                pltpu.VMEM((X_SLOTS, ROWS, TILE), f32),
                pltpu.VMEM((X_SLOTS, HALF, TILE), f32),
                pltpu.VMEM((n_dn, HALF, TILE), bf),
                pltpu.VMEM((2, n_dn, HALF, TILE), bf),
                dma((SLOTS,)), dma((n_dn,)), dma((2, KV_SLOTS)), dma((2,)),
                dma((X_SLOTS,)), dma((X_SLOTS,)), dma((n_dn,)), dma((2, n_dn)), dma((2, n_dn)), dma((2, n_dn)), dma((2,)),
            ],
            compiler_params=pltpu.CompilerParams(
                collective_id=0, has_side_effects=True, vmem_limit_bytes=67_043_328),
            name="decoder",
        )(lengths.reshape(1, tokens), jnp.asarray(table), norm_gain, x_in, w_q, w_k, w_v, w_o, w_gate, w_up, w_down,
          rows_of(k_cache), rows_of(v_cache))

    return jax.shard_map(per_device, mesh=mesh, in_specs=arg_specs, out_specs=P('dp', None), check_vma=False)
```
